256 devices in a mesh: groups: 2 (over z), seq: 16 (over x, core), qset: 8 (over y).
Axes of the slice: x: 8, y: 8, z: 2, core: 2. Of those that a mesh axis runs over, the one named last changes fastest.
The devices are a block of a 8x8x16 slice.
Arguments:
- states: bfloat16 [16, 16, 128, 4096], P(('groups', 'qset'), 'seq'), parts along dimension 0, may hold values from -7 to 7
- enc_gain: bfloat16 [4096], replicated, may hold values from 0.25 to 1.75
- dec_states: bfloat16 [32, 64, 4096], P(('groups', 'qset')), parts along dimension 0, may hold values from -7 to 7
- dec_gain: bfloat16 [4096], replicated, may hold values from 0.25 to 1.75
- query_weight: bfloat16 [4096, 4096], P(None, 'seq'), may hold values from -0.375 to 0.375
- key_value_weight: bfloat16 [4096, 2, 4096], P(None, None, 'seq'), may hold values from -0.0625 to 0.0625
- out_weight: bfloat16 [4096, 4096], P('seq'), may hold values from -0.75 to 0.75
- question_of: int32 [16, 16, 1], P('groups'), parts along dimension 0, may hold values from 0 to 15; in each aligned block of 16 rows (0 to 15, 16 to 31, ..., all dimensions but the last counted through in order) at most 2 rows name the same one
Outputs:
- mixed: bfloat16 [32, 64, 4096], P(('groups', 'qset'), None, 'seq'), parts along dimension 0
The draws below stay inside these ranges and needn't reach their ends.
There are 2 independent parts, one for each index of `groups`. The reference program is written for one: setup_inputs(seed, part) draws one part's arguments, and reference() takes and returns one part's arrays. A program takes and returns all parts, laid end to end along the dimension named above; an argument that names none is the same for every part. Nothing has to cross between parts.
Inputs may be any that keep to these rules, and one draw needn't show every extreme that they name: `question_of`: within each index of the first dimension (one source group of 16 passages) at most 2 passages name the same question, and exactly 2 do for some question in some groups; every question is named by at least one passage.
All inputs are finite; a program needn't handle non-finite values.
Results may differ from the reference program's by a relative error of at most 0.014.
The reference program's roundings to bfloat16 on the way count: a program that leaves them out, or rounds other values in their place, can miss the bound.
Values may be sent and summed in bfloat16 or wider, within the bound.
A program may use at most 128 MiB of HBM per device.

```python
import math
import jax
import jax.numpy as jnp
import numpy as np
from jax import lax

D = 4096
HEADS = 64
HD = 64
PLEN = 128
CAP = 2
DTOK = 64
QUESTIONS = 16
N_SEQ = 16
N_QSET = 8


def drawn_rows(salt_key, lead_shape):
    values = jax.random.normal(jax.random.fold_in(salt_key, 105), lead_shape + (D,), jnp.float32)
    return jnp.clip(values, -6.0, 6.0)


def draw_states(key, part):
    salt_key = jax.random.fold_in(key, 11)
    lead_shape = (N_QSET, N_SEQ, PLEN)
    result = drawn_rows(salt_key, lead_shape)
    return result.astype(jnp.bfloat16)


def draw_dec_states(key, part):
    salt_key = jax.random.fold_in(key, 12)
    lead_shape = (QUESTIONS, DTOK)
    result = drawn_rows(salt_key, lead_shape)
    return result.astype(jnp.bfloat16)


def weight_tables(key):
    key_part = jax.random.normal(jax.random.fold_in(key, 201), (D, 2, HEADS * HD), jnp.float32)
    key_part = jnp.clip(key_part, -4.0, 4.0) * D ** (-0.5)
    query_part = jax.random.normal(jax.random.fold_in(key, 202), (D, HEADS * HD), jnp.float32)
    query_part = jnp.clip(query_part, -4.0, 4.0) * (D * HD) ** (-0.5)
    return (key_part, query_part)


def draw_key_value_weight(key, part):
    key_part, query_part = weight_tables(key)
    return key_part.astype(jnp.bfloat16)


def draw_query_weight(key, part):
    key_part, query_part = weight_tables(key)
    result = query_part
    return result.astype(jnp.bfloat16)


def steps_of(own_key, dims, split, low, largest):
    def one(dim, blocks):
        draws = jax.random.uniform(jax.random.fold_in(jax.random.fold_in(own_key, 6), dim), (blocks,), jnp.float32, low / len(split), largest / len(split))
        return jnp.repeat(jnp.exp(draws), dims[dim] // blocks).reshape((-1,) + (1,) * (len(dims) - dim - 1))

    loudness = one(*split[0])
    for cut in split[1:]:
        loudness = loudness * one(*cut)
    return loudness


def shared_out(rng, own, number, rows, amount, top, bound, slope):
    order = jax.random.permutation(rng, amount)
    heavy_load, ordinary = load_shares(amount, rows * top, bound, slope, True), load_shares(amount, rows * top, bound, slope, False)
    places = jnp.arange(amount)

    def named(tallies, offset_by):
        used = int((tallies > 0).sum())
        fixed = max(1, used // 4)
        shifted = fixed + (places - fixed + offset_by * (used - fixed)) % max(1, amount - fixed)
        return jnp.zeros((amount,), jnp.int32).at[order[jnp.where(places < fixed, places, shifted)]].set(jnp.asarray(tallies, jnp.int32))

    tallies = jnp.where(number % 4 == 0, named(heavy_load, number // 4), named(ordinary, number - number // 4 - 1))
    mixed = jax.random.permutation(jax.random.fold_in(own, 3), amount)
    giver, sink = mixed[0:amount // 2 * 2:2], mixed[1:amount // 2 * 2:2]
    room = jnp.minimum(tallies[giver] - 1, bound - tallies[sink]) // 2
    room = jnp.where((giver == order[0]) | (sink == order[0]) | (tallies[sink] == 0), 0, jnp.maximum(room, 0))
    shifted = jax.random.randint(jax.random.fold_in(own, 4), (amount // 2,), 0, 1 << 20) % (room + 1)
    tallies = tallies.at[giver].add(-shifted).at[sink].add(shifted)
    items = jnp.searchsorted(jnp.cumsum(tallies), jnp.arange(rows * top), side="right").astype(jnp.int32)
    table = items.reshape(top, rows).T
    table = table[jax.random.permutation(jax.random.fold_in(own, 1), rows)]
    offset_by = jax.random.randint(jax.random.fold_in(own, 2), (rows, 1), 0, top)
    return jnp.take_along_axis(table, (jnp.arange(top)[None, :] + offset_by) % top, axis=1)


def load_shares(amount, total, reach, skew, full):
    portions = [(1 << 20) // math.isqrt(rank ** skew) + 1 for rank in range(1, amount + 1)]
    largest = reach if full else min(reach, max(-(-total // amount), total * portions[0] // sum(portions)))
    least = 1 if total - largest >= amount - 1 else 0
    given, surplus = [largest] + [least] * (amount - 1), total - largest - least * (amount - 1)
    while surplus > 0:
        movable = [i for i in range(1, amount) if given[i] < largest] or [i for i in range(1, amount) if given[i] < reach]
        whole, budget = sum([portions[i] for i in movable]), surplus
        for i in movable:
            more = min(reach - given[i], max(1, budget * portions[i] // whole), surplus)
            given[i] = given[i] + more
            surplus = surplus - more
    return np.array(given)


def normal_values(rng, shape, width, limit, split=(), held_as=jnp.bfloat16):
    array = jax.random.normal(rng, shape, jnp.float32) * width
    if len(split) > 0:
        array = steps_of(rng, shape, split, -0.22, 0.18) * array
    return jnp.clip(array, min=-limit, max=limit).astype(held_as)


def setup_inputs(seed: int = 0, part: int = 0) -> dict:
    arg_keys = jax.random.split(jax.random.key(seed), 9)
    part_keys = jax.random.split(jax.random.fold_in(arg_keys[8], part), 9)
    states = draw_states(jax.random.fold_in(jax.random.fold_in(arg_keys[8], part), 71), part)
    enc_gain = jnp.clip(1.0 + 0.15 * jax.random.normal(arg_keys[1], (D,), jnp.float32), 0.25, 1.75).astype(jnp.bfloat16)
    dec_states = draw_dec_states(jax.random.fold_in(jax.random.fold_in(arg_keys[8], part), 71), part)
    dec_gain = jnp.clip(1.0 + 0.15 * jax.random.normal(arg_keys[3], (D,), jnp.float32), 0.25, 1.75).astype(jnp.bfloat16)
    query_weight = draw_query_weight(jax.random.fold_in(arg_keys[8], 71), part)
    key_value_weight = draw_key_value_weight(jax.random.fold_in(arg_keys[8], 71), part)
    out_weight = normal_values(arg_keys[6], (HEADS * HD, D), HD ** -0.5, 0.75, ((0, 16),))
    question_of_keys = jax.random.split(jax.random.fold_in(part_keys[7], 1), N_QSET * N_SEQ // N_SEQ)
    question_of_turns = jax.random.permutation(jax.random.fold_in(part_keys[7], 3), N_QSET * N_SEQ // N_SEQ)
    question_of = jax.vmap(lambda own, number: shared_out(jax.random.fold_in(part_keys[7], 2), own, number, N_SEQ, QUESTIONS, 1, CAP, 2))(question_of_keys, question_of_turns).reshape((N_QSET, N_SEQ, 1))
    return {"states": states, "enc_gain": enc_gain, "dec_states": dec_states, "dec_gain": dec_gain, "query_weight": query_weight, "key_value_weight": key_value_weight, "out_weight": out_weight, "question_of": question_of}


EPSILON = 1e-06
MASKED_SCORE = -1e+30

def scaled_norm(rows_in, gain_vec):
    rows_f32 = rows_in.astype(jnp.float32)
    mean_square = lax.optimization_barrier(jnp.mean(rows_f32 * rows_f32, axis=-1, keepdims=True))
    return rows_f32 * lax.rsqrt(mean_square + EPSILON) * gain_vec.astype(jnp.float32)

def rounded(values_in):
    return lax.optimization_barrier(values_in.astype(jnp.bfloat16)).astype(jnp.float32)

def reference(states, enc_gain, dec_states, dec_gain, query_weight, key_value_weight, out_weight, question_of):
    enc_rows = scaled_norm(states, enc_gain).astype(jnp.bfloat16).reshape(-1, D)
    passage_question = question_of.reshape(-1).astype(jnp.int32)
    row_question = jnp.repeat(passage_question, PLEN)
    question_count = dec_states.shape[0]
    live_mask = row_question[None, :] == jnp.arange(question_count, dtype=jnp.int32)[:, None]
    dec_rows = scaled_norm(dec_states, dec_gain).astype(jnp.bfloat16).reshape(-1, D)
    query_heads = jnp.transpose(query_weight.reshape(D, HEADS, HD), (1, 0, 2))
    key_heads = jnp.transpose(key_value_weight[:, 0, :].reshape(D, HEADS, HD), (1, 0, 2))
    value_heads = jnp.transpose(key_value_weight[:, 1, :].reshape(D, HEADS, HD), (1, 0, 2))
    out_heads = out_weight.reshape(HEADS, HD, D)

    def one_head(carry, weights_in):
        w_query, w_key, w_value, w_out = weights_in
        queries = jnp.dot(dec_rows, w_query, preferred_element_type=jnp.float32).astype(jnp.bfloat16)
        key_rows = jnp.dot(enc_rows, w_key, preferred_element_type=jnp.float32).astype(jnp.bfloat16)
        value_rows = jnp.dot(enc_rows, w_value, preferred_element_type=jnp.float32).astype(jnp.bfloat16)
        query_blocks = rounded(queries).reshape(question_count, -1, HD)
        scores = jnp.einsum('qtd,rd->qtr', query_blocks, key_rows.astype(jnp.float32))
        scores = jnp.where(live_mask[:, None, :], scores, MASKED_SCORE)
        row_peak = lax.optimization_barrier(jnp.max(scores, axis=-1, keepdims=True))
        weights = jnp.where(live_mask[:, None, :], jnp.exp(scores - row_peak), 0.0)
        row_total = lax.optimization_barrier(jnp.sum(weights, axis=-1, keepdims=True))
        summed = jnp.einsum('qtr,rd->qtd', rounded(weights), value_rows.astype(jnp.float32))
        attended = (summed / row_total).astype(jnp.bfloat16).reshape(-1, HD)
        return (carry + jnp.dot(attended, w_out, preferred_element_type=jnp.float32), None)
    start_sum = jnp.zeros((dec_rows.shape[0], D), jnp.float32)
    projected, unused = lax.scan(one_head, start_sum, (query_heads, key_heads, value_heads, out_heads))
    mixed = dec_states.astype(jnp.float32) + projected.reshape(dec_states.shape)
    return mixed.astype(jnp.bfloat16)
```

```python
import functools

import jax
import jax.numpy as jnp
from jax import lax
from jax.experimental import pallas as pl
from jax.experimental.pallas import tpu as pltpu
from jax.sharding import PartitionSpec as P

HD = 64
EPSILON = 1e-06
DEAD = -1e30
LANES = 128
CORES = 2
CHUNKS = 4
F32 = jnp.float32
BF16 = jnp.bfloat16


def normalise(src, gain, dst_at, total_rows):
    step = 16

    def one(i, carry):
        at = pl.ds(pl.multiple_of(i * step, step), step)
        rows = src[at, :].astype(F32)
        mean_square = jnp.mean(rows * rows, axis=-1, keepdims=True)
        dst_at[at, :] = (rows * lax.rsqrt(mean_square + EPSILON) * gain[...]).astype(BF16)
        return carry

    lax.fori_loop(0, total_rows // step, one, 0)


def kernel(
    table, states_hbm, enc_gain, dec_hbm, dec_gain, wq_hbm, wkv_hbm, wo_hbm, out_ref,
    raw, dec_raw, dec_rows, rows, wq, wkv, wo, kv, qbuf, num, peak, total,
    osend, orecv, lsend, lrecv, lpack, att, psend, precv, xsend, xrecv, first, second, hits,
    load_sem, rs, rr, ls, lr, ds, dr, qs, qr, os_, or_, ss, sr, ps, pr, xs, xr,
):
    shards, groups = lax.axis_size("seq"), lax.axis_size("qset")
    chips = shards // CORES
    me, g = lax.axis_index("seq"), lax.axis_index("qset")
    x, c = lax.div(me, CORES), lax.rem(me, CORES)
    plen, width = raw.shape
    questions, tokens, cols = qbuf.shape
    mine = questions // groups
    piece = plen // CHUNKS
    messages = (chips - 1) * CHUNKS // 2

    def seq_at(chip, core):
        return lax.rem(chip + 2 * chips, chips) * CORES + core

    right, left = seq_at(x + 1, c), seq_at(x - 1, c)
    other = 1 - c
    partner = seq_at(x, other)

    def load(i, src, dst):
        return pltpu.make_async_copy(src, dst, load_sem.at[i])

    loads = [
        load(0, states_hbm, raw),
        load(1, dec_hbm, dec_raw),
        load(2, wq_hbm, wq),
        load(3, wkv_hbm, wkv),
    ]
    for one in loads:
        one.start()
    wide = wo.shape[2]

    def wo_load(i):
        return load(4 + i, wo_hbm.at[:, pl.ds(pl.multiple_of(i * wide, wide), wide)], wo.at[i])

    lax.fori_loop(0, shards, lambda i, n: (wo_load(i).start(), n)[1], 0)

    barrier = pltpu.get_barrier_semaphore()

    def greet_seq(i, n):
        pl.semaphore_signal(barrier, inc=1, device_id={"seq": seq_at(x + i, c)})
        return n

    def greet_qset(i, n):
        pl.semaphore_signal(barrier, inc=1, device_id={"qset": lax.rem(g + i, groups)})
        return n

    pl.semaphore_signal(barrier, inc=1, device_id={"seq": partner})
    lax.fori_loop(1, chips, greet_seq, 0)
    lax.fori_loop(1, groups, greet_qset, 0)

    loads[0].wait()
    normalise(raw, enc_gain, rows.at[me], plen)
    pl.semaphore_wait(barrier, 1 + (chips - 1) + (groups - 1))

    def part(slot, chunk):
        return rows.at[slot, pl.ds(pl.multiple_of(chunk * piece, piece), piece), :]

    def right_copy(m, behind):
        at = part(seq_at(x - lax.div(m, CHUNKS) - behind, c), lax.rem(m, CHUNKS))
        return pltpu.make_async_remote_copy(at, at, rs.at[m], rr.at[m], device_id={"seq": right})

    def left_copy(m, behind):
        at = part(seq_at(x + lax.div(m, CHUNKS) + behind, c), CHUNKS - 1 - lax.rem(m, CHUNKS))
        return pltpu.make_async_remote_copy(at, at, ls.at[m], lr.at[m], device_id={"seq": left})

    def die_copy(k, slot, chunk):
        at = part(slot, chunk)
        return pltpu.make_async_remote_copy(at, at, ds.at[k], dr.at[k], device_id={"seq": partner})

    def from_left(m, core):
        return seq_at(x - lax.div(m, CHUNKS) - 1, core), lax.rem(m, CHUNKS)

    def from_right(m, core):
        return seq_at(x + lax.div(m, CHUNKS) + 1, core), CHUNKS - 1 - lax.rem(m, CHUNKS)

    def start_own(m, n):
        right_copy(m, 0).start()
        left_copy(m, 0).start()
        die_copy(m, me, m).start()
        return n

    lax.fori_loop(0, CHUNKS, start_own, 0)

    loads[1].wait()
    normalise(dec_raw, dec_gain, dec_rows, dec_raw.shape[0])
    loads[2].wait()
    queries = jnp.dot(dec_rows[...], wq[...], preferred_element_type=F32).astype(BF16)
    own_q = qbuf.at[pl.ds(g * mine, mine)]
    own_q[...] = queries.reshape(mine, tokens, cols)

    def query_copy(i):
        to = lax.rem(g + i, groups)
        return pltpu.make_async_remote_copy(
            own_q, own_q, qs.at[i], qr.at[i], device_id={"qset": to}
        )

    def query_arrival(i):
        at = qbuf.at[pl.ds(lax.rem(g - i + groups, groups) * mine, mine)]
        return pltpu.make_async_remote_copy(at, at, qs.at[i], qr.at[i], device_id={"qset": g})

    lax.fori_loop(1, groups, lambda i, n: (query_copy(i).start(), n)[1], 0)

    passages = table.shape[1]

    def find(q, n):
        def look(p, found):
            at0, at1, count = found
            hit = table[g, p] == q
            at0 = jnp.where(hit & (count == 0), p, at0)
            at1 = jnp.where(hit & (count == 1), p, at1)
            return at0, at1, count + hit.astype(jnp.int32)

        zero = jnp.int32(0)
        at0, at1, count = lax.fori_loop(0, passages, look, (zero, zero, zero))
        first[q], second[q], hits[q] = at0, at1, count
        return n

    lax.fori_loop(0, questions, find, 0)

    lane = lax.broadcasted_iota(jnp.int32, (1, LANES), 1)
    low = lane < HD

    def key_values(slots):
        together = jnp.concatenate([part(*s)[...] for s in slots], axis=0)
        result = jnp.dot(together, wkv[...], preferred_element_type=F32).astype(BF16)
        for i, (slot, chunk) in enumerate(slots):
            at = pl.ds(pl.multiple_of(chunk * piece, piece), piece)
            kv[slot, at, :] = result[i * piece : (i + 1) * piece]

    def attend(slot):
        asked = qbuf[table[g, slot]]
        for j in range(cols // LANES):
            at = slice(j * LANES, (j + 1) * LANES)
            pair = asked[:, at]
            none = jnp.zeros_like(pair)
            stacked = jnp.concatenate([jnp.where(low, pair, none), jnp.where(low, none, pair)], axis=0)
            keys = kv[slot, :, at]
            values = kv[slot, :, cols + j * LANES : cols + (j + 1) * LANES]
            scores = lax.dot_general(
                stacked, keys, (((1,), (1,)), ((), ())), preferred_element_type=F32
            )
            top = jnp.max(scores, axis=-1, keepdims=True)
            weights = jnp.exp(scores - top)
            summed = jnp.sum(weights, axis=-1, keepdims=True)
            product = jnp.dot(weights.astype(BF16), values, preferred_element_type=F32)
            num[slot, :, at] = jnp.where(low, product[:tokens], product[tokens:])
            peak[slot, :, at] = jnp.where(low, top[:tokens], top[tokens:])
            total[slot, :, at] = jnp.where(low, summed[:tokens], summed[tokens:])

    loads[3].wait()

    def own_values(m, n):
        key_values([(me, m)])
        die_copy(m, partner, m).wait_recv()
        key_values([(partner, m)])
        return n

    lax.fori_loop(0, CHUNKS, own_values, 0)

    def partner_part(m):
        die_copy(CHUNKS + m, *from_left(m, other)).wait_recv()
        die_copy(CHUNKS + messages + m, *from_right(m, other)).wait_recv()
        key_values([from_left(m, other), from_right(m, other)])

    def step(m, n):
        right_copy(m, 1).wait_recv()

        @pl.when(m + CHUNKS < messages)
        def _():
            right_copy(m + CHUNKS, 0).start()

        die_copy(CHUNKS + m, *from_left(m, c)).start()
        left_copy(m, 1).wait_recv()

        @pl.when(m + CHUNKS < messages)
        def _():
            left_copy(m + CHUNKS, 0).start()

        die_copy(CHUNKS + messages + m, *from_right(m, c)).start()
        key_values([from_left(m, c), from_right(m, c)])

        @pl.when(m > 0)
        def _():
            partner_part(m - 1)

        @pl.when(m == CHUNKS // 2)
        def _():
            lax.fori_loop(1, groups, lambda i, k: (query_arrival(i).wait_recv(), k)[1], 0)
            lax.fori_loop(0, CORES, lambda i, k: (attend(seq_at(x, i)), k)[1], 0)

        @pl.when((m >= CHUNKS) & (lax.rem(m, CHUNKS) == 0))
        def _():
            far = lax.div(m, CHUNKS)

            def both(i, k):
                attend(seq_at(x - far, i))
                attend(seq_at(x + far, i))
                return k

            lax.fori_loop(0, CORES, both, 0)

        return n

    lax.fori_loop(0, messages, step, 0)
    partner_part(messages - 1)
    lax.fori_loop(0, CORES, lambda i, k: (attend(seq_at(x + chips // 2, i)), k)[1], 0)

    lpack[...] = jnp.zeros_like(lpack)
    stride = LANES // 2 // groups
    pairs = cols // LANES

    def out_copy(i, own):
        to = lax.rem(g + i, groups)
        source = lax.rem(g - i + groups, groups)
        dst = orecv.at[source if own else g]
        return pltpu.make_async_remote_copy(
            osend.at[to], dst, os_.at[i], or_.at[i], device_id={"qset": to}
        )

    def lse_copy(i, own):
        to = lax.rem(g + i, groups)
        source = lax.rem(g - i + groups, groups)
        dst = lrecv.at[source if own else g]
        return pltpu.make_async_remote_copy(
            lsend.at[to], dst, ss.at[i], sr.at[i], device_id={"qset": to}
        )

    def merge(i, n):
        to = lax.rem(g + i, groups)
        for own in range(mine):
            q = to * mine + own
            at0, at1, count = first[q], second[q], hits[q]
            for j in range(pairs):
                at = slice(j * LANES, (j + 1) * LANES)
                top0 = jnp.where(count >= 1, peak[at0, :, at], DEAD)
                top1 = jnp.where(count >= 2, peak[at1, :, at], DEAD)
                top = jnp.maximum(top0, top1)
                scale0 = jnp.where(count >= 1, jnp.exp(top0 - top), 0.0)
                scale1 = jnp.where(count >= 2, jnp.exp(top1 - top), 0.0)
                mass = scale0 * total[at0, :, at] + scale1 * total[at1, :, at]
                mass = jnp.where(count >= 1, mass, 1.0)
                mix = (scale0 * num[at0, :, at] + scale1 * num[at1, :, at]) / mass
                osend[to, own * tokens : (own + 1) * tokens, at] = mix.astype(BF16)
                lse = jnp.where(count >= 1, top + jnp.log(mass), DEAD)
                spot = to * stride + own * pairs + j
                hit = (lane == spot) | (lane == HD + spot + stride // 2)
                lpack[:tokens, :] = jnp.where(hit, lse, lpack[:tokens, :])
        return n

    def merge_and_send(i, n):
        merge(i, n)
        out_copy(i, False).start()
        return n

    lax.fori_loop(1, groups, merge_and_send, 0)
    merge(0, 0)
    turned = jnp.transpose(lpack[...])
    lsend[...] = (turned[: LANES // 2] + turned[LANES // 2 :]).reshape(groups, stride, LANES)
    lax.fori_loop(1, groups, lambda i, n: (lse_copy(i, False).start(), n)[1], 0)
    lrecv[g] = lsend[g]
    orecv[g] = osend[g]

    for i in range(shards):
        wo_load(i).wait()

    def arrived(i, n):
        lse_copy(i, True).wait_recv()
        out_copy(i, True).wait_recv()
        return n

    lax.fori_loop(1, groups, arrived, 0)
    every = lrecv[...]
    top = jnp.max(every, axis=0, keepdims=True)
    share = jnp.exp(every - top)
    share = share / jnp.sum(share, axis=0, keepdims=True)
    share = share.reshape(groups * stride, LANES)
    lpack[...] = jnp.transpose(jnp.concatenate([share, share], axis=0))
    for own in range(mine):
        for j in range(pairs):
            at = slice(j * LANES, (j + 1) * LANES)
            here = slice(own * tokens, (own + 1) * tokens)
            mixed = jnp.zeros((tokens, LANES), F32)
            for source in range(groups):
                spot = source * stride + own * pairs + j
                odd = spot + stride // 2
                scale = jnp.where(
                    low, lpack[:tokens, spot : spot + 1], lpack[:tokens, odd : odd + 1]
                )
                mixed = mixed + scale * orecv[source, here, at].astype(F32)
            att[here, at] = mixed.astype(BF16)

    def product(chip, core):
        return jnp.dot(att[...], wo[chip * CORES + core], preferred_element_type=F32)

    def pair_copy(i):
        return pltpu.make_async_remote_copy(
            psend.at[i], precv.at[i], ps.at[i], pr.at[i], device_id={"seq": partner}
        )

    def sum_copy(i, own):
        to = lax.rem(x + i, chips)
        source = lax.rem(x - i + chips, chips)
        return pltpu.make_async_remote_copy(
            xsend.at[i], xrecv.at[i], xs.at[i], xr.at[i], device_id={"seq": seq_at(to, c)}
        )

    def to_partner(k, n):
        i = lax.rem(k + chips // 2, chips)
        psend[i] = product(lax.rem(x + i, chips), other).astype(BF16)
        pair_copy(i).start()
        return n

    lax.fori_loop(0, chips, to_partner, 0)

    def to_chip(k, n):
        i = lax.rem(k + chips // 2, chips)
        half = product(lax.rem(x + i, chips), c)
        pair_copy(i).wait_recv()
        xsend[i] = (half + precv[i].astype(F32)).astype(BF16)

        @pl.when(i > 0)
        def _():
            sum_copy(i, False).start()

        return n

    lax.fori_loop(0, chips, to_chip, 0)
    feature = pl.ds(pl.multiple_of(me * cols, cols), cols)
    result = dec_raw[:, feature].astype(F32) + xsend[0].astype(F32)
    for i in range(1, chips):
        sum_copy(i, True).wait_recv()
        result = result + xrecv[i].astype(F32)
    out_ref[...] = result.astype(BF16).reshape(out_ref.shape)

    def sent(m, n):
        right_copy(m, 0).wait_send()
        left_copy(m, 0).wait_send()
        return n

    lax.fori_loop(0, messages, sent, 0)
    lax.fori_loop(
        0, CHUNKS * chips, lambda k, n: (die_copy(k, me, 0).wait_send(), n)[1], 0
    )

    def sent_qset(i, n):
        query_copy(i).wait_send()
        out_copy(i, False).wait_send()
        lse_copy(i, False).wait_send()
        return n

    lax.fori_loop(1, groups, sent_qset, 0)
    lax.fori_loop(0, chips, lambda i, n: (pair_copy(i).wait_send(), n)[1], 0)
    lax.fori_loop(1, chips, lambda i, n: (sum_copy(i, False).wait_send(), n)[1], 0)


def body(
    states, enc_gain, dec_states, dec_gain, query_weight, key_value_weight, out_weight, question_of
):
    shards, groups = lax.axis_size("seq"), lax.axis_size("qset")
    chips = shards // CORES
    plen, width = states.shape[2:]
    mine, tokens = dec_states.shape[:2]
    cols = query_weight.shape[1]
    questions = mine * groups
    messages = (chips - 1) * CHUNKS // 2
    hbm = pl.BlockSpec(memory_space=pl.ANY)
    vmem = pl.BlockSpec(memory_space=pltpu.VMEM)
    smem = pl.BlockSpec(memory_space=pltpu.SMEM)
    dma = lambda n: pltpu.SemaphoreType.DMA((n,))
    return pl.pallas_call(
        kernel,
        out_shape=jax.ShapeDtypeStruct((mine, tokens, cols), BF16),
        in_specs=[smem, hbm, vmem, hbm, vmem, hbm, hbm, hbm],
        out_specs=vmem,
        scratch_shapes=[
            pltpu.VMEM((plen, width), BF16),
            pltpu.VMEM((mine * tokens, width), BF16),
            pltpu.VMEM((mine * tokens, width), BF16),
            pltpu.VMEM((shards, plen, width), BF16),
            pltpu.VMEM((width, cols), BF16),
            pltpu.VMEM((width, 2 * cols), BF16),
            pltpu.VMEM((shards, cols, cols), BF16),
            pltpu.VMEM((shards, plen, 2 * cols), BF16),
            pltpu.VMEM((questions, tokens, cols), BF16),
            pltpu.VMEM((shards, tokens, cols), F32),
            pltpu.VMEM((shards, tokens, cols), F32),
            pltpu.VMEM((shards, tokens, cols), F32),
            pltpu.VMEM((groups, mine * tokens, cols), BF16),
            pltpu.VMEM((groups, mine * tokens, cols), BF16),
            pltpu.VMEM((groups, LANES // 2 // groups, LANES), F32),
            pltpu.VMEM((groups, LANES // 2 // groups, LANES), F32),
            pltpu.VMEM((LANES, LANES), F32),
            pltpu.VMEM((mine * tokens, cols), BF16),
            pltpu.VMEM((chips, mine * tokens, cols), BF16),
            pltpu.VMEM((chips, mine * tokens, cols), BF16),
            pltpu.VMEM((chips, mine * tokens, cols), BF16),
            pltpu.VMEM((chips, mine * tokens, cols), BF16),
            pltpu.SMEM((questions,), jnp.int32),
            pltpu.SMEM((questions,), jnp.int32),
            pltpu.SMEM((questions,), jnp.int32),
            dma(4 + shards),
            dma(messages), dma(messages), dma(messages), dma(messages),
            dma(CHUNKS * chips), dma(CHUNKS * chips),
            dma(groups), dma(groups), dma(groups), dma(groups), dma(groups), dma(groups),
            dma(chips), dma(chips), dma(chips), dma(chips),
        ],
        compiler_params=pltpu.CompilerParams(
            collective_id=0, has_side_effects=True, vmem_limit_bytes=60 * 1024 * 1024
        ),
        name="reader_step",
    )(
        question_of[:, :, 0],
        states.reshape(plen, width),
        enc_gain.astype(F32).reshape(1, width),
        dec_states.reshape(mine * tokens, width),
        dec_gain.astype(F32).reshape(1, width),
        query_weight,
        key_value_weight.reshape(width, 2 * cols),
        out_weight,
    )


def solution(mesh):
    return jax.shard_map(
        body,
        mesh=mesh,
        in_specs=(
            P(("groups", "qset"), "seq", None, None),
            P(),
            P(("groups", "qset"), None, None),
            P(),
            P(None, "seq"),
            P(None, None, "seq"),
            P("seq", None),
            P("groups", None, None),
        ),
        out_specs=P(("groups", "qset"), None, "seq"),
        check_vma=False,
    )
```

```python
import functools

import jax
import jax.numpy as jnp
from jax import lax
from jax.experimental import pallas as pl
from jax.experimental.pallas import tpu as pltpu
from jax.sharding import PartitionSpec as P

HD = 64
EPSILON = 1e-06
DEAD = -1e30
LANES = 128
CORES = 2
CHUNKS = 4
F32 = jnp.float32
BF16 = jnp.bfloat16


def normalise(src, gain, dst_at, total_rows):
    step = 16

    def one(i, carry):
        at = pl.ds(pl.multiple_of(i * step, step), step)
        rows = src[at, :].astype(F32)
        mean_square = jnp.mean(rows * rows, axis=-1, keepdims=True)
        dst_at[at, :] = (rows * lax.rsqrt(mean_square + EPSILON) * gain[...]).astype(BF16)
        return carry

    lax.fori_loop(0, total_rows // step, one, 0)


def kernel(
    table, states_hbm, enc_gain, dec_hbm, dec_gain, wq_hbm, wkv_hbm, wo_hbm, out_ref,
    raw, dec_raw, dec_rows, rows, wq, wkv_in, wkv, wo, kv, qbuf, num, peak, total,
    osend, orecv, lsend, lrecv, shares, att, half, psend, precv, xsend, xrecv, gains,
    first, second, hits,
    load_sem, rs, rr, ls, lr, ds, dr, qs, qr, os_, or_, ss, sr, ps, pr, xs, xr, rising, falling,
):
    shards, groups = lax.axis_size("seq"), lax.axis_size("qset")
    chips = shards // CORES
    me, g = lax.axis_index("seq"), lax.axis_index("qset")
    x, c = lax.div(me, CORES), lax.rem(me, CORES)
    plen, width = raw.shape
    questions, tokens, cols = qbuf.shape
    mine = questions // groups
    piece = plen // CHUNKS
    messages = (chips - 1) * CHUNKS // 2

    def seq_at(chip, core):
        return lax.rem(chip + 2 * chips, chips) * CORES + core

    right, left = seq_at(x + 1, c), seq_at(x - 1, c)
    other = 1 - c
    partner = seq_at(x, other)

    def load(i, src, dst):
        return pltpu.make_async_copy(src, dst, load_sem.at[i])

    states_load = load(0, states_hbm, raw)
    dec_load = load(1, dec_hbm, dec_raw)
    wq_load = load(2, wq_hbm, wq)
    wkv_load = load(3, wkv_hbm, wkv_in)

    def wo_load(i):
        chip, core = lax.div(i, CORES), lax.rem(i, CORES)
        src = wo_hbm.at[:, pl.ds(pl.multiple_of(i * cols, cols), cols)]
        dst = wo.at[core, :, pl.ds(pl.multiple_of(chip * cols, cols), cols)]
        return load(4 + i, src, dst)

    states_load.start()

    barrier = pltpu.get_barrier_semaphore()
    above, below = g + 1, g - 1

    def greet_seq(i, n):
        pl.semaphore_signal(barrier, inc=1, device_id={"seq": seq_at(x + i, c)})
        return n

    pl.semaphore_signal(barrier, inc=1, device_id={"seq": partner})
    lax.fori_loop(1, chips, greet_seq, 0)

    def if_above(do):
        pl.when(g < groups - 1)(do)

    def if_below(do):
        pl.when(g > 0)(do)

    if_above(lambda: pl.semaphore_signal(barrier, inc=1, device_id={"qset": above}))
    if_below(lambda: pl.semaphore_signal(barrier, inc=1, device_id={"qset": below}))

    gains[0:1, :] = enc_gain[...].astype(F32).reshape(1, width)
    gains[8:9, :] = dec_gain[...].astype(F32).reshape(1, width)
    states_load.wait()
    dec_load.start()
    wq_load.start()
    wkv_load.start()
    lax.fori_loop(0, shards, lambda i, n: (wo_load(i).start(), n)[1], 0)
    normalise(raw, gains.at[0:1, :], rows.at[me], plen)
    rows_beside = lax.div(g + groups - 1, groups) + 1 - lax.div(g + 1, groups)
    pl.semaphore_wait(barrier, chips + rows_beside)

    def part(slot, chunk):
        return rows.at[slot, pl.ds(pl.multiple_of(chunk * piece, piece), piece), :]

    def right_copy(m, behind):
        at = part(seq_at(x - lax.div(m, CHUNKS) - behind, c), lax.rem(m, CHUNKS))
        return pltpu.make_async_remote_copy(at, at, rs.at[m], rr.at[m], device_id={"seq": right})

    def left_copy(m, behind):
        at = part(seq_at(x + lax.div(m, CHUNKS) + behind, c), CHUNKS - 1 - lax.rem(m, CHUNKS))
        return pltpu.make_async_remote_copy(at, at, ls.at[m], lr.at[m], device_id={"seq": left})

    def die_copy(k, slot, chunk):
        at = part(slot, chunk)
        return pltpu.make_async_remote_copy(at, at, ds.at[k], dr.at[k], device_id={"seq": partner})

    def from_left(m, core):
        return seq_at(x - lax.div(m, CHUNKS) - 1, core), lax.rem(m, CHUNKS)

    def from_right(m, core):
        return seq_at(x + lax.div(m, CHUNKS) + 1, core), CHUNKS - 1 - lax.rem(m, CHUNKS)

    def start_own(m, n):
        right_copy(m, 0).start()
        left_copy(m, 0).start()
        die_copy(m, me, m).start()
        return n

    lax.fori_loop(0, CHUNKS, start_own, 0)

    dec_load.wait()
    normalise(dec_raw, gains.at[8:9, :], dec_rows, dec_raw.shape[0])
    wq_load.wait()
    queries = jnp.dot(dec_rows[...], wq[...], preferred_element_type=F32).astype(BF16)
    own_q = qbuf.at[pl.ds(g * mine, mine)]
    own_q[...] = queries.reshape(mine, tokens, cols)

    def query_copy(i):
        to = lax.rem(g + i, groups)
        return pltpu.make_async_remote_copy(
            own_q, own_q, qs.at[i], qr.at[i], device_id={"qset": to}
        )

    def query_arrival(i):
        at = qbuf.at[pl.ds(lax.rem(g - i + groups, groups) * mine, mine)]
        return pltpu.make_async_remote_copy(at, at, qs.at[i], qr.at[i], device_id={"qset": g})

    passages = table.shape[1]

    def find(q, n):
        def look(p, found):
            at0, at1, count = found
            hit = table[g, p] == q
            at0 = jnp.where(hit & (count == 0), p, at0)
            at1 = jnp.where(hit & (count == 1), p, at1)
            return at0, at1, count + hit.astype(jnp.int32)

        zero = jnp.int32(0)
        at0, at1, count = lax.fori_loop(0, passages, look, (zero, zero, zero))
        first[q], second[q], hits[q] = at0, at1, count
        return n

    lax.fori_loop(0, questions, find, 0)

    lane = lax.broadcasted_iota(jnp.int32, (1, LANES), 1)
    low = lane < HD

    def key_values(slots):
        together = jnp.concatenate([part(*s)[...] for s in slots], axis=0)
        result = jnp.dot(together, wkv[...], preferred_element_type=F32).astype(BF16)
        for i, (slot, chunk) in enumerate(slots):
            at = pl.ds(pl.multiple_of(chunk * piece, piece), piece)
            kv[slot, at, :] = result[i * piece : (i + 1) * piece]

    def attend(slot):
        asked = qbuf[table[g, slot]]
        for j in range(cols // LANES):
            at = slice(j * LANES, (j + 1) * LANES)
            pair = asked[:, at]
            none = jnp.zeros_like(pair)
            stacked = jnp.concatenate([jnp.where(low, pair, none), jnp.where(low, none, pair)], axis=0)
            keys = kv[slot, :, at]
            values = kv[slot, :, cols + j * LANES : cols + (j + 1) * LANES]
            scores = lax.dot_general(
                stacked, keys, (((1,), (1,)), ((), ())), preferred_element_type=F32
            )
            top = jnp.max(scores, axis=-1, keepdims=True)
            weights = jnp.exp(scores - top)
            summed = jnp.sum(weights, axis=-1, keepdims=True)
            product = jnp.dot(weights.astype(BF16), values, preferred_element_type=F32)
            num[slot, :, at] = jnp.where(low, product[:tokens], product[tokens:])
            peak[slot, :, at] = jnp.where(low, top[:tokens], top[tokens:])
            total[slot, :, at] = jnp.where(low, summed[:tokens], summed[tokens:])

    wkv_load.wait()
    block = 64

    def unzip(i, n):
        at = pl.ds(pl.multiple_of(i * block, block), block)
        wkv[at, :cols] = wkv_in[at, 0, :]
        wkv[at, cols:] = wkv_in[at, 1, :]
        return n

    lax.fori_loop(0, width // block, unzip, 0)

    def own_values(m, n):
        key_values([(me, m)])
        die_copy(m, partner, m).wait_recv()
        key_values([(partner, m)])
        return n

    lax.fori_loop(0, CHUNKS, own_values, 0)

    def partner_part(m):
        die_copy(CHUNKS + m, *from_left(m, other)).wait_recv()
        die_copy(CHUNKS + messages + m, *from_right(m, other)).wait_recv()
        key_values([from_left(m, other), from_right(m, other)])

    def step(m, n):
        right_copy(m, 1).wait_recv()

        @pl.when(m + CHUNKS < messages)
        def _():
            right_copy(m + CHUNKS, 0).start()

        die_copy(CHUNKS + m, *from_left(m, c)).start()
        left_copy(m, 1).wait_recv()

        @pl.when(m + CHUNKS < messages)
        def _():
            left_copy(m + CHUNKS, 0).start()

        die_copy(CHUNKS + messages + m, *from_right(m, c)).start()
        key_values([from_left(m, c), from_right(m, c)])

        @pl.when(m > 0)
        def _():
            partner_part(m - 1)

        @pl.when(m == CHUNKS // 2)
        def _():
            if_above(lambda: pl.semaphore_wait(falling, 1))
            if_below(lambda: pl.semaphore_signal(falling, inc=1, device_id={"qset": below}))
            lax.fori_loop(1, groups, lambda i, k: (query_copy(i).start(), k)[1], 0)

        @pl.when(m == messages // 2)
        def _():
            lax.fori_loop(1, groups, lambda i, k: (query_arrival(i).wait_recv(), k)[1], 0)
            lax.fori_loop(0, CORES, lambda i, k: (attend(seq_at(x, i)), k)[1], 0)

        for far in range(1, chips // 2):

            @pl.when(m == max(far * CHUNKS, messages // 2 + far))
            def _():
                def both(i, k):
                    attend(seq_at(x - far, i))
                    attend(seq_at(x + far, i))
                    return k

                lax.fori_loop(0, CORES, both, 0)

        return n

    if_below(lambda: pl.semaphore_wait(rising, 1))
    if_above(lambda: pl.semaphore_signal(rising, inc=1, device_id={"qset": above}))
    lax.fori_loop(0, messages, step, 0)
    attend(seq_at(x + chips // 2, c))
    partner_part(messages - 1)
    attend(seq_at(x + chips // 2, other))

    pairs = cols // LANES
    odd_row = 4
    lse_rows = lsend.shape[2]

    def alternate(k, n):
        reach = lax.div(k + 1, 2)
        return n // 2 - reach + 2 * reach * lax.rem(k, 2)

    def out_copy(own, i, arrival):
        to = lax.rem(g + i, groups)
        source = lax.rem(g - i + groups, groups)
        at = own * groups + i
        return pltpu.make_async_remote_copy(
            osend.at[own, to],
            orecv.at[own, source if arrival else g],
            os_.at[at], or_.at[at], device_id={"qset": to},
        )

    def lse_copy(own, i, arrival):
        to = lax.rem(g + i, groups)
        source = lax.rem(g - i + groups, groups)
        at = own * groups + i
        return pltpu.make_async_remote_copy(
            lsend.at[own, to],
            lrecv.at[own, source if arrival else g],
            ss.at[at], sr.at[at], device_id={"qset": to},
        )

    def merge(own, to, mix_at, lse_at):
        q = to * mine + own
        at0, at1, count = first[q], second[q], hits[q]
        packed = jnp.zeros((tokens, LANES), F32)
        for j in range(pairs):
            at = slice(j * LANES, (j + 1) * LANES)
            top0 = jnp.where(count >= 1, peak[at0, :, at], DEAD)
            top1 = jnp.where(count >= 2, peak[at1, :, at], DEAD)
            top = jnp.maximum(top0, top1)
            scale0 = jnp.where(count >= 1, jnp.exp(top0 - top), 0.0)
            scale1 = jnp.where(count >= 2, jnp.exp(top1 - top), 0.0)
            mass = scale0 * total[at0, :, at] + scale1 * total[at1, :, at]
            mass = jnp.where(count >= 1, mass, 1.0)
            mix = (scale0 * num[at0, :, at] + scale1 * num[at1, :, at]) / mass
            mix_at[:, at] = mix.astype(BF16)
            lse = jnp.where(count >= 1, top + jnp.log(mass), DEAD)
            packed = jnp.where((lane == j) | (lane == HD + odd_row + j), lse, packed)
        turned = jnp.transpose(packed)
        lse_at[:, :tokens] = turned[:lse_rows] + turned[HD : HD + lse_rows]

    lsend[...] = jnp.zeros_like(lsend)
    lrecv_pad = jnp.zeros(lrecv.shape[2:], F32)

    def merge_and_send(own):
        def one(k, n):
            i = alternate(k, groups)
            to = lax.rem(g + i, groups)
            merge(own, to, osend.at[own, to], lsend.at[own, to])
            lse_copy(own, i, False).start()
            out_copy(own, i, False).start()
            return n

        lax.fori_loop(0, groups - 1, one, 0)

    for own in range(mine):
        merge_and_send(own)
    for own in range(mine):
        lrecv[own, g] = lrecv_pad
        merge(own, g, orecv.at[own, g], lrecv.at[own, g])
    lax.fori_loop(0, shards, lambda i, n: (wo_load(i).wait(), n)[1], 0)

    def pair_copy(own):
        return pltpu.make_async_remote_copy(
            psend.at[own], precv.at[own], ps.at[own], pr.at[own], device_id={"seq": partner}
        )

    def chip_part(chip):
        return pl.ds(pl.multiple_of(chip * cols, cols), cols)

    def sum_copy(own, i):
        to = lax.rem(x + i, chips)
        at = own * chips + i
        return pltpu.make_async_remote_copy(
            xsend.at[own, :, chip_part(to)], xrecv.at[own, i],
            xs.at[at], xr.at[at], device_id={"seq": seq_at(to, c)},
        )

    def project(own):
        def arrived(k, n):
            i = alternate(k, groups)
            lse_copy(own, i, True).wait_recv()
            out_copy(own, i, True).wait_recv()
            return n

        lax.fori_loop(0, groups - 1, arrived, 0)
        every = lrecv[own]
        top = jnp.max(every, axis=0, keepdims=True)
        share = jnp.exp(every - top)
        share = share / jnp.sum(share, axis=0, keepdims=True)
        shares[...] = jnp.transpose(share.reshape(groups * lse_rows, LANES))
        for j in range(pairs):
            at = slice(j * LANES, (j + 1) * LANES)
            mixed = jnp.zeros((tokens, LANES), F32)
            for source in range(groups):
                even, odd = source * lse_rows + j, source * lse_rows + odd_row + j
                scale = jnp.where(
                    low, shares[:tokens, even : even + 1], shares[:tokens, odd : odd + 1]
                )
                mixed = mixed + scale * orecv[own, source, :, at].astype(F32)
            att[:, at] = mixed.astype(BF16)

        psend[own] = jnp.dot(att[...], wo[other], preferred_element_type=F32).astype(BF16)
        pair_copy(own).start()
        half[...] = jnp.dot(att[...], wo[c], preferred_element_type=F32)
        pair_copy(own).wait_recv()

        def add(i):
            at = chip_part(lax.rem(x + i, chips))
            xsend[own, :, at] = (half[:, at] + precv[own, :, at].astype(F32)).astype(BF16)

        def to_chip(k, n):
            i = alternate(k, chips)
            add(i)
            sum_copy(own, i).start()
            return n

        lax.fori_loop(0, chips - 1, to_chip, 0)
        add(0)

    for own in range(mine):
        project(own)

    feature = pl.ds(pl.multiple_of(me * cols, cols), cols)
    for own in range(mine):
        here = slice(own * tokens, (own + 1) * tokens)
        result = dec_raw[here, feature].astype(F32) + xsend[own, :, chip_part(x)].astype(F32)
        for i in range(1, chips):
            sum_copy(own, i).wait_recv()
            result = result + xrecv[own, i].astype(F32)
        out_ref[own] = result.astype(BF16)

    def sent(m, n):
        right_copy(m, 0).wait_send()
        left_copy(m, 0).wait_send()
        return n

    lax.fori_loop(0, messages, sent, 0)
    lax.fori_loop(
        0, CHUNKS * chips, lambda k, n: (die_copy(k, me, 0).wait_send(), n)[1], 0
    )

    lax.fori_loop(1, groups, lambda i, n: (query_copy(i).wait_send(), n)[1], 0)
    for own in range(mine):

        def sent_qset(i, n):
            out_copy(own, i, False).wait_send()
            lse_copy(own, i, False).wait_send()
            return n

        lax.fori_loop(1, groups, sent_qset, 0)
        pair_copy(own).wait_send()
        lax.fori_loop(1, chips, lambda i, n: (sum_copy(own, i).wait_send(), n)[1], 0)


def body(
    states, enc_gain, dec_states, dec_gain, query_weight, key_value_weight, out_weight, question_of
):
    shards, groups = lax.axis_size("seq"), lax.axis_size("qset")
    chips = shards // CORES
    plen, width = states.shape[2:]
    mine, tokens = dec_states.shape[:2]
    cols = query_weight.shape[1]
    questions = mine * groups
    messages = (chips - 1) * CHUNKS // 2
    hbm = pl.BlockSpec(memory_space=pl.ANY)
    vmem = pl.BlockSpec(memory_space=pltpu.VMEM)
    smem = pl.BlockSpec(memory_space=pltpu.SMEM)
    dma = lambda n: pltpu.SemaphoreType.DMA((n,))
    return pl.pallas_call(
        kernel,
        out_shape=jax.ShapeDtypeStruct((mine, tokens, cols), BF16),
        in_specs=[smem, hbm, vmem, hbm, vmem, hbm, hbm, hbm],
        out_specs=vmem,
        scratch_shapes=[
            pltpu.VMEM((plen, width), BF16),
            pltpu.VMEM((mine * tokens, width), BF16),
            pltpu.VMEM((mine * tokens, width), BF16),
            pltpu.VMEM((shards, plen, width), BF16),
            pltpu.VMEM((width, cols), BF16),
            pltpu.VMEM((width, 2, cols), BF16),
            pltpu.VMEM((width, 2 * cols), BF16),
            pltpu.VMEM((CORES, cols, chips * cols), BF16),
            pltpu.VMEM((shards, plen, 2 * cols), BF16),
            pltpu.VMEM((questions, tokens, cols), BF16),
            pltpu.VMEM((shards, tokens, cols), F32),
            pltpu.VMEM((shards, tokens, cols), F32),
            pltpu.VMEM((shards, tokens, cols), F32),
            pltpu.VMEM((mine, groups, tokens, cols), BF16),
            pltpu.VMEM((mine, groups, tokens, cols), BF16),
            pltpu.VMEM((mine, groups, 8, LANES), F32),
            pltpu.VMEM((mine, groups, 8, LANES), F32),
            pltpu.VMEM((LANES, groups * 8), F32),
            pltpu.VMEM((tokens, cols), BF16),
            pltpu.VMEM((tokens, chips * cols), F32),
            pltpu.VMEM((mine, tokens, chips * cols), BF16),
            pltpu.VMEM((mine, tokens, chips * cols), BF16),
            pltpu.VMEM((mine, tokens, chips * cols), BF16),
            pltpu.VMEM((mine, chips, tokens, cols), BF16),
            pltpu.VMEM((16, width), F32),
            pltpu.SMEM((questions,), jnp.int32),
            pltpu.SMEM((questions,), jnp.int32),
            pltpu.SMEM((questions,), jnp.int32),
            dma(4 + shards),
            dma(messages), dma(messages), dma(messages), dma(messages),
            dma(CHUNKS * chips), dma(CHUNKS * chips),
            dma(groups), dma(groups),
            dma(mine * groups), dma(mine * groups), dma(mine * groups), dma(mine * groups),
            dma(mine), dma(mine), dma(mine * chips), dma(mine * chips),
            pltpu.SemaphoreType.REGULAR, pltpu.SemaphoreType.REGULAR,
        ],
        compiler_params=pltpu.CompilerParams(
            collective_id=0, has_side_effects=True, vmem_limit_bytes=60 * 1024 * 1024
        ),
        name="reader_step",
    )(
        question_of[:, :, 0],
        states.reshape(plen, width),
        enc_gain,
        dec_states.reshape(mine * tokens, width),
        dec_gain,
        query_weight,
        key_value_weight,
        out_weight,
    )


def solution(mesh):
    return jax.shard_map(
        body,
        mesh=mesh,
        in_specs=(
            P(("groups", "qset"), "seq", None, None),
            P(),
            P(("groups", "qset"), None, None),
            P(),
            P(None, "seq"),
            P(None, None, "seq"),
            P("seq", None),
            P("groups", None, None),
        ),
        out_specs=P(("groups", "qset"), None, "seq"),
        check_vma=False,
    )
```

```python
import functools

import jax
import jax.numpy as jnp
from jax import lax
from jax.experimental import pallas as pl
from jax.experimental.pallas import tpu as pltpu
from jax.sharding import PartitionSpec as P

HD = 64
EPSILON = 1e-06
DEAD = -1e30
LANES = 128
CORES = 2
CHUNKS = 4
LAG = 4
PARTS = 2
F32 = jnp.float32
BF16 = jnp.bfloat16


def normalise(src, gain, dst_at, total_rows):
    step = 16

    def one(i, carry):
        at = pl.ds(pl.multiple_of(i * step, step), step)
        rows = src[at, :].astype(F32)
        mean_square = jnp.mean(rows * rows, axis=-1, keepdims=True)
        dst_at[at, :] = (rows * lax.rsqrt(mean_square + EPSILON) * gain[...]).astype(BF16)
        return carry

    lax.fori_loop(0, total_rows // step, one, 0)


def kernel(
    table, states_hbm, enc_gain, dec_hbm, dec_gain, wq_hbm, wkv_hbm, wo_hbm, out_ref,
    raw, dec_raw, dec_rows, rows, wq, wkv_in, wkv, wo, kv, qbuf, num, peak, total,
    osend, orecv, lsend, lrecv, shares, att, half, psend, precv, xsend, xrecv, gains,
    first, second, hits,
    load_sem, rs, rr, ls, lr, ds, dr, qs, qr, os_, or_, ss, sr, ps, pr, xs, xr, rising, falling,
):
    shards, groups = lax.axis_size("seq"), lax.axis_size("qset")
    chips = shards // CORES
    me, g = lax.axis_index("seq"), lax.axis_index("qset")
    x, c = lax.div(me, CORES), lax.rem(me, CORES)
    plen, width = raw.shape
    questions, tokens, cols = qbuf.shape
    mine = questions // groups
    piece = plen // CHUNKS
    messages = (chips - 1) * CHUNKS // 2

    def seq_at(chip, core):
        return lax.rem(chip + 2 * chips, chips) * CORES + core

    right, left = seq_at(x + 1, c), seq_at(x - 1, c)
    other = 1 - c
    partner = seq_at(x, other)

    def load(i, src, dst):
        return pltpu.make_async_copy(src, dst, load_sem.at[i])

    states_load = load(0, states_hbm, raw)
    dec_load = load(1, dec_hbm, dec_raw)
    wq_load = load(2, wq_hbm, wq)
    wkv_load = load(3, wkv_hbm, wkv_in)

    def wo_load(i):
        chip, core = lax.div(i, CORES), lax.rem(i, CORES)
        src = wo_hbm.at[:, pl.ds(pl.multiple_of(i * cols, cols), cols)]
        dst = wo.at[core, :, pl.ds(pl.multiple_of(chip * cols, cols), cols)]
        return load(4 + i, src, dst)

    states_load.start()

    barrier = pltpu.get_barrier_semaphore()
    above, below = g + 1, g - 1

    def if_above(do):
        pl.when(g < groups - 1)(do)

    def if_below(do):
        pl.when(g > 0)(do)

    pl.semaphore_signal(barrier, inc=1, device_id={"seq": left})
    pl.semaphore_signal(barrier, inc=1, device_id={"seq": right})

    @pl.when(c == 1)
    def _():
        pl.semaphore_signal(barrier, inc=1, device_id={"seq": partner})

    if_below(lambda: pl.semaphore_signal(barrier, inc=1, device_id={"qset": below}))

    gains[0:1, :] = enc_gain[...].astype(F32).reshape(1, width)
    gains[8:9, :] = dec_gain[...].astype(F32).reshape(1, width)
    states_load.wait()
    dec_load.start()
    wq_load.start()
    wkv_load.start()
    lax.fori_loop(0, shards, lambda i, n: (wo_load(i).start(), n)[1], 0)
    normalise(raw, gains.at[0:1, :], rows.at[me], plen)
    pl.semaphore_wait(barrier, 2 + (1 - c) + 1 - lax.div(g + 1, groups))

    def part(slot, chunk):
        return rows.at[slot, pl.ds(pl.multiple_of(chunk * piece, piece), piece), :]

    def right_copy(m, behind):
        at = part(seq_at(x - lax.div(m, CHUNKS) - behind, c), lax.rem(m, CHUNKS))
        return pltpu.make_async_remote_copy(at, at, rs.at[m], rr.at[m], device_id={"seq": right})

    def left_copy(m, behind):
        at = part(seq_at(x + lax.div(m, CHUNKS) + behind, c), CHUNKS - 1 - lax.rem(m, CHUNKS))
        return pltpu.make_async_remote_copy(at, at, ls.at[m], lr.at[m], device_id={"seq": left})

    def die_copy(k, slot, chunk):
        at = part(slot, chunk)
        return pltpu.make_async_remote_copy(at, at, ds.at[k], dr.at[k], device_id={"seq": partner})

    def from_left(m, core):
        return seq_at(x - lax.div(m, CHUNKS) - 1, core), lax.rem(m, CHUNKS)

    def from_right(m, core):
        return seq_at(x + lax.div(m, CHUNKS) + 1, core), CHUNKS - 1 - lax.rem(m, CHUNKS)

    def start_own(m, n):
        right_copy(m, 0).start()
        left_copy(m, 0).start()

        @pl.when(c == 0)
        def _():
            die_copy(m, me, m).start()

        return n

    lax.fori_loop(0, CHUNKS, start_own, 0)

    @pl.when(g == 0)
    def _():
        pl.semaphore_signal(rising, inc=1, device_id={"qset": above})

    own_q = qbuf.at[pl.ds(g * mine, mine)]

    def own_queries():
        dec_load.wait()
        normalise(dec_raw, gains.at[8:9, :], dec_rows, dec_raw.shape[0])
        wq_load.wait()
        queries = jnp.dot(dec_rows[...], wq[...], preferred_element_type=F32).astype(BF16)
        own_q[...] = queries.reshape(mine, tokens, cols)

    def query_copy(i):
        to = lax.rem(g + i, groups)
        return pltpu.make_async_remote_copy(
            own_q, own_q, qs.at[i], qr.at[i], device_id={"qset": to}
        )

    def query_arrival(i):
        at = qbuf.at[pl.ds(lax.rem(g - i + groups, groups) * mine, mine)]
        return pltpu.make_async_remote_copy(at, at, qs.at[i], qr.at[i], device_id={"qset": g})

    passages = table.shape[1]

    def find(q, n):
        def look(p, found):
            at0, at1, count = found
            hit = table[g, p] == q
            at0 = jnp.where(hit & (count == 0), p, at0)
            at1 = jnp.where(hit & (count == 1), p, at1)
            return at0, at1, count + hit.astype(jnp.int32)

        zero = jnp.int32(0)
        at0, at1, count = lax.fori_loop(0, passages, look, (zero, zero, zero))
        first[q], second[q], hits[q] = at0, at1, count
        return n

    lane = lax.broadcasted_iota(jnp.int32, (1, LANES), 1)
    low = lane < HD

    def key_values(slots):
        together = jnp.concatenate([part(*s)[...] for s in slots], axis=0)
        result = jnp.dot(together, wkv[...], preferred_element_type=F32).astype(BF16)
        for i, (slot, chunk) in enumerate(slots):
            at = pl.ds(pl.multiple_of(chunk * piece, piece), piece)
            kv[slot, at, :] = result[i * piece : (i + 1) * piece]

    def attend(slot):
        asked = qbuf[table[g, slot]]
        for j in range(cols // LANES):
            at = slice(j * LANES, (j + 1) * LANES)
            pair = asked[:, at]
            none = jnp.zeros_like(pair)
            stacked = jnp.concatenate([jnp.where(low, pair, none), jnp.where(low, none, pair)], axis=0)
            keys = kv[slot, :, at]
            values = kv[slot, :, cols + j * LANES : cols + (j + 1) * LANES]
            scores = lax.dot_general(
                stacked, keys, (((1,), (1,)), ((), ())), preferred_element_type=F32
            )
            top = jnp.max(scores, axis=-1, keepdims=True)
            weights = jnp.exp(scores - top)
            summed = jnp.sum(weights, axis=-1, keepdims=True)
            product = jnp.dot(weights.astype(BF16), values, preferred_element_type=F32)
            num[slot, :, at] = jnp.where(low, product[:tokens], product[tokens:])
            peak[slot, :, at] = jnp.where(low, top[:tokens], top[tokens:])
            total[slot, :, at] = jnp.where(low, summed[:tokens], summed[tokens:])

    wkv_load.wait()
    block = 64

    def unzip(i, n):
        at = pl.ds(pl.multiple_of(i * block, block), block)
        wkv[at, :cols] = wkv_in[at, 0, :]
        wkv[at, cols:] = wkv_in[at, 1, :]
        return n

    lax.fori_loop(0, width // block, unzip, 0)

    def whole_values(slot):
        result = jnp.dot(rows[slot], wkv[...], preferred_element_type=F32)
        kv[slot] = result.astype(BF16)

    def partner_part(m):
        die_copy(CHUNKS + m, *from_left(m, other)).wait_recv()
        die_copy(CHUNKS + messages + m, *from_right(m, other)).wait_recv()
        key_values([from_left(m, other), from_right(m, other)])

    def die_right(m):
        die_copy(CHUNKS + m, *from_left(m, c)).start()

    def die_left(m):
        die_copy(CHUNKS + messages + m, *from_right(m, c)).start()

    hold = 2
    catch = messages - 4
    partner_at = min(LAG, catch)

    def part_done(m):
        return m + LAG if m + LAG < catch else max(catch, m + 1)

    def step(m, n):
        right_copy(m, 1).wait_recv()

        @pl.when(m + CHUNKS < messages)
        def _():
            right_copy(m + CHUNKS, 0).start()

        @pl.when((1 - c) * messages + m > hold)
        def _():
            die_right(m)

        left_copy(m, 1).wait_recv()

        @pl.when(m + CHUNKS < messages)
        def _():
            left_copy(m + CHUNKS, 0).start()

        @pl.when((1 - c) * messages + m > hold)
        def _():
            die_left(m)

        @pl.when(m == 0)
        def _():
            whole_values(me)

        key_values([from_left(m, c), from_right(m, c)])

        @pl.when(m == 1)
        def _():
            own_queries()
            if_below(lambda: pl.semaphore_wait(rising, 1))

            @pl.when(g > 0)
            def _():
                if_above(
                    lambda: pl.semaphore_signal(rising, inc=1, device_id={"qset": above})
                )

        @pl.when(m == hold)
        def _():
            @pl.when(c == 1)
            def _():
                die_copy(0, partner, 0).wait_recv()
                lax.fori_loop(0, CHUNKS, lambda k, t: (die_copy(k, me, k).start(), t)[1], 0)

                def late(k, t):
                    die_right(k)
                    die_left(k)
                    return t

                lax.fori_loop(0, hold + 1, late, 0)

            if_above(lambda: pl.semaphore_wait(falling, 1))
            if_below(lambda: pl.semaphore_signal(falling, inc=1, device_id={"qset": below}))
            lax.fori_loop(1, groups, lambda i, k: (query_copy(i).start(), k)[1], 0)

        @pl.when(m == hold + 1)
        def _():
            lax.fori_loop(0, questions, find, 0)

        @pl.when(m == partner_at)
        def _():
            @pl.when(c == 0)
            def _():
                die_copy(0, partner, 0).wait_recv()

            lax.fori_loop(
                1, CHUNKS, lambda k, t: (die_copy(k, partner, k).wait_recv(), t)[1], 0
            )
            whole_values(partner)

        if catch > LAG:

            @pl.when(m >= LAG)
            def _():
                @pl.when(m < catch)
                def _():
                    partner_part(m - LAG)

        @pl.when(m == catch)
        def _():
            lax.fori_loop(
                max(0, catch - LAG), catch, lambda k, t: (partner_part(k), t)[1], 0
            )

        @pl.when(m > catch)
        def _():
            partner_part(m - 1)

        @pl.when(m == messages // 2)
        def _():
            lax.fori_loop(1, groups, lambda i, k: (query_arrival(i).wait_recv(), k)[1], 0)
            lax.fori_loop(0, CORES, lambda i, k: (attend(seq_at(x, i)), k)[1], 0)

        for far in range(1, chips // 2):

            @pl.when(m == max(part_done(far * CHUNKS - 1), messages // 2 + far))
            def _():
                def both(i, k):
                    attend(seq_at(x - far, i))
                    attend(seq_at(x + far, i))
                    return k

                lax.fori_loop(0, CORES, both, 0)

        return n

    lax.fori_loop(0, messages, step, 0)
    partner_part(messages - 1)
    attend(seq_at(x + chips // 2, c))
    attend(seq_at(x + chips // 2, other))

    pairs = cols // LANES
    odd_row = 4
    lse_rows = lsend.shape[2]

    def alternate(k, n):
        reach = lax.div(k + 1, 2)
        return n // 2 - reach + 2 * reach * lax.rem(k, 2)

    short = tokens // PARTS

    def out_copy(own, cut, i, arrival):
        to = lax.rem(g + i, groups)
        source = lax.rem(g - i + groups, groups)
        at = (own * PARTS + cut) * groups + i
        here = pl.ds(cut * short, short)
        return pltpu.make_async_remote_copy(
            osend.at[own, to, here],
            orecv.at[own, source if arrival else g, here],
            os_.at[at], or_.at[at], device_id={"qset": to},
        )

    def lse_copy(own, i, arrival):
        to = lax.rem(g + i, groups)
        source = lax.rem(g - i + groups, groups)
        at = own * groups + i
        return pltpu.make_async_remote_copy(
            lsend.at[own, to],
            lrecv.at[own, source if arrival else g],
            ss.at[at], sr.at[at], device_id={"qset": to},
        )

    def merge(own, to, mix_at, lse_at):
        q = to * mine + own
        at0, at1, count = first[q], second[q], hits[q]
        packed = jnp.zeros((tokens, LANES), F32)
        for j in range(pairs):
            at = slice(j * LANES, (j + 1) * LANES)
            top0 = jnp.where(count >= 1, peak[at0, :, at], DEAD)
            top1 = jnp.where(count >= 2, peak[at1, :, at], DEAD)
            top = jnp.maximum(top0, top1)
            scale0 = jnp.where(count >= 1, jnp.exp(top0 - top), 0.0)
            scale1 = jnp.where(count >= 2, jnp.exp(top1 - top), 0.0)
            mass = scale0 * total[at0, :, at] + scale1 * total[at1, :, at]
            mass = jnp.where(count >= 1, mass, 1.0)
            mix = (scale0 * num[at0, :, at] + scale1 * num[at1, :, at]) / mass
            mix_at[:, at] = mix.astype(BF16)
            lse = jnp.where(count >= 1, top + jnp.log(mass), DEAD)
            packed = jnp.where((lane == j) | (lane == HD + odd_row + j), lse, packed)
        turned = jnp.transpose(packed)
        lse_at[:, :tokens] = turned[:lse_rows] + turned[HD : HD + lse_rows]

    lsend[...] = jnp.zeros_like(lsend)
    lrecv_pad = jnp.zeros(lrecv.shape[2:], F32)

    def merge_and_send(own):
        def one(k, n):
            i = alternate(k, groups)
            to = lax.rem(g + i, groups)
            merge(own, to, osend.at[own, to], lsend.at[own, to])
            lse_copy(own, i, False).start()
            out_copy(own, 0, i, False).start()
            return n

        lax.fori_loop(0, groups - 1, one, 0)
        for cut in range(1, PARTS):

            def rest(k, n):
                out_copy(own, cut, alternate(k, groups), False).start()
                return n

            lax.fori_loop(0, groups - 1, rest, 0)

    for own in range(mine):
        merge_and_send(own)
    for own in range(mine):
        lrecv[own, g] = lrecv_pad
        merge(own, g, orecv.at[own, g], lrecv.at[own, g])
    lax.fori_loop(0, shards, lambda i, n: (wo_load(i).wait(), n)[1], 0)

    def pair_copy(piece):
        return pltpu.make_async_remote_copy(
            psend.at[piece], precv.at[piece], ps.at[piece], pr.at[piece],
            device_id={"seq": partner},
        )

    def chip_part(chip):
        return pl.ds(pl.multiple_of(chip * cols, cols), cols)

    def sum_copy(piece, i):
        to = lax.rem(x + i, chips)
        at = piece * chips + i
        return pltpu.make_async_remote_copy(
            xsend.at[piece, :, chip_part(to)], xrecv.at[piece, i],
            xs.at[at], xr.at[at], device_id={"seq": seq_at(to, c)},
        )

    def share_of(own):
        lax.fori_loop(
            0, groups - 1,
            lambda k, n: (lse_copy(own, alternate(k, groups), True).wait_recv(), n)[1], 0,
        )
        every = lrecv[own]
        top = jnp.max(every, axis=0, keepdims=True)
        share = jnp.exp(every - top)
        share = share / jnp.sum(share, axis=0, keepdims=True)
        shares[...] = jnp.transpose(share.reshape(groups * lse_rows, LANES))

    def project(own, cut):
        piece = own * PARTS + cut
        here = slice(cut * short, (cut + 1) * short)
        lax.fori_loop(
            0, groups - 1,
            lambda k, n: (out_copy(own, cut, alternate(k, groups), True).wait_recv(), n)[1], 0,
        )
        for j in range(pairs):
            at = slice(j * LANES, (j + 1) * LANES)
            mixed = jnp.zeros((short, LANES), F32)
            for source in range(groups):
                even, odd = source * lse_rows + j, source * lse_rows + odd_row + j
                scale = jnp.where(low, shares[here, even : even + 1], shares[here, odd : odd + 1])
                mixed = mixed + scale * orecv[own, source, here, at].astype(F32)
            att[:, at] = mixed.astype(BF16)

        psend[piece] = jnp.dot(att[...], wo[other], preferred_element_type=F32).astype(BF16)
        pair_copy(piece).start()
        half[...] = jnp.dot(att[...], wo[c], preferred_element_type=F32)
        pair_copy(piece).wait_recv()

        def add(i):
            at = chip_part(lax.rem(x + i, chips))
            xsend[piece, :, at] = (half[:, at] + precv[piece, :, at].astype(F32)).astype(BF16)

        def to_chip(k, n):
            i = alternate(k, chips)
            add(i)
            sum_copy(piece, i).start()
            return n

        lax.fori_loop(0, chips - 1, to_chip, 0)
        add(0)

    for own in range(mine):
        share_of(own)
        for cut in range(PARTS):
            project(own, cut)

    def sent(m, n):
        right_copy(m, 0).wait_send()
        left_copy(m, 0).wait_send()
        return n

    lax.fori_loop(0, messages, sent, 0)
    lax.fori_loop(
        0, CHUNKS * chips, lambda k, n: (die_copy(k, me, 0).wait_send(), n)[1], 0
    )

    lax.fori_loop(1, groups, lambda i, n: (query_copy(i).wait_send(), n)[1], 0)
    for own in range(mine):

        def sent_qset(i, n):
            lse_copy(own, i, False).wait_send()
            for cut in range(PARTS):
                out_copy(own, cut, i, False).wait_send()
            return n

        lax.fori_loop(1, groups, sent_qset, 0)

    feature = pl.ds(pl.multiple_of(me * cols, cols), cols)
    for piece in range(mine * PARTS):
        here = slice(piece * short, (piece + 1) * short)
        result = dec_raw[here, feature].astype(F32) + xsend[piece, :, chip_part(x)].astype(F32)
        for i in range(1, chips):
            sum_copy(piece, i).wait_recv()
            result = result + xrecv[piece, i].astype(F32)
        own, cut = divmod(piece, PARTS)
        out_ref[own, cut * short : (cut + 1) * short, :] = result.astype(BF16)
    for piece in range(mine * PARTS):
        pair_copy(piece).wait_send()
        lax.fori_loop(1, chips, lambda i, n: (sum_copy(piece, i).wait_send(), n)[1], 0)


def body(
    states, enc_gain, dec_states, dec_gain, query_weight, key_value_weight, out_weight, question_of
):
    shards, groups = lax.axis_size("seq"), lax.axis_size("qset")
    chips = shards // CORES
    plen, width = states.shape[2:]
    mine, tokens = dec_states.shape[:2]
    cols = query_weight.shape[1]
    questions = mine * groups
    messages = (chips - 1) * CHUNKS // 2
    pieces, short = mine * PARTS, tokens // PARTS
    hbm = pl.BlockSpec(memory_space=pl.ANY)
    vmem = pl.BlockSpec(memory_space=pltpu.VMEM)
    smem = pl.BlockSpec(memory_space=pltpu.SMEM)
    dma = lambda n: pltpu.SemaphoreType.DMA((n,))
    return pl.pallas_call(
        kernel,
        out_shape=jax.ShapeDtypeStruct((mine, tokens, cols), BF16),
        in_specs=[smem, hbm, vmem, hbm, vmem, hbm, hbm, hbm],
        out_specs=vmem,
        scratch_shapes=[
            pltpu.VMEM((plen, width), BF16),
            pltpu.VMEM((mine * tokens, width), BF16),
            pltpu.VMEM((mine * tokens, width), BF16),
            pltpu.VMEM((shards, plen, width), BF16),
            pltpu.VMEM((width, cols), BF16),
            pltpu.VMEM((width, 2, cols), BF16),
            pltpu.VMEM((width, 2 * cols), BF16),
            pltpu.VMEM((CORES, cols, chips * cols), BF16),
            pltpu.VMEM((shards, plen, 2 * cols), BF16),
            pltpu.VMEM((questions, tokens, cols), BF16),
            pltpu.VMEM((shards, tokens, cols), F32),
            pltpu.VMEM((shards, tokens, cols), F32),
            pltpu.VMEM((shards, tokens, cols), F32),
            pltpu.VMEM((mine, groups, tokens, cols), BF16),
            pltpu.VMEM((mine, groups, tokens, cols), BF16),
            pltpu.VMEM((mine, groups, 8, LANES), F32),
            pltpu.VMEM((mine, groups, 8, LANES), F32),
            pltpu.VMEM((LANES, groups * 8), F32),
            pltpu.VMEM((short, cols), BF16),
            pltpu.VMEM((short, chips * cols), F32),
            pltpu.VMEM((pieces, short, chips * cols), BF16),
            pltpu.VMEM((pieces, short, chips * cols), BF16),
            pltpu.VMEM((pieces, short, chips * cols), BF16),
            pltpu.VMEM((pieces, chips, short, cols), BF16),
            pltpu.VMEM((16, width), F32),
            pltpu.SMEM((questions,), jnp.int32),
            pltpu.SMEM((questions,), jnp.int32),
            pltpu.SMEM((questions,), jnp.int32),
            dma(4 + shards),
            dma(messages), dma(messages), dma(messages), dma(messages),
            dma(CHUNKS * chips), dma(CHUNKS * chips),
            dma(groups), dma(groups),
            dma(pieces * groups), dma(pieces * groups), dma(mine * groups), dma(mine * groups),
            dma(pieces), dma(pieces), dma(pieces * chips), dma(pieces * chips),
            pltpu.SemaphoreType.REGULAR, pltpu.SemaphoreType.REGULAR,
        ],
        compiler_params=pltpu.CompilerParams(
            collective_id=0, has_side_effects=True, vmem_limit_bytes=60 * 1024 * 1024
        ),
        name="reader_step",
    )(
        question_of[:, :, 0],
        states.reshape(plen, width),
        enc_gain,
        dec_states.reshape(mine * tokens, width),
        dec_gain,
        query_weight,
        key_value_weight,
        out_weight,
    )


def solution(mesh):
    return jax.shard_map(
        body,
        mesh=mesh,
        in_specs=(
            P(("groups", "qset"), "seq", None, None),
            P(),
            P(("groups", "qset"), None, None),
            P(),
            P(None, "seq"),
            P(None, None, "seq"),
            P("seq", None),
            P("groups", None, None),
        ),
        out_specs=P(("groups", "qset"), None, "seq"),
        check_vma=False,
    )
```

```python
import functools

import jax
import jax.numpy as jnp
from jax import lax
from jax.experimental import pallas as pl
from jax.experimental.pallas import tpu as pltpu
from jax.sharding import PartitionSpec as P

HD = 64
EPSILON = 1e-06
DEAD = -1e30
LANES = 128
CORES = 2
CHUNKS = 4
LAG = 4
PARTS = 2
F32 = jnp.float32
BF16 = jnp.bfloat16


def normalise(src, gain, dst_at, start, rows_here):
    step = 16

    def one(i, carry):
        at = pl.ds(pl.multiple_of(start + i * step, step), step)
        rows = src[at, :].astype(F32)
        mean_square = jnp.mean(rows * rows, axis=-1, keepdims=True)
        dst_at[at, :] = (rows * lax.rsqrt(mean_square + EPSILON) * gain[...]).astype(BF16)
        return carry

    lax.fori_loop(0, rows_here // step, one, 0)


def kernel(
    table_hbm, states_hbm, enc_gain_hbm, dec_hbm, dec_gain_hbm, wq_hbm, wkv_hbm, wo_hbm, out_ref,
    raw, dec_raw, dec_rows, rows, wq, wkv_in, wkv, wo, kv, qbuf, num, peak, total,
    osend, orecv, lsend, lrecv, shares, att, half, psend, precv, xsend, xrecv, gains,
    enc_gain, dec_gain, table, first, second, hits,
    load_sem, rs, rr, lr, ds, dr, qs, qr, os_, or_, ss, sr, ps, pr, xs, xr, rising, falling,
):
    shards, groups = lax.axis_size("seq"), lax.axis_size("qset")
    chips = shards // CORES
    me, g = lax.axis_index("seq"), lax.axis_index("qset")
    x, c = lax.div(me, CORES), lax.rem(me, CORES)
    plen, width = raw.shape
    questions, tokens, cols = qbuf.shape
    mine = questions // groups
    piece = plen // CHUNKS
    messages = (chips - 1) * CHUNKS // 2

    def seq_at(chip, core):
        return lax.rem(chip + 2 * chips, chips) * CORES + core

    right, left = seq_at(x + 1, c), seq_at(x - 1, c)
    other = 1 - c
    partner = seq_at(x, other)

    def load(i, src, dst):
        return pltpu.make_async_copy(src, dst, load_sem.at[i])

    def states_load(k):
        at = pl.ds(k * piece, piece)
        return load(k, states_hbm.at[at], raw.at[at])

    enc_gain_load = load(CHUNKS, enc_gain_hbm, enc_gain)
    dec_load = load(CHUNKS + 1, dec_hbm, dec_raw)
    wq_load = load(CHUNKS + 2, wq_hbm, wq)
    wkv_load = load(CHUNKS + 3, wkv_hbm, wkv_in)
    dec_gain_load = load(CHUNKS + 4, dec_gain_hbm, dec_gain)
    table_load = load(CHUNKS + 5, table_hbm, table)

    def wo_load(i):
        chip, core = lax.div(i, CORES), lax.rem(i, CORES)
        src = wo_hbm.at[:, pl.ds(pl.multiple_of(i * cols, cols), cols)]
        dst = wo.at[core, :, pl.ds(pl.multiple_of(chip * cols, cols), cols)]
        return load(CHUNKS + 6, src, dst)

    inward = [k // 2 if k % 2 == 0 else CHUNKS - 1 - k // 2 for k in range(CHUNKS)]
    enc_gain_load.start()
    for k in inward:
        states_load(k).start()

    barrier = pltpu.get_barrier_semaphore()
    above, below = g + 1, g - 1

    def if_above(do):
        pl.when(g < groups - 1)(do)

    def if_below(do):
        pl.when(g > 0)(do)

    pl.semaphore_signal(barrier, inc=1, device_id={"seq": left})
    pl.semaphore_signal(barrier, inc=1, device_id={"seq": right})

    @pl.when(c == 1)
    def _():
        pl.semaphore_signal(barrier, inc=1, device_id={"seq": partner})

    if_below(lambda: pl.semaphore_signal(barrier, inc=1, device_id={"qset": below}))

    def part(slot, chunk):
        return rows.at[slot, pl.ds(pl.multiple_of(chunk * piece, piece), piece), :]

    def right_copy(m, behind):
        at = part(seq_at(x - lax.div(m, CHUNKS) - behind, c), lax.rem(m, CHUNKS))
        return pltpu.make_async_remote_copy(at, at, rs, rr.at[m], device_id={"seq": right})

    def left_copy(m, behind):
        at = part(seq_at(x + lax.div(m, CHUNKS) + behind, c), CHUNKS - 1 - lax.rem(m, CHUNKS))
        return pltpu.make_async_remote_copy(at, at, rs, lr.at[m], device_id={"seq": left})

    def die_copy(k, slot, chunk):
        at = part(slot, chunk)
        return pltpu.make_async_remote_copy(at, at, ds, dr.at[k], device_id={"seq": partner})

    def from_left(m, core):
        return seq_at(x - lax.div(m, CHUNKS) - 1, core), lax.rem(m, CHUNKS)

    def from_right(m, core):
        return seq_at(x + lax.div(m, CHUNKS) + 1, core), CHUNKS - 1 - lax.rem(m, CHUNKS)

    enc_gain_load.wait()
    gains[0:1, :] = enc_gain[...].astype(F32).reshape(1, width)
    done, sent_right, sent_left = set(), 0, 0
    for k in inward:
        states_load(k).wait()
        normalise(raw, gains.at[0:1, :], rows.at[me], k * piece, piece)
        if not done:
            pl.semaphore_wait(barrier, 2 + (1 - c) + 1 - lax.div(g + 1, groups))
        done.add(k)
        while sent_right in done:
            right_copy(jnp.int32(sent_right), 0).start()
            sent_right += 1
        while CHUNKS - 1 - sent_left in done:
            left_copy(jnp.int32(sent_left), 0).start()
            sent_left += 1
    for one in (wkv_load, dec_load, dec_gain_load, wq_load, table_load):
        one.start()
    lax.fori_loop(0, shards, lambda i, n: (wo_load(i).start(), n)[1], 0)

    @pl.when(c == 0)
    def _():
        lax.fori_loop(0, CHUNKS, lambda m, n: (die_copy(m, me, m).start(), n)[1], 0)

    @pl.when(g == 0)
    def _():
        pl.semaphore_signal(rising, inc=1, device_id={"qset": above})

    own_q = qbuf.at[pl.ds(g * mine, mine)]

    def own_queries():
        dec_load.wait()
        dec_gain_load.wait()
        gains[8:9, :] = dec_gain[...].astype(F32).reshape(1, width)
        normalise(dec_raw, gains.at[8:9, :], dec_rows, 0, dec_raw.shape[0])
        wq_load.wait()
        queries = jnp.dot(dec_rows[...], wq[...], preferred_element_type=F32).astype(BF16)
        own_q[...] = queries.reshape(mine, tokens, cols)

    def query_copy(i):
        to = lax.rem(g + i, groups)
        return pltpu.make_async_remote_copy(
            own_q, own_q, qs, qr, device_id={"qset": to}
        )

    def query_all():
        at = qbuf.at[pl.ds(0, questions - mine)]
        return pltpu.make_async_remote_copy(at, at, qs, qr, device_id={"qset": above})

    passages = table.shape[1]

    def find(q, n):
        def look(p, found):
            at0, at1, count = found
            hit = table[g, p] == q
            at0 = jnp.where(hit & (count == 0), p, at0)
            at1 = jnp.where(hit & (count == 1), p, at1)
            return at0, at1, count + hit.astype(jnp.int32)

        zero = jnp.int32(0)
        at0, at1, count = lax.fori_loop(0, passages, look, (zero, zero, zero))
        first[q], second[q], hits[q] = at0, at1, count
        return n

    lane = lax.broadcasted_iota(jnp.int32, (1, LANES), 1)
    low = lane < HD

    def key_values(slots):
        together = jnp.concatenate([part(*s)[...] for s in slots], axis=0)
        result = jnp.dot(together, wkv[...], preferred_element_type=F32).astype(BF16)
        for i, (slot, chunk) in enumerate(slots):
            at = pl.ds(pl.multiple_of(chunk * piece, piece), piece)
            kv[slot, at, :] = result[i * piece : (i + 1) * piece]

    def attend(slot):
        asked = qbuf[table[g, slot]]
        for j in range(cols // LANES):
            at = slice(j * LANES, (j + 1) * LANES)
            pair = asked[:, at]
            none = jnp.zeros_like(pair)
            stacked = jnp.concatenate([jnp.where(low, pair, none), jnp.where(low, none, pair)], axis=0)
            keys = kv[slot, :, at]
            values = kv[slot, :, cols + j * LANES : cols + (j + 1) * LANES]
            scores = lax.dot_general(
                stacked, keys, (((1,), (1,)), ((), ())), preferred_element_type=F32
            )
            top = jnp.max(scores, axis=-1, keepdims=True)
            weights = jnp.exp(scores - top)
            summed = jnp.sum(weights, axis=-1, keepdims=True)
            product = jnp.dot(weights.astype(BF16), values, preferred_element_type=F32)
            num[slot, :, at] = jnp.where(low, product[:tokens], product[tokens:])
            peak[slot, :, at] = jnp.where(low, top[:tokens], top[tokens:])
            total[slot, :, at] = jnp.where(low, summed[:tokens], summed[tokens:])

    wkv_load.wait()
    block = 64

    def unzip(i, n):
        at = pl.ds(pl.multiple_of(i * block, block), block)
        wkv[at, :cols] = wkv_in[at, 0, :]
        wkv[at, cols:] = wkv_in[at, 1, :]
        return n

    lax.fori_loop(0, width // block, unzip, 0)

    def whole_values(slot):
        result = jnp.dot(rows[slot], wkv[...], preferred_element_type=F32)
        kv[slot] = result.astype(BF16)

    def partner_part(m):
        die_copy(CHUNKS + m, *from_left(m, other)).wait_recv()
        die_copy(CHUNKS + messages + m, *from_right(m, other)).wait_recv()
        key_values([from_left(m, other), from_right(m, other)])

    def die_right(m):
        die_copy(CHUNKS + m, *from_left(m, c)).start()

    def die_left(m):
        die_copy(CHUNKS + messages + m, *from_right(m, c)).start()

    hold = 2
    catch = messages - 4
    partner_at = min(LAG, catch)

    def part_done(m):
        return m + LAG if m + LAG < catch else max(catch, m + 1)

    def step(m, n):
        right_copy(m, 1).wait_recv()

        @pl.when(m + CHUNKS < messages)
        def _():
            right_copy(m + CHUNKS, 0).start()

        @pl.when((1 - c) * messages + m > hold)
        def _():
            die_right(m)

        left_copy(m, 1).wait_recv()

        @pl.when(m + CHUNKS < messages)
        def _():
            left_copy(m + CHUNKS, 0).start()

        @pl.when((1 - c) * messages + m > hold)
        def _():
            die_left(m)

        @pl.when(m == 0)
        def _():
            whole_values(me)

        key_values([from_left(m, c), from_right(m, c)])

        @pl.when(m == 1)
        def _():
            own_queries()
            if_below(lambda: pl.semaphore_wait(rising, 1))

            @pl.when(g > 0)
            def _():
                if_above(
                    lambda: pl.semaphore_signal(rising, inc=1, device_id={"qset": above})
                )

        @pl.when(m == hold)
        def _():
            @pl.when(c == 1)
            def _():
                die_copy(0, partner, 0).wait_recv()
                lax.fori_loop(0, CHUNKS, lambda k, t: (die_copy(k, me, k).start(), t)[1], 0)

                def late(k, t):
                    die_right(k)
                    die_left(k)
                    return t

                lax.fori_loop(0, hold + 1, late, 0)

            if_above(lambda: pl.semaphore_wait(falling, 1))
            if_below(lambda: pl.semaphore_signal(falling, inc=1, device_id={"qset": below}))
            lax.fori_loop(1, groups, lambda i, k: (query_copy(i).start(), k)[1], 0)

        @pl.when(m == hold + 1)
        def _():
            table_load.wait()
            lax.fori_loop(0, questions, find, 0)

        @pl.when(m == partner_at)
        def _():
            @pl.when(c == 0)
            def _():
                die_copy(0, partner, 0).wait_recv()

            lax.fori_loop(
                1, CHUNKS, lambda k, t: (die_copy(k, partner, k).wait_recv(), t)[1], 0
            )
            whole_values(partner)

        if catch > LAG:

            @pl.when(m >= LAG)
            def _():
                @pl.when(m < catch)
                def _():
                    partner_part(m - LAG)

        @pl.when(m == catch)
        def _():
            lax.fori_loop(
                max(0, catch - LAG), catch, lambda k, t: (partner_part(k), t)[1], 0
            )

        @pl.when(m > catch)
        def _():
            partner_part(m - 1)

        @pl.when(m == messages // 2)
        def _():
            query_all().wait_recv()
            lax.fori_loop(0, CORES, lambda i, k: (attend(seq_at(x, i)), k)[1], 0)

        for far in range(1, chips // 2):

            @pl.when(m == max(part_done(far * CHUNKS - 1), messages // 2 + far))
            def _():
                def both(i, k):
                    attend(seq_at(x - far, i))
                    attend(seq_at(x + far, i))
                    return k

                lax.fori_loop(0, CORES, both, 0)

        return n

    lax.fori_loop(0, messages, step, 0)
    partner_part(messages - 1)
    attend(seq_at(x + chips // 2, c))
    attend(seq_at(x + chips // 2, other))

    pairs = cols // LANES
    odd_row = 4
    lse_rows = lsend.shape[2]

    def alternate(k, n):
        reach = lax.div(k + 1, 2)
        return n // 2 - reach + 2 * reach * lax.rem(k, 2)

    short = tokens // PARTS

    def out_copy(own, cut, i):
        to = lax.rem(g + i, groups)
        here = pl.ds(cut * short, short)
        return pltpu.make_async_remote_copy(
            osend.at[own, to, here],
            orecv.at[own, g, here],
            os_, or_.at[own * PARTS + cut], device_id={"qset": to},
        )

    def out_all(own, cut):
        at = orecv.at[own, pl.ds(0, groups - 1), pl.ds(cut * short, short)]
        return pltpu.make_async_remote_copy(
            at, at, os_, or_.at[own * PARTS + cut], device_id={"qset": above}
        )

    def lse_copy(own, i):
        to = lax.rem(g + i, groups)
        return pltpu.make_async_remote_copy(
            lsend.at[own, to],
            lrecv.at[own, g],
            ss, sr.at[own], device_id={"qset": to},
        )

    def lse_all(own):
        at = lrecv.at[own, pl.ds(0, groups - 1)]
        return pltpu.make_async_remote_copy(at, at, ss, sr.at[own], device_id={"qset": above})

    def merge(own, to, mix_at, lse_at):
        q = to * mine + own
        at0, at1, count = first[q], second[q], hits[q]
        packed = jnp.zeros((tokens, LANES), F32)
        for j in range(pairs):
            at = slice(j * LANES, (j + 1) * LANES)
            top0 = jnp.where(count >= 1, peak[at0, :, at], DEAD)
            top1 = jnp.where(count >= 2, peak[at1, :, at], DEAD)
            top = jnp.maximum(top0, top1)
            scale0 = jnp.where(count >= 1, jnp.exp(top0 - top), 0.0)
            scale1 = jnp.where(count >= 2, jnp.exp(top1 - top), 0.0)
            mass = scale0 * total[at0, :, at] + scale1 * total[at1, :, at]
            mass = jnp.where(count >= 1, mass, 1.0)
            mix = (scale0 * num[at0, :, at] + scale1 * num[at1, :, at]) / mass
            mix_at[:, at] = mix.astype(BF16)
            lse = jnp.where(count >= 1, top + jnp.log(mass), DEAD)
            packed = jnp.where((lane == j) | (lane == HD + odd_row + j), lse, packed)
        turned = jnp.transpose(packed)
        lse_at[:, :tokens] = turned[:lse_rows] + turned[HD : HD + lse_rows]

    lsend[...] = jnp.zeros_like(lsend)
    lrecv_pad = jnp.zeros(lrecv.shape[2:], F32)

    def merge_and_send(own):
        def one(k, n):
            i = alternate(k, groups)
            to = lax.rem(g + i, groups)
            merge(own, to, osend.at[own, to], lsend.at[own, to])
            lse_copy(own, i).start()
            out_copy(own, 0, i).start()
            return n

        lax.fori_loop(0, groups - 1, one, 0)
        for cut in range(1, PARTS):

            def rest(k, n):
                out_copy(own, cut, alternate(k, groups)).start()
                return n

            lax.fori_loop(0, groups - 1, rest, 0)

    for own in range(mine):
        merge_and_send(own)
    for own in range(mine):
        lrecv[own, g] = lrecv_pad
        merge(own, g, orecv.at[own, g], lrecv.at[own, g])
    pltpu.make_async_copy(wo, wo, load_sem.at[CHUNKS + 6]).wait()

    def pair_copy(piece):
        return pltpu.make_async_remote_copy(
            psend.at[piece], precv.at[piece], ps, pr.at[piece],
            device_id={"seq": partner},
        )

    def chip_part(chip):
        return pl.ds(pl.multiple_of(chip * cols, cols), cols)

    def sum_copy(piece, i):
        to = lax.rem(x + i, chips)
        return pltpu.make_async_remote_copy(
            xsend.at[piece, :, chip_part(to)], xrecv.at[piece, i],
            xs, xr.at[piece], device_id={"seq": seq_at(to, c)},
        )

    def sum_all(piece):
        at = xrecv.at[piece, pl.ds(1, chips - 1)]
        return pltpu.make_async_remote_copy(at, at, xs, xr.at[piece], device_id={"seq": right})

    def share_of(own):
        lse_all(own).wait_recv()
        every = lrecv[own]
        top = jnp.max(every, axis=0, keepdims=True)
        share = jnp.exp(every - top)
        share = share / jnp.sum(share, axis=0, keepdims=True)
        shares[...] = jnp.transpose(share.reshape(groups * lse_rows, LANES))

    def project(own, cut):
        piece = own * PARTS + cut
        here = slice(cut * short, (cut + 1) * short)
        out_all(own, cut).wait_recv()
        for j in range(pairs):
            at = slice(j * LANES, (j + 1) * LANES)
            mixed = jnp.zeros((short, LANES), F32)
            for source in range(groups):
                even, odd = source * lse_rows + j, source * lse_rows + odd_row + j
                scale = jnp.where(low, shares[here, even : even + 1], shares[here, odd : odd + 1])
                mixed = mixed + scale * orecv[own, source, here, at].astype(F32)
            att[:, at] = mixed.astype(BF16)

        psend[piece] = jnp.dot(att[...], wo[other], preferred_element_type=F32).astype(BF16)
        pair_copy(piece).start()
        half[...] = jnp.dot(att[...], wo[c], preferred_element_type=F32)
        pair_copy(piece).wait_recv()

        def add(i):
            at = chip_part(lax.rem(x + i, chips))
            xsend[piece, :, at] = (half[:, at] + precv[piece, :, at].astype(F32)).astype(BF16)

        def to_chip(k, n):
            i = alternate(k, chips)
            add(i)
            sum_copy(piece, i).start()
            return n

        lax.fori_loop(0, chips - 1, to_chip, 0)
        add(0)

    for own in range(mine):
        share_of(own)
        for cut in range(PARTS):
            project(own, cut)

    def sent(all_of, sem):
        pltpu.make_async_remote_copy(
            all_of, all_of, sem, qr, device_id={"seq": right}
        ).wait_send()

    sent(rows.at[pl.ds(0, chips - 1)], rs)
    sent(rows.at[pl.ds(0, chips)], ds)
    sent(qbuf.at[pl.ds(0, questions - mine)], qs)
    sent(osend.at[:, pl.ds(0, groups - 1)], os_)
    sent(lsend.at[:, pl.ds(0, groups - 1)], ss)
    feature = pl.ds(pl.multiple_of(me * cols, cols), cols)
    for piece in range(mine * PARTS):
        here = slice(piece * short, (piece + 1) * short)
        result = dec_raw[here, feature].astype(F32) + xsend[piece, :, chip_part(x)].astype(F32)
        sum_all(piece).wait_recv()
        for i in range(1, chips):
            result = result + xrecv[piece, i].astype(F32)
        own, cut = divmod(piece, PARTS)
        out_ref[own, cut * short : (cut + 1) * short, :] = result.astype(BF16)
    sent(psend, ps)
    sent(xrecv.at[:, pl.ds(0, chips - 1)], xs)


def body(
    states, enc_gain, dec_states, dec_gain, query_weight, key_value_weight, out_weight, question_of
):
    shards, groups = lax.axis_size("seq"), lax.axis_size("qset")
    chips = shards // CORES
    plen, width = states.shape[2:]
    mine, tokens = dec_states.shape[:2]
    cols = query_weight.shape[1]
    questions = mine * groups
    messages = (chips - 1) * CHUNKS // 2
    pieces, short = mine * PARTS, tokens // PARTS
    hbm = pl.BlockSpec(memory_space=pl.ANY)
    vmem = pl.BlockSpec(memory_space=pltpu.VMEM)
    dma = lambda n: pltpu.SemaphoreType.DMA((n,))
    one = pltpu.SemaphoreType.DMA
    return pl.pallas_call(
        kernel,
        out_shape=jax.ShapeDtypeStruct((mine, tokens, cols), BF16),
        in_specs=[hbm] * 8,
        out_specs=vmem,
        scratch_shapes=[
            pltpu.VMEM((plen, width), BF16),
            pltpu.VMEM((mine * tokens, width), BF16),
            pltpu.VMEM((mine * tokens, width), BF16),
            pltpu.VMEM((shards, plen, width), BF16),
            pltpu.VMEM((width, cols), BF16),
            pltpu.VMEM((width, 2, cols), BF16),
            pltpu.VMEM((width, 2 * cols), BF16),
            pltpu.VMEM((CORES, cols, chips * cols), BF16),
            pltpu.VMEM((shards, plen, 2 * cols), BF16),
            pltpu.VMEM((questions, tokens, cols), BF16),
            pltpu.VMEM((shards, tokens, cols), F32),
            pltpu.VMEM((shards, tokens, cols), F32),
            pltpu.VMEM((shards, tokens, cols), F32),
            pltpu.VMEM((mine, groups, tokens, cols), BF16),
            pltpu.VMEM((mine, groups, tokens, cols), BF16),
            pltpu.VMEM((mine, groups, 8, LANES), F32),
            pltpu.VMEM((mine, groups, 8, LANES), F32),
            pltpu.VMEM((LANES, groups * 8), F32),
            pltpu.VMEM((short, cols), BF16),
            pltpu.VMEM((short, chips * cols), F32),
            pltpu.VMEM((pieces, short, chips * cols), BF16),
            pltpu.VMEM((pieces, short, chips * cols), BF16),
            pltpu.VMEM((pieces, short, chips * cols), BF16),
            pltpu.VMEM((pieces, chips, short, cols), BF16),
            pltpu.VMEM((16, width), F32),
            pltpu.VMEM((width,), BF16),
            pltpu.VMEM((width,), BF16),
            pltpu.SMEM(question_of.shape[:2], jnp.int32),
            pltpu.SMEM((questions,), jnp.int32),
            pltpu.SMEM((questions,), jnp.int32),
            pltpu.SMEM((questions,), jnp.int32),
            dma(CHUNKS + 7),
            one, dma(messages), dma(messages),
            one, dma(CHUNKS * chips),
            one, one, one, dma(pieces), one, dma(mine),
            one, dma(pieces), one, dma(pieces),
            pltpu.SemaphoreType.REGULAR, pltpu.SemaphoreType.REGULAR,
        ],
        compiler_params=pltpu.CompilerParams(
            collective_id=0, has_side_effects=True, vmem_limit_bytes=60 * 1024 * 1024
        ),
        name="reader_step",
    )(
        question_of[:, :, 0],
        states.reshape(plen, width),
        enc_gain,
        dec_states.reshape(mine * tokens, width),
        dec_gain,
        query_weight,
        key_value_weight,
        out_weight,
    )


def solution(mesh):
    return jax.shard_map(
        body,
        mesh=mesh,
        in_specs=(
            P(("groups", "qset"), "seq", None, None),
            P(),
            P(("groups", "qset"), None, None),
            P(),
            P(None, "seq"),
            P(None, None, "seq"),
            P("seq", None),
            P("groups", None, None),
        ),
        out_specs=P(("groups", "qset"), None, "seq"),
        check_vma=False,
    )
```

```python
import functools

import jax
import jax.numpy as jnp
from jax import lax
from jax.experimental import pallas as pl
from jax.experimental.pallas import tpu as pltpu
from jax.sharding import PartitionSpec as P

HD = 64
EPSILON = 1e-06
DEAD = -1e30
LANES = 128
CORES = 2
CHUNKS = 4
LAG = 4
PARTS = 2
F32 = jnp.float32
BF16 = jnp.bfloat16


def normalise(src, gain, dst_at, start, rows_here):
    step = 16

    def one(i, carry):
        at = pl.ds(pl.multiple_of(start + i * step, step), step)
        rows = src[at, :].astype(F32)
        mean_square = jnp.mean(rows * rows, axis=-1, keepdims=True)
        dst_at[at, :] = (rows * lax.rsqrt(mean_square + EPSILON) * gain[...]).astype(BF16)
        return carry

    lax.fori_loop(0, rows_here // step, one, 0)


def kernel(
    table_hbm, states_hbm, enc_gain_hbm, dec_hbm, dec_gain_hbm, wq_hbm, wkv_hbm, wo_hbm, out_ref,
    raw, dec_raw, dec_rows, rows, wq, wkv_in, wkv, wo, kv, qbuf, num, peak, total,
    osend, orecv, lsend, lrecv, shares, att, half, psend, precv, xsend, xrecv, gains,
    enc_gain, dec_gain, table, first, second, hits,
    load_sem, rs, rr, lr, ds, dr, qs, qr, os_, or_, ss, sr, ps, pr, xs, xr, rising, falling,
):
    shards, groups = lax.axis_size("seq"), lax.axis_size("qset")
    chips = shards // CORES
    me, g = lax.axis_index("seq"), lax.axis_index("qset")
    x, c = lax.div(me, CORES), lax.rem(me, CORES)
    plen, width = raw.shape
    questions, tokens, cols = qbuf.shape
    mine = questions // groups
    piece = plen // CHUNKS
    messages = (chips - 1) * CHUNKS // 2

    def seq_at(chip, core):
        return lax.rem(chip + 2 * chips, chips) * CORES + core

    right, left = seq_at(x + 1, c), seq_at(x - 1, c)
    other = 1 - c
    partner = seq_at(x, other)

    def load(i, src, dst):
        return pltpu.make_async_copy(src, dst, load_sem.at[i])

    def states_load(k):
        at = pl.ds(k * piece, piece)
        return load(k, states_hbm.at[at], raw.at[at])

    enc_gain_load = load(CHUNKS, enc_gain_hbm, enc_gain)
    dec_load = load(CHUNKS + 1, dec_hbm, dec_raw)
    wq_load = load(CHUNKS + 2, wq_hbm, wq)
    wkv_load = load(CHUNKS + 3, wkv_hbm, wkv_in)
    dec_gain_load = load(CHUNKS + 4, dec_gain_hbm, dec_gain)
    table_load = load(CHUNKS + 5, table_hbm, table)

    def wo_load(i):
        chip, core = lax.div(i, CORES), lax.rem(i, CORES)
        src = wo_hbm.at[:, pl.ds(pl.multiple_of(i * cols, cols), cols)]
        dst = wo.at[core, :, pl.ds(pl.multiple_of(chip * cols, cols), cols)]
        return load(CHUNKS + 6, src, dst)

    inward = [k // 2 if k % 2 == 0 else CHUNKS - 1 - k // 2 for k in range(CHUNKS)]
    enc_gain_load.start()
    for k in inward:
        states_load(k).start()

    barrier = pltpu.get_barrier_semaphore()
    above, below = g + 1, g - 1

    def if_above(do):
        pl.when(g < groups - 1)(do)

    def if_below(do):
        pl.when(g > 0)(do)

    pl.semaphore_signal(barrier, inc=1, device_id={"seq": left})
    pl.semaphore_signal(barrier, inc=1, device_id={"seq": right})

    @pl.when(c == 1)
    def _():
        pl.semaphore_signal(barrier, inc=1, device_id={"seq": partner})

    if_below(lambda: pl.semaphore_signal(barrier, inc=1, device_id={"qset": below}))

    def part(slot, chunk):
        return rows.at[slot, pl.ds(pl.multiple_of(chunk * piece, piece), piece), :]

    def right_copy(m, behind):
        at = part(seq_at(x - lax.div(m, CHUNKS) - behind, c), lax.rem(m, CHUNKS))
        return pltpu.make_async_remote_copy(at, at, rs, rr.at[m], device_id={"seq": right})

    def left_copy(m, behind):
        at = part(seq_at(x + lax.div(m, CHUNKS) + behind, c), CHUNKS - 1 - lax.rem(m, CHUNKS))
        return pltpu.make_async_remote_copy(at, at, rs, lr.at[m], device_id={"seq": left})

    def die_copy(k, slot, chunk):
        at = part(slot, chunk)
        return pltpu.make_async_remote_copy(at, at, ds, dr.at[k], device_id={"seq": partner})

    def from_left(m, core):
        return seq_at(x - lax.div(m, CHUNKS) - 1, core), lax.rem(m, CHUNKS)

    def from_right(m, core):
        return seq_at(x + lax.div(m, CHUNKS) + 1, core), CHUNKS - 1 - lax.rem(m, CHUNKS)

    enc_gain_load.wait()
    gains[0:1, :] = enc_gain[...].astype(F32).reshape(1, width)
    done, sent_right, sent_left = set(), 0, 0
    for k in inward:
        states_load(k).wait()
        normalise(raw, gains.at[0:1, :], rows.at[me], k * piece, piece)
        if not done:
            pl.semaphore_wait(barrier, 2 + (1 - c) + 1 - lax.div(g + 1, groups))
        done.add(k)
        while sent_right in done:
            right_copy(jnp.int32(sent_right), 0).start()
            sent_right += 1
        while CHUNKS - 1 - sent_left in done:
            left_copy(jnp.int32(sent_left), 0).start()
            sent_left += 1
    for one in (wkv_load, dec_load, dec_gain_load, wq_load, table_load):
        one.start()
    lax.fori_loop(0, shards, lambda i, n: (wo_load(i).start(), n)[1], 0)

    @pl.when(c == 0)
    def _():
        lax.fori_loop(0, CHUNKS, lambda m, n: (die_copy(m, me, m).start(), n)[1], 0)

    @pl.when(g == 0)
    def _():
        pl.semaphore_signal(rising, inc=1, device_id={"qset": above})

    own_q = qbuf.at[pl.ds(g * mine, mine)]

    def own_queries():
        dec_load.wait()
        dec_gain_load.wait()
        gains[8:9, :] = dec_gain[...].astype(F32).reshape(1, width)
        normalise(dec_raw, gains.at[8:9, :], dec_rows, 0, dec_raw.shape[0])
        wq_load.wait()
        queries = jnp.dot(dec_rows[...], wq[...], preferred_element_type=F32).astype(BF16)
        own_q[...] = queries.reshape(mine, tokens, cols)

    def query_copy(i):
        to = lax.rem(g + i, groups)
        return pltpu.make_async_remote_copy(
            own_q, own_q, qs, qr, device_id={"qset": to}
        )

    def query_all():
        at = qbuf.at[pl.ds(0, questions - mine)]
        return pltpu.make_async_remote_copy(at, at, qs, qr, device_id={"qset": above})

    passages = table.shape[1]

    def find(q, n):
        def look(p, found):
            at0, at1, count = found
            hit = table[g, p] == q
            at0 = jnp.where(hit & (count == 0), p, at0)
            at1 = jnp.where(hit & (count == 1), p, at1)
            return at0, at1, count + hit.astype(jnp.int32)

        zero = jnp.int32(0)
        at0, at1, count = lax.fori_loop(0, passages, look, (zero, zero, zero))
        first[q], second[q], hits[q] = at0, at1, count
        return n

    lane = lax.broadcasted_iota(jnp.int32, (1, LANES), 1)
    low = lane < HD

    def key_values(slots):
        together = jnp.concatenate([part(*s)[...] for s in slots], axis=0)
        result = jnp.dot(together, wkv[...], preferred_element_type=F32).astype(BF16)
        for i, (slot, chunk) in enumerate(slots):
            at = pl.ds(pl.multiple_of(chunk * piece, piece), piece)
            kv[slot, at, :] = result[i * piece : (i + 1) * piece]

    def attend(slot):
        asked = qbuf[table[g, slot]]
        for j in range(cols // LANES):
            at = slice(j * LANES, (j + 1) * LANES)
            pair = asked[:, at]
            none = jnp.zeros_like(pair)
            stacked = jnp.concatenate([jnp.where(low, pair, none), jnp.where(low, none, pair)], axis=0)
            keys = kv[slot, :, at]
            values = kv[slot, :, cols + j * LANES : cols + (j + 1) * LANES]
            scores = lax.dot_general(
                stacked, keys, (((1,), (1,)), ((), ())), preferred_element_type=F32
            )
            top = jnp.max(scores, axis=-1, keepdims=True)
            weights = jnp.exp(scores - top)
            summed = jnp.sum(weights, axis=-1, keepdims=True)
            product = jnp.dot(weights.astype(BF16), values, preferred_element_type=F32)
            num[slot, :, at] = jnp.where(low, product[:tokens], product[tokens:])
            peak[slot, :, at] = jnp.where(low, top[:tokens], top[tokens:])
            total[slot, :, at] = jnp.where(low, summed[:tokens], summed[tokens:])

    wkv_load.wait()
    block = 64

    def unzip(i, n):
        at = pl.ds(pl.multiple_of(i * block, block), block)
        wkv[at, :cols] = wkv_in[at, 0, :]
        wkv[at, cols:] = wkv_in[at, 1, :]
        return n

    lax.fori_loop(0, width // block, unzip, 0)

    def whole_values(slot):
        result = jnp.dot(rows[slot], wkv[...], preferred_element_type=F32)
        kv[slot] = result.astype(BF16)

    def partner_part(m):
        die_copy(CHUNKS + m, *from_left(m, other)).wait_recv()
        die_copy(CHUNKS + messages + m, *from_right(m, other)).wait_recv()
        key_values([from_left(m, other), from_right(m, other)])

    def die_right(m):
        die_copy(CHUNKS + m, *from_left(m, c)).start()

    def die_left(m):
        die_copy(CHUNKS + messages + m, *from_right(m, c)).start()

    hold = 2
    catch = messages - 4
    partner_at = min(LAG, catch)

    def part_done(m):
        return m + LAG if m + LAG < catch else max(catch, m + 1)

    def step(m, n):
        @pl.when(m > catch)
        def _():
            partner_part(m - 1)

        right_copy(m, 1).wait_recv()

        @pl.when(m + CHUNKS < messages)
        def _():
            right_copy(m + CHUNKS, 0).start()

        @pl.when((1 - c) * messages + m > hold)
        def _():
            die_right(m)

        left_copy(m, 1).wait_recv()

        @pl.when(m + CHUNKS < messages)
        def _():
            left_copy(m + CHUNKS, 0).start()

        @pl.when((1 - c) * messages + m > hold)
        def _():
            die_left(m)

        @pl.when(m == 0)
        def _():
            whole_values(me)

        key_values([from_left(m, c), from_right(m, c)])

        @pl.when(m == 1)
        def _():
            own_queries()
            if_below(lambda: pl.semaphore_wait(rising, 1))

            @pl.when(g > 0)
            def _():
                if_above(
                    lambda: pl.semaphore_signal(rising, inc=1, device_id={"qset": above})
                )

        @pl.when(m == hold)
        def _():
            @pl.when(c == 1)
            def _():
                die_copy(0, partner, 0).wait_recv()
                lax.fori_loop(0, CHUNKS, lambda k, t: (die_copy(k, me, k).start(), t)[1], 0)

                def late(k, t):
                    die_right(k)
                    die_left(k)
                    return t

                lax.fori_loop(0, hold + 1, late, 0)

            if_above(lambda: pl.semaphore_wait(falling, 1))
            if_below(lambda: pl.semaphore_signal(falling, inc=1, device_id={"qset": below}))
            lax.fori_loop(1, groups, lambda i, k: (query_copy(i).start(), k)[1], 0)

        @pl.when(m == hold + 1)
        def _():
            table_load.wait()
            lax.fori_loop(0, questions, find, 0)

        @pl.when(m == partner_at)
        def _():
            @pl.when(c == 0)
            def _():
                die_copy(0, partner, 0).wait_recv()

            lax.fori_loop(
                1, CHUNKS, lambda k, t: (die_copy(k, partner, k).wait_recv(), t)[1], 0
            )
            whole_values(partner)

        if catch > LAG:

            @pl.when(m >= LAG)
            def _():
                @pl.when(m < catch)
                def _():
                    partner_part(m - LAG)

        @pl.when(m == catch)
        def _():
            lax.fori_loop(
                max(0, catch - LAG), catch, lambda k, t: (partner_part(k), t)[1], 0
            )

        @pl.when(m == messages // 2)
        def _():
            query_all().wait_recv()
            lax.fori_loop(0, CORES, lambda i, k: (attend(seq_at(x, i)), k)[1], 0)

        for far in range(1, chips // 2):

            @pl.when(m == max(part_done(far * CHUNKS - 1), messages // 2 + far))
            def _():
                def both(i, k):
                    attend(seq_at(x - far, i))
                    attend(seq_at(x + far, i))
                    return k

                lax.fori_loop(0, CORES, both, 0)

        return n

    lax.fori_loop(0, messages, step, 0)
    attend(seq_at(x + chips // 2, c))
    partner_part(messages - 1)
    attend(seq_at(x + chips // 2, other))

    pairs = cols // LANES

    def alternate(k, n):
        reach = lax.div(k + 1, 2)
        return n // 2 - reach + 2 * reach * lax.rem(k, 2)

    short = tokens // PARTS

    def out_copy(own, cut, i):
        to = lax.rem(g + i, groups)
        here = pl.ds(cut * short, short)
        return pltpu.make_async_remote_copy(
            osend.at[own, to, here],
            orecv.at[own, g, here],
            os_, or_.at[own * PARTS + cut], device_id={"qset": to},
        )

    def out_all(own, cut):
        at = orecv.at[own, pl.ds(0, groups - 1), pl.ds(cut * short, short)]
        return pltpu.make_async_remote_copy(
            at, at, os_, or_.at[own * PARTS + cut], device_id={"qset": above}
        )

    def lse_copy(own, i):
        to = lax.rem(g + i, groups)
        return pltpu.make_async_remote_copy(
            lsend.at[own, to],
            lrecv.at[own, g],
            ss, sr.at[own], device_id={"qset": to},
        )

    def lse_all(own):
        at = lrecv.at[own, pl.ds(0, groups - 1)]
        return pltpu.make_async_remote_copy(at, at, ss, sr.at[own], device_id={"qset": above})

    def merge(own, to, mix_at, lse_at):
        q = to * mine + own
        at0, at1, count = first[q], second[q], hits[q]
        lses = []
        for j in range(pairs):
            at = slice(j * LANES, (j + 1) * LANES)
            top0 = jnp.where(count >= 1, peak[at0, :, at], DEAD)
            top1 = jnp.where(count >= 2, peak[at1, :, at], DEAD)
            top = jnp.maximum(top0, top1)
            scale0 = jnp.where(count >= 1, jnp.exp(top0 - top), 0.0)
            scale1 = jnp.where(count >= 2, jnp.exp(top1 - top), 0.0)
            mass = scale0 * total[at0, :, at] + scale1 * total[at1, :, at]
            mass = jnp.where(count >= 1, mass, 1.0)
            mix = (scale0 * num[at0, :, at] + scale1 * num[at1, :, at]) / mass
            mix_at[:, at] = mix.astype(BF16)
            lse = jnp.where(count >= 1, top + jnp.log(mass), DEAD)
            turned = jnp.transpose(lse)
            lses += [turned[:1], turned[HD : HD + 1]]
        lse_at[...] = jnp.concatenate(lses, axis=1)

    def merge_and_send(own):
        def one(k, n):
            i = alternate(k, groups)
            to = lax.rem(g + i, groups)
            merge(own, to, osend.at[own, to], lsend.at[own, to])
            lse_copy(own, i).start()
            out_copy(own, 0, i).start()
            return n

        lax.fori_loop(0, groups - 1, one, 0)
        for cut in range(1, PARTS):

            def rest(k, n):
                out_copy(own, cut, alternate(k, groups)).start()
                return n

            lax.fori_loop(0, groups - 1, rest, 0)

    for own in range(mine):
        merge_and_send(own)
    for own in range(mine):
        merge(own, g, orecv.at[own, g], lrecv.at[own, g])
    pltpu.make_async_copy(wo, wo, load_sem.at[CHUNKS + 6]).wait()

    def pair_copy(piece):
        return pltpu.make_async_remote_copy(
            psend.at[piece], precv.at[piece], ps, pr.at[piece],
            device_id={"seq": partner},
        )

    def chip_part(chip):
        return pl.ds(pl.multiple_of(chip * cols, cols), cols)

    def sum_copy(piece, i):
        to = lax.rem(x + i, chips)
        return pltpu.make_async_remote_copy(
            xsend.at[piece, :, chip_part(to)], xrecv.at[piece, i],
            xs, xr.at[piece], device_id={"seq": seq_at(to, c)},
        )

    def sum_all(piece):
        at = xrecv.at[piece, pl.ds(1, chips - 1)]
        return pltpu.make_async_remote_copy(at, at, xs, xr.at[piece], device_id={"seq": right})

    def share_of(own):
        lse_all(own).wait_recv()
        every = jnp.concatenate([lrecv[own, k] for k in range(groups)], axis=0)
        top = jnp.max(every, axis=0, keepdims=True)
        share = jnp.exp(every - top)
        share = share / jnp.sum(share, axis=0, keepdims=True)
        for j in range(pairs):
            shares[j] = jnp.transpose(share[:, j * LANES : (j + 1) * LANES])

    def project(own, cut):
        piece = own * PARTS + cut
        here = slice(cut * short, (cut + 1) * short)
        odd_here = slice(HD + cut * short, HD + (cut + 1) * short)
        out_all(own, cut).wait_recv()
        for j in range(pairs):
            at = slice(j * LANES, (j + 1) * LANES)
            mixed = jnp.zeros((short, LANES), F32)
            for source in range(groups):
                at_source = slice(source, source + 1)
                scale = jnp.where(
                    low, shares[j, here, at_source], shares[j, odd_here, at_source]
                )
                mixed = mixed + scale * orecv[own, source, here, at].astype(F32)
            att[:, at] = mixed.astype(BF16)

        psend[piece] = jnp.dot(att[...], wo[other], preferred_element_type=F32).astype(BF16)
        pair_copy(piece).start()
        half[...] = jnp.dot(att[...], wo[c], preferred_element_type=F32)
        pair_copy(piece).wait_recv()

        def add(i):
            at = chip_part(lax.rem(x + i, chips))
            xsend[piece, :, at] = (half[:, at] + precv[piece, :, at].astype(F32)).astype(BF16)

        def to_chip(k, n):
            i = alternate(k, chips)
            add(i)
            sum_copy(piece, i).start()
            return n

        lax.fori_loop(0, chips - 1, to_chip, 0)
        add(0)

    for own in range(mine):
        share_of(own)
        for cut in range(PARTS):
            project(own, cut)

    def sent(all_of, sem):
        pltpu.make_async_remote_copy(
            all_of, all_of, sem, qr, device_id={"seq": right}
        ).wait_send()

    sent(rows.at[pl.ds(0, chips - 1)], rs)
    sent(rows.at[pl.ds(0, chips)], ds)
    sent(qbuf.at[pl.ds(0, questions - mine)], qs)
    sent(osend.at[:, pl.ds(0, groups - 1)], os_)
    sent(lsend.at[:, pl.ds(0, groups - 1)], ss)
    feature = pl.ds(pl.multiple_of(me * cols, cols), cols)
    for piece in range(mine * PARTS):
        here = slice(piece * short, (piece + 1) * short)
        result = dec_raw[here, feature].astype(F32) + xsend[piece, :, chip_part(x)].astype(F32)
        sum_all(piece).wait_recv()
        for i in range(1, chips):
            result = result + xrecv[piece, i].astype(F32)
        own, cut = divmod(piece, PARTS)
        out_ref[own, cut * short : (cut + 1) * short, :] = result.astype(BF16)
    sent(psend, ps)
    sent(xrecv.at[:, pl.ds(0, chips - 1)], xs)


def body(
    states, enc_gain, dec_states, dec_gain, query_weight, key_value_weight, out_weight, question_of
):
    shards, groups = lax.axis_size("seq"), lax.axis_size("qset")
    chips = shards // CORES
    plen, width = states.shape[2:]
    mine, tokens = dec_states.shape[:2]
    cols = query_weight.shape[1]
    questions = mine * groups
    messages = (chips - 1) * CHUNKS // 2
    pieces, short = mine * PARTS, tokens // PARTS
    hbm = pl.BlockSpec(memory_space=pl.ANY)
    vmem = pl.BlockSpec(memory_space=pltpu.VMEM)
    dma = lambda n: pltpu.SemaphoreType.DMA((n,))
    one = pltpu.SemaphoreType.DMA
    return pl.pallas_call(
        kernel,
        out_shape=jax.ShapeDtypeStruct((mine, tokens, cols), BF16),
        in_specs=[hbm] * 8,
        out_specs=vmem,
        scratch_shapes=[
            pltpu.VMEM((plen, width), BF16),
            pltpu.VMEM((mine * tokens, width), BF16),
            pltpu.VMEM((mine * tokens, width), BF16),
            pltpu.VMEM((shards, plen, width), BF16),
            pltpu.VMEM((width, cols), BF16),
            pltpu.VMEM((width, 2, cols), BF16),
            pltpu.VMEM((width, 2 * cols), BF16),
            pltpu.VMEM((CORES, cols, chips * cols), BF16),
            pltpu.VMEM((shards, plen, 2 * cols), BF16),
            pltpu.VMEM((questions, tokens, cols), BF16),
            pltpu.VMEM((shards, tokens, cols), F32),
            pltpu.VMEM((shards, tokens, cols), F32),
            pltpu.VMEM((shards, tokens, cols), F32),
            pltpu.VMEM((mine, groups, tokens, cols), BF16),
            pltpu.VMEM((mine, groups, tokens, cols), BF16),
            pltpu.VMEM((mine, groups, 1, tokens * cols // HD), F32),
            pltpu.VMEM((mine, groups, 1, tokens * cols // HD), F32),
            pltpu.VMEM((cols // LANES, LANES, groups), F32),
            pltpu.VMEM((short, cols), BF16),
            pltpu.VMEM((short, chips * cols), F32),
            pltpu.VMEM((pieces, short, chips * cols), BF16),
            pltpu.VMEM((pieces, short, chips * cols), BF16),
            pltpu.VMEM((pieces, short, chips * cols), BF16),
            pltpu.VMEM((pieces, chips, short, cols), BF16),
            pltpu.VMEM((16, width), F32),
            pltpu.VMEM((width,), BF16),
            pltpu.VMEM((width,), BF16),
            pltpu.SMEM(question_of.shape[:2], jnp.int32),
            pltpu.SMEM((questions,), jnp.int32),
            pltpu.SMEM((questions,), jnp.int32),
            pltpu.SMEM((questions,), jnp.int32),
            dma(CHUNKS + 7),
            one, dma(messages), dma(messages),
            one, dma(CHUNKS * chips),
            one, one, one, dma(pieces), one, dma(mine),
            one, dma(pieces), one, dma(pieces),
            pltpu.SemaphoreType.REGULAR, pltpu.SemaphoreType.REGULAR,
        ],
        compiler_params=pltpu.CompilerParams(
            collective_id=0, has_side_effects=True, vmem_limit_bytes=60 * 1024 * 1024
        ),
        name="reader_step",
    )(
        question_of[:, :, 0],
        states.reshape(plen, width),
        enc_gain,
        dec_states.reshape(mine * tokens, width),
        dec_gain,
        query_weight,
        key_value_weight,
        out_weight,
    )


def solution(mesh):
    return jax.shard_map(
        body,
        mesh=mesh,
        in_specs=(
            P(("groups", "qset"), "seq", None, None),
            P(),
            P(("groups", "qset"), None, None),
            P(),
            P(None, "seq"),
            P(None, None, "seq"),
            P("seq", None),
            P("groups", None, None),
        ),
        out_specs=P(("groups", "qset"), None, "seq"),
        check_vma=False,
    )
```

```python
import functools

import jax
import jax.numpy as jnp
from jax import lax
from jax.experimental import pallas as pl
from jax.experimental.pallas import tpu as pltpu
from jax.sharding import PartitionSpec as P

HD = 64
EPSILON = 1e-06
DEAD = -1e30
LANES = 128
CORES = 2
CHUNKS = 4
LAG = 4
F32 = jnp.float32
BF16 = jnp.bfloat16


def pieces_of(mine, tokens):
    half, quarter = tokens // 2, tokens // 4
    pieces = [(own, start, half) for own in range(mine) for start in (0, half)]
    return pieces[:-1] + [(mine - 1, half, quarter), (mine - 1, half + quarter, quarter)]


def normalise(src, gain, dst_at, start, rows_here):
    step = 16

    def one(i, carry):
        at = pl.ds(pl.multiple_of(start + i * step, step), step)
        rows = src[at, :].astype(F32)
        mean_square = jnp.mean(rows * rows, axis=-1, keepdims=True)
        dst_at[at, :] = (rows * lax.rsqrt(mean_square + EPSILON) * gain[...]).astype(BF16)
        return carry

    lax.fori_loop(0, rows_here // step, one, 0)


def kernel(
    table_hbm, states_hbm, enc_gain_hbm, dec_hbm, dec_gain_hbm, wq_hbm, wkv_hbm, wo_hbm, out_hbm,
    raw, dec_raw, dec_rows, rows, wq, wkv_in, wkv, wo, kv, qbuf, num, peak, total,
    osend, orecv, lsend, lrecv, shares, att, half, psend, precv, xsend, xrecv, out_here, gains,
    enc_gain, dec_gain, table, first, second, hits,
    load_sem, rs, rr, lr, ds, dr, qs, qr, os_, or_, ss, sr, ps, pr, xs, xr, rising, falling,
):
    shards, groups = lax.axis_size("seq"), lax.axis_size("qset")
    chips = shards // CORES
    me, g = lax.axis_index("seq"), lax.axis_index("qset")
    x, c = lax.div(me, CORES), lax.rem(me, CORES)
    plen, width = raw.shape
    questions, tokens, cols = qbuf.shape
    mine = questions // groups
    piece = plen // CHUNKS
    messages = (chips - 1) * CHUNKS // 2

    def seq_at(chip, core):
        return lax.rem(chip + 2 * chips, chips) * CORES + core

    right, left = seq_at(x + 1, c), seq_at(x - 1, c)
    other = 1 - c
    partner = seq_at(x, other)

    def load(i, src, dst):
        return pltpu.make_async_copy(src, dst, load_sem.at[i])

    def states_load(k):
        at = pl.ds(k * piece, piece)
        return load(k, states_hbm.at[at], raw.at[at])

    enc_gain_load = load(CHUNKS, enc_gain_hbm, enc_gain)
    dec_load = load(CHUNKS + 1, dec_hbm, dec_raw)
    wq_load = load(CHUNKS + 2, wq_hbm, wq)
    wkv_load = load(CHUNKS + 3, wkv_hbm, wkv_in)
    dec_gain_load = load(CHUNKS + 4, dec_gain_hbm, dec_gain)
    table_load = load(CHUNKS + 5, table_hbm, table)

    def wo_load(i):
        chip, core = lax.div(i, CORES), lax.rem(i, CORES)
        src = wo_hbm.at[:, pl.ds(pl.multiple_of(i * cols, cols), cols)]
        dst = wo.at[core, :, pl.ds(pl.multiple_of(chip * cols, cols), cols)]
        return load(CHUNKS + 6, src, dst)

    inward = [k // 2 if k % 2 == 0 else CHUNKS - 1 - k // 2 for k in range(CHUNKS)]
    enc_gain_load.start()
    for k in inward:
        states_load(k).start()

    barrier = pltpu.get_barrier_semaphore()
    above, below = g + 1, g - 1

    def if_above(do):
        pl.when(g < groups - 1)(do)

    def if_below(do):
        pl.when(g > 0)(do)

    pl.semaphore_signal(barrier, inc=1, device_id={"seq": left})
    pl.semaphore_signal(barrier, inc=1, device_id={"seq": right})

    @pl.when(c == 1)
    def _():
        pl.semaphore_signal(barrier, inc=1, device_id={"seq": partner})

    if_below(lambda: pl.semaphore_signal(barrier, inc=1, device_id={"qset": below}))

    def part(slot, chunk):
        return rows.at[slot, pl.ds(pl.multiple_of(chunk * piece, piece), piece), :]

    def right_copy(m, behind):
        at = part(seq_at(x - lax.div(m, CHUNKS) - behind, c), lax.rem(m, CHUNKS))
        return pltpu.make_async_remote_copy(at, at, rs, rr.at[m], device_id={"seq": right})

    def left_copy(m, behind):
        at = part(seq_at(x + lax.div(m, CHUNKS) + behind, c), CHUNKS - 1 - lax.rem(m, CHUNKS))
        return pltpu.make_async_remote_copy(at, at, rs, lr.at[m], device_id={"seq": left})

    def die_copy(k, slot, chunk):
        at = part(slot, chunk)
        return pltpu.make_async_remote_copy(at, at, ds, dr.at[k], device_id={"seq": partner})

    def from_left(m, core):
        return seq_at(x - lax.div(m, CHUNKS) - 1, core), lax.rem(m, CHUNKS)

    def from_right(m, core):
        return seq_at(x + lax.div(m, CHUNKS) + 1, core), CHUNKS - 1 - lax.rem(m, CHUNKS)

    enc_gain_load.wait()
    gains[0:1, :] = enc_gain[...].astype(F32).reshape(1, width)
    done, sent_right, sent_left = set(), 0, 0
    for k in inward:
        states_load(k).wait()
        normalise(raw, gains.at[0:1, :], rows.at[me], k * piece, piece)
        if not done:
            pl.semaphore_wait(barrier, 2 + (1 - c) + 1 - lax.div(g + 1, groups))
        done.add(k)
        while sent_right in done:
            right_copy(jnp.int32(sent_right), 0).start()
            sent_right += 1
        while CHUNKS - 1 - sent_left in done:
            left_copy(jnp.int32(sent_left), 0).start()
            sent_left += 1
    for one in (wkv_load, dec_load, dec_gain_load, wq_load, table_load):
        one.start()
    lax.fori_loop(0, shards, lambda i, n: (wo_load(i).start(), n)[1], 0)

    @pl.when(c == 0)
    def _():
        lax.fori_loop(0, CHUNKS, lambda m, n: (die_copy(m, me, m).start(), n)[1], 0)

    @pl.when(g == 0)
    def _():
        pl.semaphore_signal(rising, inc=1, device_id={"qset": above})

    own_q = qbuf.at[pl.ds(g * mine, mine)]

    def own_queries():
        dec_load.wait()
        dec_gain_load.wait()
        gains[8:9, :] = dec_gain[...].astype(F32).reshape(1, width)
        normalise(dec_raw, gains.at[8:9, :], dec_rows, 0, dec_raw.shape[0])
        wq_load.wait()
        queries = jnp.dot(dec_rows[...], wq[...], preferred_element_type=F32).astype(BF16)
        own_q[...] = queries.reshape(mine, tokens, cols)

    def query_copy(i):
        to = lax.rem(g + i, groups)
        return pltpu.make_async_remote_copy(
            own_q, own_q, qs, qr, device_id={"qset": to}
        )

    def query_all():
        at = qbuf.at[pl.ds(0, questions - mine)]
        return pltpu.make_async_remote_copy(at, at, qs, qr, device_id={"qset": above})

    passages = table.shape[1]

    def find(q, n):
        def look(p, found):
            at0, at1, count = found
            hit = table[g, p] == q
            at0 = jnp.where(hit & (count == 0), p, at0)
            at1 = jnp.where(hit & (count == 1), p, at1)
            return at0, at1, count + hit.astype(jnp.int32)

        zero = jnp.int32(0)
        at0, at1, count = lax.fori_loop(0, passages, look, (zero, zero, zero))
        first[q], second[q], hits[q] = at0, at1, count
        return n

    lane = lax.broadcasted_iota(jnp.int32, (1, LANES), 1)
    low = lane < HD

    def key_values(slots):
        together = jnp.concatenate([part(*s)[...] for s in slots], axis=0)
        result = jnp.dot(together, wkv[...], preferred_element_type=F32).astype(BF16)
        for i, (slot, chunk) in enumerate(slots):
            at = pl.ds(pl.multiple_of(chunk * piece, piece), piece)
            kv[slot, at, :] = result[i * piece : (i + 1) * piece]

    def attend(slot):
        asked = qbuf[table[g, slot]]
        for j in range(cols // LANES):
            at = slice(j * LANES, (j + 1) * LANES)
            pair = asked[:, at]
            none = jnp.zeros_like(pair)
            stacked = jnp.concatenate([jnp.where(low, pair, none), jnp.where(low, none, pair)], axis=0)
            keys = kv[slot, :, at]
            values = kv[slot, :, cols + j * LANES : cols + (j + 1) * LANES]
            scores = lax.dot_general(
                stacked, keys, (((1,), (1,)), ((), ())), preferred_element_type=F32
            )
            top = jnp.max(scores, axis=-1, keepdims=True)
            weights = jnp.exp(scores - top)
            summed = jnp.sum(weights, axis=-1, keepdims=True)
            product = jnp.dot(weights.astype(BF16), values, preferred_element_type=F32)
            num[slot, :, at] = jnp.where(low, product[:tokens], product[tokens:])
            peak[slot, :, at] = jnp.where(low, top[:tokens], top[tokens:])
            total[slot, :, at] = jnp.where(low, summed[:tokens], summed[tokens:])

    wkv_load.wait()
    block = 64

    def unzip(i, n):
        at = pl.ds(pl.multiple_of(i * block, block), block)
        wkv[at, :cols] = wkv_in[at, 0, :]
        wkv[at, cols:] = wkv_in[at, 1, :]
        return n

    lax.fori_loop(0, width // block, unzip, 0)

    def whole_values(slot):
        result = jnp.dot(rows[slot], wkv[...], preferred_element_type=F32)
        kv[slot] = result.astype(BF16)

    def partner_part(m):
        die_copy(CHUNKS + m, *from_left(m, other)).wait_recv()
        die_copy(CHUNKS + messages + m, *from_right(m, other)).wait_recv()
        key_values([from_left(m, other), from_right(m, other)])

    def die_right(m):
        die_copy(CHUNKS + m, *from_left(m, c)).start()

    def die_left(m):
        die_copy(CHUNKS + messages + m, *from_right(m, c)).start()

    hold = 2
    catch = messages - 4
    partner_at = min(LAG, catch)

    def part_done(m):
        return m + LAG if m + LAG < catch else max(catch, m + 1)

    def step(m, n):
        @pl.when(m > catch)
        def _():
            partner_part(m - 1)

        right_copy(m, 1).wait_recv()

        @pl.when(m + CHUNKS < messages)
        def _():
            right_copy(m + CHUNKS, 0).start()

        @pl.when((1 - c) * messages + m > hold)
        def _():
            die_right(m)

        left_copy(m, 1).wait_recv()

        @pl.when(m + CHUNKS < messages)
        def _():
            left_copy(m + CHUNKS, 0).start()

        @pl.when((1 - c) * messages + m > hold)
        def _():
            die_left(m)

        @pl.when(m == 0)
        def _():
            whole_values(me)

        key_values([from_left(m, c), from_right(m, c)])

        @pl.when(m == 1)
        def _():
            own_queries()
            if_below(lambda: pl.semaphore_wait(rising, 1))

            @pl.when(g > 0)
            def _():
                if_above(
                    lambda: pl.semaphore_signal(rising, inc=1, device_id={"qset": above})
                )

        @pl.when(m == hold)
        def _():
            @pl.when(c == 1)
            def _():
                die_copy(0, partner, 0).wait_recv()
                lax.fori_loop(0, CHUNKS, lambda k, t: (die_copy(k, me, k).start(), t)[1], 0)

                def late(k, t):
                    die_right(k)
                    die_left(k)
                    return t

                lax.fori_loop(0, hold + 1, late, 0)

            if_above(lambda: pl.semaphore_wait(falling, 1))
            if_below(lambda: pl.semaphore_signal(falling, inc=1, device_id={"qset": below}))
            lax.fori_loop(1, groups, lambda i, k: (query_copy(i).start(), k)[1], 0)

        @pl.when(m == hold + 1)
        def _():
            table_load.wait()
            lax.fori_loop(0, questions, find, 0)

        @pl.when(m == partner_at)
        def _():
            @pl.when(c == 0)
            def _():
                die_copy(0, partner, 0).wait_recv()

            lax.fori_loop(
                1, CHUNKS, lambda k, t: (die_copy(k, partner, k).wait_recv(), t)[1], 0
            )
            whole_values(partner)

        if catch > LAG:

            @pl.when(m >= LAG)
            def _():
                @pl.when(m < catch)
                def _():
                    partner_part(m - LAG)

        @pl.when(m == catch)
        def _():
            lax.fori_loop(
                max(0, catch - LAG), catch, lambda k, t: (partner_part(k), t)[1], 0
            )

        @pl.when(m == messages // 2)
        def _():
            query_all().wait_recv()
            lax.fori_loop(0, CORES, lambda i, k: (attend(seq_at(x, i)), k)[1], 0)

        for far in range(1, chips // 2):

            @pl.when(m == max(part_done(far * CHUNKS - 1), messages // 2 + far))
            def _():
                def both(i, k):
                    attend(seq_at(x - far, i))
                    attend(seq_at(x + far, i))
                    return k

                lax.fori_loop(0, CORES, both, 0)

        return n

    lax.fori_loop(0, messages, step, 0)
    attend(seq_at(x + chips // 2, c))
    partner_part(messages - 1)
    attend(seq_at(x + chips // 2, other))

    pairs = cols // LANES

    def alternate(k, n):
        reach = lax.div(k + 1, 2)
        return n // 2 - reach + 2 * reach * lax.rem(k, 2)

    pieces = pieces_of(mine, tokens)

    def out_copy(p, i):
        own, start, size = pieces[p]
        to = lax.rem(g + i, groups)
        here = pl.ds(start, size)
        return pltpu.make_async_remote_copy(
            osend.at[own, to, here],
            orecv.at[own, g, here],
            os_, or_.at[p], device_id={"qset": to},
        )

    def out_all(p):
        own, start, size = pieces[p]
        at = orecv.at[own, pl.ds(0, groups - 1), pl.ds(start, size)]
        return pltpu.make_async_remote_copy(at, at, os_, or_.at[p], device_id={"qset": above})

    def lse_copy(own, i):
        to = lax.rem(g + i, groups)
        return pltpu.make_async_remote_copy(
            lsend.at[own, to],
            lrecv.at[own, g],
            ss, sr.at[own], device_id={"qset": to},
        )

    def lse_all(own):
        at = lrecv.at[own, pl.ds(0, groups - 1)]
        return pltpu.make_async_remote_copy(at, at, ss, sr.at[own], device_id={"qset": above})

    def merge(own, to, mix_at, lse_at):
        q = to * mine + own
        at0, at1, count = first[q], second[q], hits[q]
        lses = []
        for j in range(pairs):
            at = slice(j * LANES, (j + 1) * LANES)
            top0 = jnp.where(count >= 1, peak[at0, :, at], DEAD)
            top1 = jnp.where(count >= 2, peak[at1, :, at], DEAD)
            top = jnp.maximum(top0, top1)
            scale0 = jnp.where(count >= 1, jnp.exp(top0 - top), 0.0)
            scale1 = jnp.where(count >= 2, jnp.exp(top1 - top), 0.0)
            mass = scale0 * total[at0, :, at] + scale1 * total[at1, :, at]
            mass = jnp.where(count >= 1, mass, 1.0)
            mix = (scale0 * num[at0, :, at] + scale1 * num[at1, :, at]) / mass
            mix_at[:, at] = mix.astype(BF16)
            lse = jnp.where(count >= 1, top + jnp.log(mass), DEAD)
            turned = jnp.transpose(lse)
            lses += [turned[:1], turned[HD : HD + 1]]
        lse_at[...] = jnp.concatenate(lses, axis=1)

    def merge_and_send(own):
        lead, *others = [p for p in range(len(pieces)) if pieces[p][0] == own]

        def one(k, n):
            i = alternate(k, groups)
            to = lax.rem(g + i, groups)
            merge(own, to, osend.at[own, to], lsend.at[own, to])
            lse_copy(own, i).start()
            out_copy(lead, i).start()
            return n

        lax.fori_loop(0, groups - 1, one, 0)
        for p in others:

            def rest(k, n):
                out_copy(p, alternate(k, groups)).start()
                return n

            lax.fori_loop(0, groups - 1, rest, 0)

    for own in range(mine):
        merge_and_send(own)
    for own in range(mine):
        merge(own, g, orecv.at[own, g], lrecv.at[own, g])
    pltpu.make_async_copy(wo, wo, load_sem.at[CHUNKS + 6]).wait()

    def rows_of(p):
        own, start, size = pieces[p]
        return pl.ds(own * tokens + start, size)

    def pair_copy(p):
        at = rows_of(p)
        return pltpu.make_async_remote_copy(
            psend.at[at], precv.at[at], ps, pr.at[p], device_id={"seq": partner}
        )

    def chip_part(chip):
        return pl.ds(pl.multiple_of(chip * cols, cols), cols)

    def sum_copy(p, i):
        to = lax.rem(x + i, chips)
        return pltpu.make_async_remote_copy(
            xsend.at[rows_of(p), chip_part(to)], xrecv.at[i, rows_of(p)],
            xs, xr.at[p], device_id={"seq": seq_at(to, c)},
        )

    def sum_all(p):
        at = xrecv.at[pl.ds(1, chips - 1), rows_of(p)]
        return pltpu.make_async_remote_copy(at, at, xs, xr.at[p], device_id={"seq": right})

    def share_of(own):
        lse_all(own).wait_recv()
        every = jnp.concatenate([lrecv[own, k] for k in range(groups)], axis=0)
        top = jnp.max(every, axis=0, keepdims=True)
        share = jnp.exp(every - top)
        share = share / jnp.sum(share, axis=0, keepdims=True)
        for j in range(pairs):
            shares[j] = jnp.transpose(share[:, j * LANES : (j + 1) * LANES])

    def project(p):
        own, start, size = pieces[p]
        here = slice(start, start + size)
        odd_here = slice(HD + start, HD + start + size)
        out_all(p).wait_recv()
        for j in range(pairs):
            at = slice(j * LANES, (j + 1) * LANES)
            mixed = jnp.zeros((size, LANES), F32)
            for source in range(groups):
                at_source = slice(source, source + 1)
                scale = jnp.where(
                    low, shares[j, here, at_source], shares[j, odd_here, at_source]
                )
                mixed = mixed + scale * orecv[own, source, here, at].astype(F32)
            att[:size, at] = mixed.astype(BF16)

        attended = att[:size, :]
        psend[rows_of(p), :] = jnp.dot(
            attended, wo[other], preferred_element_type=F32
        ).astype(BF16)
        pair_copy(p).start()
        half[:size, :] = jnp.dot(attended, wo[c], preferred_element_type=F32)
        pair_copy(p).wait_recv()

        def add(i):
            at = chip_part(lax.rem(x + i, chips))
            both = half[:size, at] + precv[rows_of(p), at].astype(F32)
            xsend[rows_of(p), at] = both.astype(BF16)

        def to_chip(k, n):
            i = alternate(k, chips)
            add(i)
            sum_copy(p, i).start()
            return n

        lax.fori_loop(0, chips - 1, to_chip, 0)
        add(0)

    for p, (own, start, size) in enumerate(pieces):
        if start == 0:
            share_of(own)
        project(p)

    def sent(all_of, sem):
        pltpu.make_async_remote_copy(
            all_of, all_of, sem, qr, device_id={"seq": right}
        ).wait_send()

    sent(rows.at[pl.ds(0, chips - 1)], rs)
    sent(rows.at[pl.ds(0, chips)], ds)
    sent(qbuf.at[pl.ds(0, questions - mine)], qs)
    sent(osend.at[:, pl.ds(0, groups - 1)], os_)
    sent(lsend.at[:, pl.ds(0, groups - 1)], ss)
    feature = pl.ds(pl.multiple_of(me * cols, cols), cols)
    def out_store(p):
        own, start, size = pieces[p]
        return pltpu.make_async_copy(
            out_here.at[rows_of(p)], out_hbm.at[own, pl.ds(start, size)], load_sem.at[p]
        )

    for p in range(len(pieces)):
        at = rows_of(p)
        result = dec_raw[at, feature].astype(F32) + xsend[at, chip_part(x)].astype(F32)
        sum_all(p).wait_recv()
        for i in range(1, chips):
            result = result + xrecv[i, at].astype(F32)
        out_here[at, :] = result.astype(BF16)
        out_store(p).start()
    sent(psend, ps)
    sent(xrecv.at[pl.ds(0, chips - 1)], xs)
    for p in range(len(pieces)):
        out_store(p).wait()


def body(
    states, enc_gain, dec_states, dec_gain, query_weight, key_value_weight, out_weight, question_of
):
    shards, groups = lax.axis_size("seq"), lax.axis_size("qset")
    chips = shards // CORES
    plen, width = states.shape[2:]
    mine, tokens = dec_states.shape[:2]
    cols = query_weight.shape[1]
    questions = mine * groups
    messages = (chips - 1) * CHUNKS // 2
    pieces = len(pieces_of(mine, tokens))
    hbm = pl.BlockSpec(memory_space=pl.ANY)
    dma = lambda n: pltpu.SemaphoreType.DMA((n,))
    one = pltpu.SemaphoreType.DMA
    return pl.pallas_call(
        kernel,
        out_shape=jax.ShapeDtypeStruct((mine, tokens, cols), BF16),
        in_specs=[hbm] * 8,
        out_specs=hbm,
        scratch_shapes=[
            pltpu.VMEM((plen, width), BF16),
            pltpu.VMEM((mine * tokens, width), BF16),
            pltpu.VMEM((mine * tokens, width), BF16),
            pltpu.VMEM((shards, plen, width), BF16),
            pltpu.VMEM((width, cols), BF16),
            pltpu.VMEM((width, 2, cols), BF16),
            pltpu.VMEM((width, 2 * cols), BF16),
            pltpu.VMEM((CORES, cols, chips * cols), BF16),
            pltpu.VMEM((shards, plen, 2 * cols), BF16),
            pltpu.VMEM((questions, tokens, cols), BF16),
            pltpu.VMEM((shards, tokens, cols), F32),
            pltpu.VMEM((shards, tokens, cols), F32),
            pltpu.VMEM((shards, tokens, cols), F32),
            pltpu.VMEM((mine, groups, tokens, cols), BF16),
            pltpu.VMEM((mine, groups, tokens, cols), BF16),
            pltpu.VMEM((mine, groups, 1, tokens * cols // HD), F32),
            pltpu.VMEM((mine, groups, 1, tokens * cols // HD), F32),
            pltpu.VMEM((cols // LANES, LANES, groups), F32),
            pltpu.VMEM((tokens // 2, cols), BF16),
            pltpu.VMEM((tokens // 2, chips * cols), F32),
            pltpu.VMEM((mine * tokens, chips * cols), BF16),
            pltpu.VMEM((mine * tokens, chips * cols), BF16),
            pltpu.VMEM((mine * tokens, chips * cols), BF16),
            pltpu.VMEM((chips, mine * tokens, cols), BF16),
            pltpu.VMEM((mine * tokens, cols), BF16),
            pltpu.VMEM((16, width), F32),
            pltpu.VMEM((width,), BF16),
            pltpu.VMEM((width,), BF16),
            pltpu.SMEM(question_of.shape[:2], jnp.int32),
            pltpu.SMEM((questions,), jnp.int32),
            pltpu.SMEM((questions,), jnp.int32),
            pltpu.SMEM((questions,), jnp.int32),
            dma(CHUNKS + 7),
            one, dma(messages), dma(messages),
            one, dma(CHUNKS * chips),
            one, one, one, dma(pieces), one, dma(mine),
            one, dma(pieces), one, dma(pieces),
            pltpu.SemaphoreType.REGULAR, pltpu.SemaphoreType.REGULAR,
        ],
        compiler_params=pltpu.CompilerParams(
            collective_id=0, has_side_effects=True, vmem_limit_bytes=60 * 1024 * 1024
        ),
        name="reader_step",
    )(
        question_of[:, :, 0],
        states.reshape(plen, width),
        enc_gain,
        dec_states.reshape(mine * tokens, width),
        dec_gain,
        query_weight,
        key_value_weight,
        out_weight,
    )


def solution(mesh):
    return jax.shard_map(
        body,
        mesh=mesh,
        in_specs=(
            P(("groups", "qset"), "seq", None, None),
            P(),
            P(("groups", "qset"), None, None),
            P(),
            P(None, "seq"),
            P(None, None, "seq"),
            P("seq", None),
            P("groups", None, None),
        ),
        out_specs=P(("groups", "qset"), None, "seq"),
        check_vma=False,
    )
```

```python
import functools

import jax
import jax.numpy as jnp
from jax import lax
from jax.experimental import pallas as pl
from jax.experimental.pallas import tpu as pltpu
from jax.sharding import PartitionSpec as P

HD = 64
EPSILON = 1e-06
DEAD = -1e30
LANES = 128
CORES = 2
CHUNKS = 4
LAG = 4
PARTS = 2
F32 = jnp.float32
BF16 = jnp.bfloat16


def normalise(src, gain, dst_at, start, rows_here):
    step = 16

    def one(i, carry):
        at = pl.ds(pl.multiple_of(start + i * step, step), step)
        rows = src[at, :].astype(F32)
        mean_square = jnp.mean(rows * rows, axis=-1, keepdims=True)
        dst_at[at, :] = (rows * lax.rsqrt(mean_square + EPSILON) * gain[...]).astype(BF16)
        return carry

    lax.fori_loop(0, rows_here // step, one, 0)


def kernel(
    table_hbm, states_hbm, enc_gain_hbm, dec_hbm, dec_gain_hbm, wq_hbm, wkv_hbm, wo_hbm, out_ref,
    raw, dec_raw, dec_rows, rows, wq, wkv_in, wkv, wo, kv, qbuf, num, peak, total,
    osend, orecv, lsend, lrecv, shares, att, half, psend, precv, xsend, xrecv, gains,
    enc_gain, dec_gain, table, first, second, hits,
    load_sem, rs, rr, lr, ds, dr, qs, qr, os_, or_, ss, sr, ps, pr, xs, xr, rising, falling,
):
    shards, groups = lax.axis_size("seq"), lax.axis_size("qset")
    chips = shards // CORES
    me, g = lax.axis_index("seq"), lax.axis_index("qset")
    x, c = lax.div(me, CORES), lax.rem(me, CORES)
    plen, width = raw.shape
    questions, tokens, cols = qbuf.shape
    mine = questions // groups
    piece = plen // CHUNKS
    messages = (chips - 1) * CHUNKS // 2

    def seq_at(chip, core):
        return lax.rem(chip + 2 * chips, chips) * CORES + core

    right, left = seq_at(x + 1, c), seq_at(x - 1, c)
    other = 1 - c
    partner = seq_at(x, other)

    def load(i, src, dst):
        return pltpu.make_async_copy(src, dst, load_sem.at[i])

    def states_load(k):
        at = pl.ds(k * piece, piece)
        return load(k, states_hbm.at[at], raw.at[at])

    enc_gain_load = load(CHUNKS, enc_gain_hbm, enc_gain)
    dec_load = load(CHUNKS + 1, dec_hbm, dec_raw)
    wq_load = load(CHUNKS + 2, wq_hbm, wq)
    wkv_load = load(CHUNKS + 3, wkv_hbm, wkv_in)
    dec_gain_load = load(CHUNKS + 4, dec_gain_hbm, dec_gain)
    table_load = load(CHUNKS + 5, table_hbm, table)

    def wo_load(i):
        chip, core = lax.div(i, CORES), lax.rem(i, CORES)
        src = wo_hbm.at[:, pl.ds(pl.multiple_of(i * cols, cols), cols)]
        dst = wo.at[core, :, pl.ds(pl.multiple_of(chip * cols, cols), cols)]
        return load(CHUNKS + 6, src, dst)

    inward = [k // 2 if k % 2 == 0 else CHUNKS - 1 - k // 2 for k in range(CHUNKS)]
    enc_gain_load.start()
    for k in inward:
        states_load(k).start()

    barrier = pltpu.get_barrier_semaphore()
    above, below = g + 1, g - 1

    def if_above(do):
        pl.when(g < groups - 1)(do)

    def if_below(do):
        pl.when(g > 0)(do)

    pl.semaphore_signal(barrier, inc=1, device_id={"seq": left})
    pl.semaphore_signal(barrier, inc=1, device_id={"seq": right})

    @pl.when(c == 1)
    def _():
        pl.semaphore_signal(barrier, inc=1, device_id={"seq": partner})

    if_below(lambda: pl.semaphore_signal(barrier, inc=1, device_id={"qset": below}))

    def part(slot, chunk):
        return rows.at[slot, pl.ds(pl.multiple_of(chunk * piece, piece), piece), :]

    def right_copy(m, behind):
        at = part(seq_at(x - lax.div(m, CHUNKS) - behind, c), lax.rem(m, CHUNKS))
        return pltpu.make_async_remote_copy(at, at, rs, rr.at[m], device_id={"seq": right})

    def left_copy(m, behind):
        at = part(seq_at(x + lax.div(m, CHUNKS) + behind, c), CHUNKS - 1 - lax.rem(m, CHUNKS))
        return pltpu.make_async_remote_copy(at, at, rs, lr.at[m], device_id={"seq": left})

    def die_copy(at, k):
        return pltpu.make_async_remote_copy(at, at, ds, dr.at[k], device_id={"seq": partner})

    def die_own(slot):
        return die_copy(rows.at[slot], 0)

    def from_left(m, core):
        return seq_at(x - lax.div(m, CHUNKS) - 1, core), lax.rem(m, CHUNKS)

    def from_right(m, core):
        return seq_at(x + lax.div(m, CHUNKS) + 1, core), CHUNKS - 1 - lax.rem(m, CHUNKS)

    enc_gain_load.wait()
    gains[0:1, :] = enc_gain[...].astype(F32).reshape(1, width)
    done, sent_right, sent_left = set(), 0, 0
    for k in inward:
        states_load(k).wait()
        normalise(raw, gains.at[0:1, :], rows.at[me], k * piece, piece)
        if not done:
            pl.semaphore_wait(barrier, 2 + (1 - c) + 1 - lax.div(g + 1, groups))
        done.add(k)
        while sent_right in done:
            right_copy(jnp.int32(sent_right), 0).start()
            sent_right += 1
        while CHUNKS - 1 - sent_left in done:
            left_copy(jnp.int32(sent_left), 0).start()
            sent_left += 1
    for one in (wkv_load, dec_load, dec_gain_load, wq_load, table_load):
        one.start()
    lax.fori_loop(0, shards, lambda i, n: (wo_load(i).start(), n)[1], 0)

    @pl.when(c == 0)
    def _():
        die_own(me).start()

    @pl.when(g == 0)
    def _():
        pl.semaphore_signal(rising, inc=1, device_id={"qset": above})

    own_q = qbuf.at[pl.ds(g * mine, mine)]

    def own_queries():
        dec_load.wait()
        dec_gain_load.wait()
        gains[8:9, :] = dec_gain[...].astype(F32).reshape(1, width)
        normalise(dec_raw, gains.at[8:9, :], dec_rows, 0, dec_raw.shape[0])
        wq_load.wait()
        queries = jnp.dot(dec_rows[...], wq[...], preferred_element_type=F32).astype(BF16)
        own_q[...] = queries.reshape(mine, tokens, cols)

    def query_copy(i):
        to = lax.rem(g + i, groups)
        return pltpu.make_async_remote_copy(
            own_q, own_q, qs, qr, device_id={"qset": to}
        )

    def query_all():
        at = qbuf.at[pl.ds(0, questions - mine)]
        return pltpu.make_async_remote_copy(at, at, qs, qr, device_id={"qset": above})

    passages = table.shape[1]

    def find(q, n):
        def look(p, found):
            at0, at1, count = found
            hit = table[g, p] == q
            at0 = jnp.where(hit & (count == 0), p, at0)
            at1 = jnp.where(hit & (count == 1), p, at1)
            return at0, at1, count + hit.astype(jnp.int32)

        zero = jnp.int32(0)
        at0, at1, count = lax.fori_loop(0, passages, look, (zero, zero, zero))
        first[q], second[q], hits[q] = at0, at1, count
        return n

    lane = lax.broadcasted_iota(jnp.int32, (1, LANES), 1)
    low = lane < HD

    def key_values(slots):
        together = jnp.concatenate([part(*s)[...] for s in slots], axis=0)
        result = jnp.dot(together, wkv[...], preferred_element_type=F32).astype(BF16)
        for i, (slot, chunk) in enumerate(slots):
            at = pl.ds(pl.multiple_of(chunk * piece, piece), piece)
            kv[slot, at, :] = result[i * piece : (i + 1) * piece]

    def attend(slot):
        asked = qbuf[table[g, slot]]
        for j in range(cols // LANES):
            at = slice(j * LANES, (j + 1) * LANES)
            pair = asked[:, at]
            none = jnp.zeros_like(pair)
            stacked = jnp.concatenate([jnp.where(low, pair, none), jnp.where(low, none, pair)], axis=0)
            keys = kv[slot, :, at]
            values = kv[slot, :, cols + j * LANES : cols + (j + 1) * LANES]
            scores = lax.dot_general(
                stacked, keys, (((1,), (1,)), ((), ())), preferred_element_type=F32
            )
            top = jnp.max(scores, axis=-1, keepdims=True)
            weights = jnp.exp(scores - top)
            summed = jnp.sum(weights, axis=-1, keepdims=True)
            product = jnp.dot(weights.astype(BF16), values, preferred_element_type=F32)
            num[slot, :, at] = jnp.where(low, product[:tokens], product[tokens:])
            peak[slot, :, at] = jnp.where(low, top[:tokens], top[tokens:])
            total[slot, :, at] = jnp.where(low, summed[:tokens], summed[tokens:])

    wkv_load.wait()
    block = 64

    def unzip(i, n):
        at = pl.ds(pl.multiple_of(i * block, block), block)
        wkv[at, :cols] = wkv_in[at, 0, :]
        wkv[at, cols:] = wkv_in[at, 1, :]
        return n

    lax.fori_loop(0, width // block, unzip, 0)

    def whole_values(slot):
        result = jnp.dot(rows[slot], wkv[...], preferred_element_type=F32)
        kv[slot] = result.astype(BF16)

    def partner_part(m):
        die_copy(rows.at[partner, pl.ds(0, 2 * piece)], 1 + m).wait_recv()
        key_values([from_left(m, other), from_right(m, other)])

    def die_right(m):
        die_copy(part(*from_left(m, c)), 1 + m).start()

    def die_left(m):
        die_copy(part(*from_right(m, c)), 1 + m).start()

    hold = 2
    catch = messages - 4
    partner_at = min(LAG, catch)

    def part_done(m):
        return m + LAG if m + LAG < catch else max(catch, m + 1)

    def step(m, n):
        @pl.when(m > catch)
        def _():
            partner_part(m - 1)

        right_copy(m, 1).wait_recv()

        @pl.when(m + CHUNKS < messages)
        def _():
            right_copy(m + CHUNKS, 0).start()

        @pl.when((1 - c) * messages + m > hold)
        def _():
            die_right(m)

        left_copy(m, 1).wait_recv()

        @pl.when(m + CHUNKS < messages)
        def _():
            left_copy(m + CHUNKS, 0).start()

        @pl.when((1 - c) * messages + m > hold)
        def _():
            die_left(m)

        @pl.when(m == 0)
        def _():
            whole_values(me)

        key_values([from_left(m, c), from_right(m, c)])

        @pl.when(m == 1)
        def _():
            own_queries()
            if_below(lambda: pl.semaphore_wait(rising, 1))

            @pl.when(g > 0)
            def _():
                if_above(
                    lambda: pl.semaphore_signal(rising, inc=1, device_id={"qset": above})
                )

        @pl.when(m == hold)
        def _():
            @pl.when(c == 1)
            def _():
                die_own(partner).wait_recv()
                die_own(me).start()

                def late(k, t):
                    die_right(k)
                    die_left(k)
                    return t

                lax.fori_loop(0, hold + 1, late, 0)

            if_above(lambda: pl.semaphore_wait(falling, 1))
            if_below(lambda: pl.semaphore_signal(falling, inc=1, device_id={"qset": below}))
            lax.fori_loop(1, groups, lambda i, k: (query_copy(i).start(), k)[1], 0)

        @pl.when(m == hold + 1)
        def _():
            table_load.wait()
            lax.fori_loop(0, questions, find, 0)

        @pl.when(m == partner_at)
        def _():
            @pl.when(c == 0)
            def _():
                die_own(partner).wait_recv()

            whole_values(partner)

        if catch > LAG:

            @pl.when(m >= LAG)
            def _():
                @pl.when(m < catch)
                def _():
                    partner_part(m - LAG)

        @pl.when(m == catch)
        def _():
            lax.fori_loop(
                max(0, catch - LAG), catch, lambda k, t: (partner_part(k), t)[1], 0
            )

        @pl.when(m == messages // 2)
        def _():
            query_all().wait_recv()
            lax.fori_loop(0, CORES, lambda i, k: (attend(seq_at(x, i)), k)[1], 0)

        for far in range(1, chips // 2):

            @pl.when(m == max(part_done(far * CHUNKS - 1), messages // 2 + far))
            def _():
                def both(i, k):
                    attend(seq_at(x - far, i))
                    attend(seq_at(x + far, i))
                    return k

                lax.fori_loop(0, CORES, both, 0)

        return n

    lax.fori_loop(0, messages, step, 0)
    attend(seq_at(x + chips // 2, c))
    partner_part(messages - 1)
    attend(seq_at(x + chips // 2, other))

    pairs = cols // LANES

    def alternate(k, n):
        reach = lax.div(k + 1, 2)
        return n // 2 - reach + 2 * reach * lax.rem(k, 2)

    short = tokens // PARTS

    def out_copy(own, cut, i):
        to = lax.rem(g + i, groups)
        here = pl.ds(cut * short, short)
        return pltpu.make_async_remote_copy(
            osend.at[own, to, here],
            orecv.at[own, g, here],
            os_, or_.at[own * PARTS + cut], device_id={"qset": to},
        )

    def out_all(own, cut):
        at = orecv.at[own, pl.ds(0, groups - 1), pl.ds(cut * short, short)]
        return pltpu.make_async_remote_copy(
            at, at, os_, or_.at[own * PARTS + cut], device_id={"qset": above}
        )

    def lse_copy(own, i):
        to = lax.rem(g + i, groups)
        return pltpu.make_async_remote_copy(
            lsend.at[own, to],
            lrecv.at[own, g],
            ss, sr.at[own], device_id={"qset": to},
        )

    def lse_all(own):
        at = lrecv.at[own, pl.ds(0, groups - 1)]
        return pltpu.make_async_remote_copy(at, at, ss, sr.at[own], device_id={"qset": above})

    def merge(own, to, mix_at, lse_at):
        q = to * mine + own
        at0, at1, count = first[q], second[q], hits[q]
        lses = []
        for j in range(pairs):
            at = slice(j * LANES, (j + 1) * LANES)
            top0 = jnp.where(count >= 1, peak[at0, :, at], DEAD)
            top1 = jnp.where(count >= 2, peak[at1, :, at], DEAD)
            top = jnp.maximum(top0, top1)
            scale0 = jnp.where(count >= 1, jnp.exp(top0 - top), 0.0)
            scale1 = jnp.where(count >= 2, jnp.exp(top1 - top), 0.0)
            mass = scale0 * total[at0, :, at] + scale1 * total[at1, :, at]
            mass = jnp.where(count >= 1, mass, 1.0)
            mix = (scale0 * num[at0, :, at] + scale1 * num[at1, :, at]) / mass
            mix_at[:, at] = mix.astype(BF16)
            lse = jnp.where(count >= 1, top + jnp.log(mass), DEAD)
            turned = jnp.transpose(lse)
            lses += [turned[:1], turned[HD : HD + 1]]
        lse_at[...] = jnp.concatenate(lses, axis=1)

    def merge_and_send(own):
        def one(k, n):
            i = alternate(k, groups)
            to = lax.rem(g + i, groups)
            merge(own, to, osend.at[own, to], lsend.at[own, to])
            lse_copy(own, i).start()
            out_copy(own, 0, i).start()
            return n

        lax.fori_loop(0, groups - 1, one, 0)
        for cut in range(1, PARTS):

            def rest(k, n):
                out_copy(own, cut, alternate(k, groups)).start()
                return n

            lax.fori_loop(0, groups - 1, rest, 0)

    for own in range(mine):
        merge_and_send(own)
    for own in range(mine):
        merge(own, g, orecv.at[own, g], lrecv.at[own, g])
    pltpu.make_async_copy(wo, wo, load_sem.at[CHUNKS + 6]).wait()

    def pair_copy(piece):
        return pltpu.make_async_remote_copy(
            psend.at[piece], precv.at[piece], ps, pr.at[piece],
            device_id={"seq": partner},
        )

    def chip_part(chip):
        return pl.ds(pl.multiple_of(chip * cols, cols), cols)

    def sum_copy(piece, i):
        to = lax.rem(x + i, chips)
        return pltpu.make_async_remote_copy(
            xsend.at[piece, :, chip_part(to)], xrecv.at[piece, i],
            xs, xr.at[piece], device_id={"seq": seq_at(to, c)},
        )

    def sum_all(piece):
        at = xrecv.at[piece, pl.ds(1, chips - 1)]
        return pltpu.make_async_remote_copy(at, at, xs, xr.at[piece], device_id={"seq": right})

    def share_of(own):
        lse_all(own).wait_recv()
        every = jnp.concatenate([lrecv[own, k] for k in range(groups)], axis=0)
        top = jnp.max(every, axis=0, keepdims=True)
        share = jnp.exp(every - top)
        share = share / jnp.sum(share, axis=0, keepdims=True)
        for j in range(pairs):
            shares[j] = jnp.transpose(share[:, j * LANES : (j + 1) * LANES])

    def project(own, cut):
        piece = own * PARTS + cut
        here = slice(cut * short, (cut + 1) * short)
        odd_here = slice(HD + cut * short, HD + (cut + 1) * short)
        out_all(own, cut).wait_recv()
        for j in range(pairs):
            at = slice(j * LANES, (j + 1) * LANES)
            mixed = jnp.zeros((short, LANES), F32)
            for source in range(groups):
                at_source = slice(source, source + 1)
                scale = jnp.where(
                    low, shares[j, here, at_source], shares[j, odd_here, at_source]
                )
                mixed = mixed + scale * orecv[own, source, here, at].astype(F32)
            att[:, at] = mixed.astype(BF16)

        psend[piece] = jnp.dot(att[...], wo[other], preferred_element_type=F32).astype(BF16)
        pair_copy(piece).start()
        half[...] = jnp.dot(att[...], wo[c], preferred_element_type=F32)
        pair_copy(piece).wait_recv()

        def add(i):
            at = chip_part(lax.rem(x + i, chips))
            xsend[piece, :, at] = (half[:, at] + precv[piece, :, at].astype(F32)).astype(BF16)

        def to_chip(k, n):
            i = alternate(k, chips)
            add(i)
            sum_copy(piece, i).start()
            return n

        lax.fori_loop(0, chips - 1, to_chip, 0)
        add(0)

    for own in range(mine):
        share_of(own)
        for cut in range(PARTS):
            project(own, cut)

    def sent(all_of, sem):
        pltpu.make_async_remote_copy(
            all_of, all_of, sem, qr, device_id={"seq": right}
        ).wait_send()

    sent(rows.at[pl.ds(0, chips - 1)], rs)
    sent(rows.at[pl.ds(0, chips)], ds)
    sent(qbuf.at[pl.ds(0, questions - mine)], qs)
    sent(osend.at[:, pl.ds(0, groups - 1)], os_)
    sent(lsend.at[:, pl.ds(0, groups - 1)], ss)
    feature = pl.ds(pl.multiple_of(me * cols, cols), cols)
    for piece in range(mine * PARTS):
        here = slice(piece * short, (piece + 1) * short)
        result = dec_raw[here, feature].astype(F32) + xsend[piece, :, chip_part(x)].astype(F32)
        sum_all(piece).wait_recv()
        for i in range(1, chips):
            result = result + xrecv[piece, i].astype(F32)
        own, cut = divmod(piece, PARTS)
        out_ref[own, cut * short : (cut + 1) * short, :] = result.astype(BF16)
    sent(psend, ps)
    sent(xrecv.at[:, pl.ds(0, chips - 1)], xs)


def body(
    states, enc_gain, dec_states, dec_gain, query_weight, key_value_weight, out_weight, question_of
):
    shards, groups = lax.axis_size("seq"), lax.axis_size("qset")
    chips = shards // CORES
    plen, width = states.shape[2:]
    mine, tokens = dec_states.shape[:2]
    cols = query_weight.shape[1]
    questions = mine * groups
    messages = (chips - 1) * CHUNKS // 2
    pieces, short = mine * PARTS, tokens // PARTS
    hbm = pl.BlockSpec(memory_space=pl.ANY)
    vmem = pl.BlockSpec(memory_space=pltpu.VMEM)
    dma = lambda n: pltpu.SemaphoreType.DMA((n,))
    one = pltpu.SemaphoreType.DMA
    return pl.pallas_call(
        kernel,
        out_shape=pltpu.VMEM((mine, tokens, cols), BF16),
        in_specs=[hbm] * 8,
        out_specs=vmem,
        scratch_shapes=[
            pltpu.VMEM((plen, width), BF16),
            pltpu.VMEM((mine * tokens, width), BF16),
            pltpu.VMEM((mine * tokens, width), BF16),
            pltpu.VMEM((shards, plen, width), BF16),
            pltpu.VMEM((width, cols), BF16),
            pltpu.VMEM((width, 2, cols), BF16),
            pltpu.VMEM((width, 2 * cols), BF16),
            pltpu.VMEM((CORES, cols, chips * cols), BF16),
            pltpu.VMEM((shards, plen, 2 * cols), BF16),
            pltpu.VMEM((questions, tokens, cols), BF16),
            pltpu.VMEM((shards, tokens, cols), F32),
            pltpu.VMEM((shards, tokens, cols), F32),
            pltpu.VMEM((shards, tokens, cols), F32),
            pltpu.VMEM((mine, groups, tokens, cols), BF16),
            pltpu.VMEM((mine, groups, tokens, cols), BF16),
            pltpu.VMEM((mine, groups, 1, tokens * cols // HD), F32),
            pltpu.VMEM((mine, groups, 1, tokens * cols // HD), F32),
            pltpu.VMEM((cols // LANES, LANES, groups), F32),
            pltpu.VMEM((short, cols), BF16),
            pltpu.VMEM((short, chips * cols), F32),
            pltpu.VMEM((pieces, short, chips * cols), BF16),
            pltpu.VMEM((pieces, short, chips * cols), BF16),
            pltpu.VMEM((pieces, short, chips * cols), BF16),
            pltpu.VMEM((pieces, chips, short, cols), BF16),
            pltpu.VMEM((16, width), F32),
            pltpu.VMEM((width,), BF16),
            pltpu.VMEM((width,), BF16),
            pltpu.SMEM(question_of.shape[:2], jnp.int32),
            pltpu.SMEM((questions,), jnp.int32),
            pltpu.SMEM((questions,), jnp.int32),
            pltpu.SMEM((questions,), jnp.int32),
            dma(CHUNKS + 7),
            one, dma(messages), dma(messages),
            one, dma(1 + messages),
            one, one, one, dma(pieces), one, dma(mine),
            one, dma(pieces), one, dma(pieces),
            pltpu.SemaphoreType.REGULAR, pltpu.SemaphoreType.REGULAR,
        ],
        compiler_params=pltpu.CompilerParams(
            collective_id=0, has_side_effects=True, vmem_limit_bytes=60 * 1024 * 1024
        ),
        name="reader_step",
    )(
        question_of[:, :, 0],
        states.reshape(plen, width),
        enc_gain,
        dec_states.reshape(mine * tokens, width),
        dec_gain,
        query_weight,
        key_value_weight,
        out_weight,
    )


def solution(mesh):
    return jax.shard_map(
        body,
        mesh=mesh,
        in_specs=(
            P(("groups", "qset"), "seq", None, None),
            P(),
            P(("groups", "qset"), None, None),
            P(),
            P(None, "seq"),
            P(None, None, "seq"),
            P("seq", None),
            P("groups", None, None),
        ),
        out_specs=P(("groups", "qset"), None, "seq"),
        check_vma=False,
    )
```

```python
import functools

import jax
import jax.numpy as jnp
from jax import lax
from jax.experimental import pallas as pl
from jax.experimental.pallas import tpu as pltpu
from jax.sharding import PartitionSpec as P

HD = 64
EPSILON = 1e-06
DEAD = -1e30
LANES = 128
CORES = 2
CHUNKS = 4
LAG = 4
F32 = jnp.float32
BF16 = jnp.bfloat16


def pieces_of(mine, tokens):
    half, quarter = tokens // 2, tokens // 4
    pieces = [(own, start, half) for own in range(mine) for start in (0, half)]
    return pieces[:-1] + [(mine - 1, half, quarter), (mine - 1, half + quarter, quarter)]


def normalise(src, gain, dst_at, start, rows_here):
    step = 16

    def one(i, carry):
        at = pl.ds(pl.multiple_of(start + i * step, step), step)
        rows = src[at, :].astype(F32)
        mean_square = jnp.mean(rows * rows, axis=-1, keepdims=True)
        dst_at[at, :] = (rows * lax.rsqrt(mean_square + EPSILON) * gain[...]).astype(BF16)
        return carry

    lax.fori_loop(0, rows_here // step, one, 0)


def kernel(
    table_hbm, states_hbm, enc_gain_hbm, dec_hbm, dec_gain_hbm, wq_hbm, wkv_hbm, wo_hbm, out_ref,
    raw, dec_raw, dec_rows, rows, wq, wkv_in, wkv, wo, kv, qbuf, num, peak, total,
    osend, orecv, lsend, lrecv, shares, att, halves, psend, precv, xsend, xrecv, gains,
    enc_gain, dec_gain, table, first, second, hits,
    load_sem, rs, rr, lr, ds, dr, qs, qr, os_, or_, ss, sr, ps, pr, xs, xr, rising, falling,
):
    shards, groups = lax.axis_size("seq"), lax.axis_size("qset")
    chips = shards // CORES
    me, g = lax.axis_index("seq"), lax.axis_index("qset")
    x, c = lax.div(me, CORES), lax.rem(me, CORES)
    plen, width = raw.shape
    questions, tokens, cols = qbuf.shape
    mine = questions // groups
    piece = plen // CHUNKS
    messages = (chips - 1) * CHUNKS // 2

    def seq_at(chip, core):
        return lax.rem(chip + 2 * chips, chips) * CORES + core

    right, left = seq_at(x + 1, c), seq_at(x - 1, c)
    other = 1 - c
    partner = seq_at(x, other)

    def load(i, src, dst):
        return pltpu.make_async_copy(src, dst, load_sem.at[i])

    def states_load(k):
        at = pl.ds(k * piece, piece)
        return load(k, states_hbm.at[at], raw.at[at])

    enc_gain_load = load(CHUNKS, enc_gain_hbm, enc_gain)
    dec_load = load(CHUNKS + 1, dec_hbm, dec_raw)
    wq_load = load(CHUNKS + 2, wq_hbm, wq)
    wkv_load = load(CHUNKS + 3, wkv_hbm, wkv_in)
    dec_gain_load = load(CHUNKS + 4, dec_gain_hbm, dec_gain)
    table_load = load(CHUNKS + 5, table_hbm, table)

    def wo_load(i):
        chip, core = lax.div(i, CORES), lax.rem(i, CORES)
        src = wo_hbm.at[:, pl.ds(pl.multiple_of(i * cols, cols), cols)]
        dst = wo.at[core, :, pl.ds(pl.multiple_of(chip * cols, cols), cols)]
        return load(CHUNKS + 6, src, dst)

    inward = [k // 2 if k % 2 == 0 else CHUNKS - 1 - k // 2 for k in range(CHUNKS)]
    enc_gain_load.start()
    for k in inward:
        states_load(k).start()

    barrier = pltpu.get_barrier_semaphore()
    above, below = g + 1, g - 1

    def if_above(do):
        pl.when(g < groups - 1)(do)

    def if_below(do):
        pl.when(g > 0)(do)

    pl.semaphore_signal(barrier, inc=1, device_id={"seq": left})
    pl.semaphore_signal(barrier, inc=1, device_id={"seq": right})

    @pl.when(c == 1)
    def _():
        pl.semaphore_signal(barrier, inc=1, device_id={"seq": partner})

    if_below(lambda: pl.semaphore_signal(barrier, inc=1, device_id={"qset": below}))

    def part(slot, chunk):
        return rows.at[slot, pl.ds(pl.multiple_of(chunk * piece, piece), piece), :]

    def right_copy(m, behind):
        at = part(seq_at(x - lax.div(m, CHUNKS) - behind, c), lax.rem(m, CHUNKS))
        return pltpu.make_async_remote_copy(at, at, rs, rr.at[m], device_id={"seq": right})

    def left_copy(m, behind):
        at = part(seq_at(x + lax.div(m, CHUNKS) + behind, c), CHUNKS - 1 - lax.rem(m, CHUNKS))
        return pltpu.make_async_remote_copy(at, at, rs, lr.at[m], device_id={"seq": left})

    def die_copy(at, k):
        return pltpu.make_async_remote_copy(at, at, ds, dr.at[k], device_id={"seq": partner})

    def die_own(slot):
        return die_copy(rows.at[slot], 0)

    def from_left(m, core):
        return seq_at(x - lax.div(m, CHUNKS) - 1, core), lax.rem(m, CHUNKS)

    def from_right(m, core):
        return seq_at(x + lax.div(m, CHUNKS) + 1, core), CHUNKS - 1 - lax.rem(m, CHUNKS)

    enc_gain_load.wait()
    gains[0:1, :] = enc_gain[...].astype(F32).reshape(1, width)
    done, sent_right, sent_left = set(), 0, 0
    for k in inward:
        states_load(k).wait()
        normalise(raw, gains.at[0:1, :], rows.at[me], k * piece, piece)
        if not done:
            pl.semaphore_wait(barrier, 2 + (1 - c) + 1 - lax.div(g + 1, groups))
        done.add(k)
        while sent_right in done:
            right_copy(jnp.int32(sent_right), 0).start()
            sent_right += 1
        while CHUNKS - 1 - sent_left in done:
            left_copy(jnp.int32(sent_left), 0).start()
            sent_left += 1
    for one in (wkv_load, dec_load, dec_gain_load, wq_load, table_load):
        one.start()
    lax.fori_loop(0, shards, lambda i, n: (wo_load(i).start(), n)[1], 0)

    @pl.when(c == 0)
    def _():
        die_own(me).start()

    @pl.when(g == 0)
    def _():
        pl.semaphore_signal(rising, inc=1, device_id={"qset": above})

    own_q = qbuf.at[pl.ds(g * mine, mine)]

    def own_queries():
        dec_load.wait()
        dec_gain_load.wait()
        gains[8:9, :] = dec_gain[...].astype(F32).reshape(1, width)
        normalise(dec_raw, gains.at[8:9, :], dec_rows, 0, dec_raw.shape[0])
        wq_load.wait()
        queries = jnp.dot(dec_rows[...], wq[...], preferred_element_type=F32).astype(BF16)
        own_q[...] = queries.reshape(mine, tokens, cols)

    def query_copy(i):
        to = lax.rem(g + i, groups)
        return pltpu.make_async_remote_copy(
            own_q, own_q, qs, qr, device_id={"qset": to}
        )

    def query_all():
        at = qbuf.at[pl.ds(0, questions - mine)]
        return pltpu.make_async_remote_copy(at, at, qs, qr, device_id={"qset": above})

    passages = table.shape[1]

    def find(q, n):
        def look(p, found):
            at0, at1, count = found
            hit = table[g, p] == q
            at0 = jnp.where(hit & (count == 0), p, at0)
            at1 = jnp.where(hit & (count == 1), p, at1)
            return at0, at1, count + hit.astype(jnp.int32)

        zero = jnp.int32(0)
        at0, at1, count = lax.fori_loop(0, passages, look, (zero, zero, zero))
        first[q], second[q], hits[q] = at0, at1, count
        return n

    lane = lax.broadcasted_iota(jnp.int32, (1, LANES), 1)
    low = lane < HD

    def key_values(slots):
        together = jnp.concatenate([part(*s)[...] for s in slots], axis=0)
        result = jnp.dot(together, wkv[...], preferred_element_type=F32).astype(BF16)
        for i, (slot, chunk) in enumerate(slots):
            at = pl.ds(pl.multiple_of(chunk * piece, piece), piece)
            kv[slot, at, :] = result[i * piece : (i + 1) * piece]

    def attend(slot):
        asked = qbuf[table[g, slot]]
        ats = [slice(j * LANES, (j + 1) * LANES) for j in range(cols // LANES)]
        scores = []
        for at in ats:
            pair = asked[:, at]
            none = jnp.zeros_like(pair)
            stacked = jnp.concatenate([jnp.where(low, pair, none), jnp.where(low, none, pair)], axis=0)
            scores.append(
                lax.dot_general(
                    stacked, kv[slot, :, at], (((1,), (1,)), ((), ())), preferred_element_type=F32
                )
            )
        tops = [jnp.max(one, axis=-1, keepdims=True) for one in scores]
        weights = [jnp.exp(one - top) for one, top in zip(scores, tops)]
        products = [
            jnp.dot(
                one.astype(BF16),
                kv[slot, :, cols + j * LANES : cols + (j + 1) * LANES],
                preferred_element_type=F32,
            )
            for j, one in enumerate(weights)
        ]
        sums = [jnp.sum(one, axis=-1, keepdims=True) for one in weights]
        for at, top, summed, product in zip(ats, tops, sums, products):
            num[slot, :, at] = jnp.where(low, product[:tokens], product[tokens:])
            peak[slot, :, at] = jnp.where(low, top[:tokens], top[tokens:])
            total[slot, :, at] = jnp.where(low, summed[:tokens], summed[tokens:])

    wkv_load.wait()
    block = 64

    def unzip(i, n):
        at = pl.ds(pl.multiple_of(i * block, block), block)
        wkv[at, :cols] = wkv_in[at, 0, :]
        wkv[at, cols:] = wkv_in[at, 1, :]
        return n

    lax.fori_loop(0, width // block, unzip, 0)

    def whole_values(slot):
        result = jnp.dot(rows[slot], wkv[...], preferred_element_type=F32)
        kv[slot] = result.astype(BF16)

    def partner_part(m):
        die_copy(rows.at[partner, pl.ds(0, 2 * piece)], 1 + m).wait_recv()
        key_values([from_left(m, other), from_right(m, other)])

    def die_right(m):
        die_copy(part(*from_left(m, c)), 1 + m).start()

    def die_left(m):
        die_copy(part(*from_right(m, c)), 1 + m).start()

    hold = 2
    catch = messages - 4
    partner_at = min(LAG, catch)

    def part_done(m):
        return m + LAG if m + LAG < catch else max(catch, m + 1)

    def step(m, n):
        @pl.when(m > catch)
        def _():
            partner_part(m - 1)

        right_copy(m, 1).wait_recv()

        @pl.when(m + CHUNKS < messages)
        def _():
            right_copy(m + CHUNKS, 0).start()

        @pl.when((1 - c) * messages + m > hold)
        def _():
            die_right(m)

        left_copy(m, 1).wait_recv()

        @pl.when(m + CHUNKS < messages)
        def _():
            left_copy(m + CHUNKS, 0).start()

        @pl.when((1 - c) * messages + m > hold)
        def _():
            die_left(m)

        @pl.when(m == 0)
        def _():
            whole_values(me)

        key_values([from_left(m, c), from_right(m, c)])

        @pl.when(m == 1)
        def _():
            own_queries()
            if_below(lambda: pl.semaphore_wait(rising, 1))

            @pl.when(g > 0)
            def _():
                if_above(
                    lambda: pl.semaphore_signal(rising, inc=1, device_id={"qset": above})
                )

        @pl.when(m == hold)
        def _():
            @pl.when(c == 1)
            def _():
                die_own(partner).wait_recv()
                die_own(me).start()

                def late(k, t):
                    die_right(k)
                    die_left(k)
                    return t

                lax.fori_loop(0, hold + 1, late, 0)

            if_above(lambda: pl.semaphore_wait(falling, 1))
            if_below(lambda: pl.semaphore_signal(falling, inc=1, device_id={"qset": below}))
            lax.fori_loop(1, groups, lambda i, k: (query_copy(i).start(), k)[1], 0)

        @pl.when(m == hold + 1)
        def _():
            table_load.wait()
            lax.fori_loop(0, questions, find, 0)

        @pl.when(m == partner_at)
        def _():
            @pl.when(c == 0)
            def _():
                die_own(partner).wait_recv()

            whole_values(partner)

        if catch > LAG:

            @pl.when(m >= LAG)
            def _():
                @pl.when(m < catch)
                def _():
                    partner_part(m - LAG)

        @pl.when(m == catch)
        def _():
            lax.fori_loop(
                max(0, catch - LAG), catch, lambda k, t: (partner_part(k), t)[1], 0
            )

        @pl.when(m == messages // 2)
        def _():
            query_all().wait_recv()
            lax.fori_loop(0, CORES, lambda i, k: (attend(seq_at(x, i)), k)[1], 0)

        for far in range(1, chips // 2):

            @pl.when(m == max(part_done(far * CHUNKS - 1), messages // 2 + far))
            def _():
                def both(i, k):
                    attend(seq_at(x - far, i))
                    attend(seq_at(x + far, i))
                    return k

                lax.fori_loop(0, CORES, both, 0)

        return n

    lax.fori_loop(0, messages, step, 0)
    attend(seq_at(x + chips // 2, c))
    partner_part(messages - 1)
    attend(seq_at(x + chips // 2, other))

    pairs = cols // LANES

    def alternate(k, n):
        reach = lax.div(k + 1, 2)
        return n // 2 - reach + 2 * reach * lax.rem(k, 2)

    pieces = pieces_of(mine, tokens)

    def out_copy(p, i):
        own, start, size = pieces[p]
        to = lax.rem(g + i, groups)
        here = pl.ds(start, size)
        return pltpu.make_async_remote_copy(
            osend.at[own, to, here],
            orecv.at[own, g, here],
            os_, or_.at[p], device_id={"qset": to},
        )

    def out_all(p):
        own, start, size = pieces[p]
        at = orecv.at[own, pl.ds(0, groups - 1), pl.ds(start, size)]
        return pltpu.make_async_remote_copy(at, at, os_, or_.at[p], device_id={"qset": above})

    def lse_copy(own, i):
        to = lax.rem(g + i, groups)
        return pltpu.make_async_remote_copy(
            lsend.at[own, to],
            lrecv.at[own, g],
            ss, sr.at[own], device_id={"qset": to},
        )

    def lse_all(own):
        at = lrecv.at[own, pl.ds(0, groups - 1)]
        return pltpu.make_async_remote_copy(at, at, ss, sr.at[own], device_id={"qset": above})

    def merge(own, to, mix_at, lse_at):
        q = to * mine + own
        at0, at1, count = first[q], second[q], hits[q]
        lses = []
        for j in range(pairs):
            at = slice(j * LANES, (j + 1) * LANES)
            top0 = jnp.where(count >= 1, peak[at0, :, at], DEAD)
            top1 = jnp.where(count >= 2, peak[at1, :, at], DEAD)
            top = jnp.maximum(top0, top1)
            scale0 = jnp.where(count >= 1, jnp.exp(top0 - top), 0.0)
            scale1 = jnp.where(count >= 2, jnp.exp(top1 - top), 0.0)
            mass = scale0 * total[at0, :, at] + scale1 * total[at1, :, at]
            mass = jnp.where(count >= 1, mass, 1.0)
            mix = (scale0 * num[at0, :, at] + scale1 * num[at1, :, at]) / mass
            mix_at[:, at] = mix.astype(BF16)
            lse = jnp.where(count >= 1, top + jnp.log(mass), DEAD)
            turned = jnp.transpose(lse)
            lses += [turned[:1], turned[HD : HD + 1]]
        lse_at[...] = jnp.concatenate(lses, axis=1)

    def merge_and_send(own):
        lead, *others = [p for p in range(len(pieces)) if pieces[p][0] == own]

        def one(k, n):
            i = alternate(k, groups)
            to = lax.rem(g + i, groups)
            merge(own, to, osend.at[own, to], lsend.at[own, to])
            lse_copy(own, i).start()
            out_copy(lead, i).start()
            return n

        lax.fori_loop(0, groups - 1, one, 0)
        for p in others:

            def rest(k, n):
                out_copy(p, alternate(k, groups)).start()
                return n

            lax.fori_loop(0, groups - 1, rest, 0)

    for own in range(mine):
        merge_and_send(own)
    for own in range(mine):
        merge(own, g, orecv.at[own, g], lrecv.at[own, g])
    pltpu.make_async_copy(wo, wo, load_sem.at[CHUNKS + 6]).wait()

    def rows_of(p):
        own, start, size = pieces[p]
        return pl.ds(own * tokens + start, size)

    def pair_copy(p):
        at = rows_of(p)
        return pltpu.make_async_remote_copy(
            psend.at[at], precv.at[at], ps, pr.at[p], device_id={"seq": partner}
        )

    def chip_part(chip):
        return pl.ds(pl.multiple_of(chip * cols, cols), cols)

    def sum_copy(p, i):
        to = lax.rem(x + i, chips)
        return pltpu.make_async_remote_copy(
            xsend.at[rows_of(p), chip_part(to)], xrecv.at[i, rows_of(p)],
            xs, xr.at[p], device_id={"seq": seq_at(to, c)},
        )

    def sum_all(p):
        at = xrecv.at[pl.ds(1, chips - 1), rows_of(p)]
        return pltpu.make_async_remote_copy(at, at, xs, xr.at[p], device_id={"seq": right})

    def share_of(own):
        lse_all(own).wait_recv()
        every = jnp.concatenate([lrecv[own, k] for k in range(groups)], axis=0)
        top = jnp.max(every, axis=0, keepdims=True)
        share = jnp.exp(every - top)
        share = share / jnp.sum(share, axis=0, keepdims=True)
        for j in range(pairs):
            shares[j] = jnp.transpose(share[:, j * LANES : (j + 1) * LANES])

    def project(p):
        own, start, size = pieces[p]
        here = slice(start, start + size)
        odd_here = slice(HD + start, HD + start + size)
        out_all(p).wait_recv()
        for j in range(pairs):
            at = slice(j * LANES, (j + 1) * LANES)
            mixed = jnp.zeros((size, LANES), F32)
            for source in range(groups):
                at_source = slice(source, source + 1)
                scale = jnp.where(
                    low, shares[j, here, at_source], shares[j, odd_here, at_source]
                )
                mixed = mixed + scale * orecv[own, source, here, at].astype(F32)
            att[:size, at] = mixed.astype(BF16)

        attended = att[:size, :]
        half = halves.at[p % 2]
        psend[rows_of(p), :] = jnp.dot(
            attended, wo[other], preferred_element_type=F32
        ).astype(BF16)
        pair_copy(p).start()
        half[:size, :] = jnp.dot(attended, wo[c], preferred_element_type=F32)

    def spread(p):
        own, start, size = pieces[p]
        half = halves.at[p % 2]
        pair_copy(p).wait_recv()

        def add(i):
            at = chip_part(lax.rem(x + i, chips))
            both = half[:size, at] + precv[rows_of(p), at].astype(F32)
            xsend[rows_of(p), at] = both.astype(BF16)

        def to_chip(k, n):
            i = alternate(k, chips)
            add(i)
            sum_copy(p, i).start()
            return n

        lax.fori_loop(0, chips - 1, to_chip, 0)
        add(0)

    for p, (own, start, size) in enumerate(pieces):
        if start == 0:
            share_of(own)
        project(p)
        if p + 2 < len(pieces):
            spread(p)
        elif p + 1 == len(pieces):
            spread(p - 1)
            spread(p)

    def sent(all_of, sem):
        pltpu.make_async_remote_copy(
            all_of, all_of, sem, qr, device_id={"seq": right}
        ).wait_send()

    sent(rows.at[pl.ds(0, chips - 1)], rs)
    sent(rows.at[pl.ds(0, chips)], ds)
    sent(qbuf.at[pl.ds(0, questions - mine)], qs)
    sent(osend.at[:, pl.ds(0, groups - 1)], os_)
    sent(lsend.at[:, pl.ds(0, groups - 1)], ss)
    feature = pl.ds(pl.multiple_of(me * cols, cols), cols)
    for p in range(len(pieces)):
        at = rows_of(p)
        result = dec_raw[at, feature].astype(F32) + xsend[at, chip_part(x)].astype(F32)
        sum_all(p).wait_recv()
        for i in range(1, chips):
            result = result + xrecv[i, at].astype(F32)
        own, start, size = pieces[p]
        out_ref[own, start : start + size, :] = result.astype(BF16)
    sent(psend, ps)
    sent(xrecv.at[pl.ds(0, chips - 1)], xs)


def body(
    states, enc_gain, dec_states, dec_gain, query_weight, key_value_weight, out_weight, question_of
):
    shards, groups = lax.axis_size("seq"), lax.axis_size("qset")
    chips = shards // CORES
    plen, width = states.shape[2:]
    mine, tokens = dec_states.shape[:2]
    cols = query_weight.shape[1]
    questions = mine * groups
    messages = (chips - 1) * CHUNKS // 2
    pieces = len(pieces_of(mine, tokens))
    hbm = pl.BlockSpec(memory_space=pl.ANY)
    dma = lambda n: pltpu.SemaphoreType.DMA((n,))
    one = pltpu.SemaphoreType.DMA
    return pl.pallas_call(
        kernel,
        out_shape=pltpu.VMEM((mine, tokens, cols), BF16),
        in_specs=[hbm] * 8,
        out_specs=pl.BlockSpec(memory_space=pltpu.VMEM),
        scratch_shapes=[
            pltpu.VMEM((plen, width), BF16),
            pltpu.VMEM((mine * tokens, width), BF16),
            pltpu.VMEM((mine * tokens, width), BF16),
            pltpu.VMEM((shards, plen, width), BF16),
            pltpu.VMEM((width, cols), BF16),
            pltpu.VMEM((width, 2, cols), BF16),
            pltpu.VMEM((width, 2 * cols), BF16),
            pltpu.VMEM((CORES, cols, chips * cols), BF16),
            pltpu.VMEM((shards, plen, 2 * cols), BF16),
            pltpu.VMEM((questions, tokens, cols), BF16),
            pltpu.VMEM((shards, tokens, cols), F32),
            pltpu.VMEM((shards, tokens, cols), F32),
            pltpu.VMEM((shards, tokens, cols), F32),
            pltpu.VMEM((mine, groups, tokens, cols), BF16),
            pltpu.VMEM((mine, groups, tokens, cols), BF16),
            pltpu.VMEM((mine, groups, 1, tokens * cols // HD), F32),
            pltpu.VMEM((mine, groups, 1, tokens * cols // HD), F32),
            pltpu.VMEM((cols // LANES, LANES, groups), F32),
            pltpu.VMEM((tokens // 2, cols), BF16),
            pltpu.VMEM((2, tokens // 2, chips * cols), F32),
            pltpu.VMEM((mine * tokens, chips * cols), BF16),
            pltpu.VMEM((mine * tokens, chips * cols), BF16),
            pltpu.VMEM((mine * tokens, chips * cols), BF16),
            pltpu.VMEM((chips, mine * tokens, cols), BF16),
            pltpu.VMEM((16, width), F32),
            pltpu.VMEM((width,), BF16),
            pltpu.VMEM((width,), BF16),
            pltpu.SMEM(question_of.shape[:2], jnp.int32),
            pltpu.SMEM((questions,), jnp.int32),
            pltpu.SMEM((questions,), jnp.int32),
            pltpu.SMEM((questions,), jnp.int32),
            dma(CHUNKS + 7),
            one, dma(messages), dma(messages),
            one, dma(1 + messages),
            one, one, one, dma(pieces), one, dma(mine),
            one, dma(pieces), one, dma(pieces),
            pltpu.SemaphoreType.REGULAR, pltpu.SemaphoreType.REGULAR,
        ],
        compiler_params=pltpu.CompilerParams(
            collective_id=0, has_side_effects=True, vmem_limit_bytes=60 * 1024 * 1024
        ),
        name="reader_step",
    )(
        question_of[:, :, 0],
        states.reshape(plen, width),
        enc_gain,
        dec_states.reshape(mine * tokens, width),
        dec_gain,
        query_weight,
        key_value_weight,
        out_weight,
    )


def solution(mesh):
    return jax.shard_map(
        body,
        mesh=mesh,
        in_specs=(
            P(("groups", "qset"), "seq", None, None),
            P(),
            P(("groups", "qset"), None, None),
            P(),
            P(None, "seq"),
            P(None, None, "seq"),
            P("seq", None),
            P("groups", None, None),
        ),
        out_specs=P(("groups", "qset"), None, "seq"),
        check_vma=False,
    )
```

```python
import functools

import jax
import jax.numpy as jnp
from jax import lax
from jax.experimental import pallas as pl
from jax.experimental.pallas import tpu as pltpu
from jax.sharding import PartitionSpec as P

HD = 64
EPSILON = 1e-06
DEAD = -1e30
LANES = 128
CORES = 2
CHUNKS = 4
LAG = 4
PARTS = 2
F32 = jnp.float32
BF16 = jnp.bfloat16


def normalise(src, gain, dst_at, start, rows_here):
    step = 16

    def one(i, carry):
        at = pl.ds(pl.multiple_of(start + i * step, step), step)
        rows = src[at, :].astype(F32)
        mean_square = jnp.mean(rows * rows, axis=-1, keepdims=True)
        dst_at[at, :] = (rows * lax.rsqrt(mean_square + EPSILON) * gain[...]).astype(BF16)
        return carry

    lax.fori_loop(0, rows_here // step, one, 0)


def kernel(
    table_hbm, states_hbm, enc_gain_hbm, dec_hbm, dec_gain_hbm, wq_hbm, wkv_hbm, wo_hbm, out_ref,
    raw, dec_raw, dec_rows, rows, wq, wkv_in, wkv, wo, kv, qbuf, num, peak, total,
    osend, orecv, lsend, lrecv, shares, att, half, psend, precv, xsend, xrecv, gains,
    enc_gain, dec_gain, table, first, second, hits,
    load_sem, rs, rr, lr, ds, dr, qs, qr, os_, or_, ss, sr, ps, pr, xs, xr, rising, falling,
):
    shards, groups = lax.axis_size("seq"), lax.axis_size("qset")
    chips = shards // CORES
    me, g = lax.axis_index("seq"), lax.axis_index("qset")
    x, c = lax.div(me, CORES), lax.rem(me, CORES)
    plen, width = raw.shape
    questions, tokens, cols = qbuf.shape
    mine = questions // groups
    piece = plen // CHUNKS
    messages = (chips - 1) * CHUNKS // 2

    def seq_at(chip, core):
        return lax.rem(chip + 2 * chips, chips) * CORES + core

    right, left = seq_at(x + 1, c), seq_at(x - 1, c)
    other = 1 - c
    partner = seq_at(x, other)

    def load(i, src, dst):
        return pltpu.make_async_copy(src, dst, load_sem.at[i])

    def states_load(k):
        at = pl.ds(k * piece, piece)
        return load(k, states_hbm.at[at], raw.at[at])

    enc_gain_load = load(CHUNKS, enc_gain_hbm, enc_gain)
    dec_load = load(CHUNKS + 1, dec_hbm, dec_raw)
    wq_load = load(CHUNKS + 2, wq_hbm, wq)
    wkv_load = load(CHUNKS + 3, wkv_hbm, wkv_in)
    dec_gain_load = load(CHUNKS + 4, dec_gain_hbm, dec_gain)
    table_load = load(CHUNKS + 5, table_hbm, table)

    def wo_load(i):
        chip, core = lax.div(i, CORES), lax.rem(i, CORES)
        src = wo_hbm.at[:, pl.ds(pl.multiple_of(i * cols, cols), cols)]
        dst = wo.at[core, :, pl.ds(pl.multiple_of(chip * cols, cols), cols)]
        return load(CHUNKS + 6, src, dst)

    inward = [k // 2 if k % 2 == 0 else CHUNKS - 1 - k // 2 for k in range(CHUNKS)]
    enc_gain_load.start()
    for k in inward:
        states_load(k).start()

    barrier = pltpu.get_barrier_semaphore()
    above, below = g + 1, g - 1

    def if_above(do):
        pl.when(g < groups - 1)(do)

    def if_below(do):
        pl.when(g > 0)(do)

    pl.semaphore_signal(barrier, inc=1, device_id={"seq": left})
    pl.semaphore_signal(barrier, inc=1, device_id={"seq": right})

    @pl.when(c == 1)
    def _():
        pl.semaphore_signal(barrier, inc=1, device_id={"seq": partner})

    if_below(lambda: pl.semaphore_signal(barrier, inc=1, device_id={"qset": below}))

    def part(slot, chunk):
        return rows.at[slot, pl.ds(pl.multiple_of(chunk * piece, piece), piece), :]

    def right_copy(m, behind):
        at = part(seq_at(x - lax.div(m, CHUNKS) - behind, c), lax.rem(m, CHUNKS))
        return pltpu.make_async_remote_copy(at, at, rs, rr.at[m], device_id={"seq": right})

    def left_copy(m, behind):
        at = part(seq_at(x + lax.div(m, CHUNKS) + behind, c), CHUNKS - 1 - lax.rem(m, CHUNKS))
        return pltpu.make_async_remote_copy(at, at, rs, lr.at[m], device_id={"seq": left})

    def die_copy(at, k):
        return pltpu.make_async_remote_copy(at, at, ds, dr.at[k], device_id={"seq": partner})

    def die_own(slot):
        return die_copy(rows.at[slot], 0)

    def from_left(m, core):
        return seq_at(x - lax.div(m, CHUNKS) - 1, core), lax.rem(m, CHUNKS)

    def from_right(m, core):
        return seq_at(x + lax.div(m, CHUNKS) + 1, core), CHUNKS - 1 - lax.rem(m, CHUNKS)

    enc_gain_load.wait()
    gains[0:1, :] = enc_gain[...].astype(F32).reshape(1, width)
    done, sent_right, sent_left = set(), 0, 0
    for k in inward:
        states_load(k).wait()
        normalise(raw, gains.at[0:1, :], rows.at[me], k * piece, piece)
        if not done:
            pl.semaphore_wait(barrier, 2 + (1 - c) + 1 - lax.div(g + 1, groups))
        done.add(k)
        while sent_right in done:
            right_copy(jnp.int32(sent_right), 0).start()
            sent_right += 1
        while CHUNKS - 1 - sent_left in done:
            left_copy(jnp.int32(sent_left), 0).start()
            sent_left += 1
    for one in (wkv_load, dec_load, dec_gain_load, wq_load, table_load):
        one.start()
    lax.fori_loop(0, shards, lambda i, n: (wo_load(i).start(), n)[1], 0)

    @pl.when(c == 0)
    def _():
        die_own(me).start()

    @pl.when(g == 0)
    def _():
        pl.semaphore_signal(rising, inc=1, device_id={"qset": above})

    own_q = qbuf.at[pl.ds(g * mine, mine)]

    def own_queries():
        dec_load.wait()
        dec_gain_load.wait()
        gains[8:9, :] = dec_gain[...].astype(F32).reshape(1, width)
        normalise(dec_raw, gains.at[8:9, :], dec_rows, 0, dec_raw.shape[0])
        wq_load.wait()
        queries = jnp.dot(dec_rows[...], wq[...], preferred_element_type=F32).astype(BF16)
        own_q[...] = queries.reshape(mine, tokens, cols)

    def query_copy(i):
        to = lax.rem(g + i, groups)
        return pltpu.make_async_remote_copy(
            own_q, own_q, qs, qr, device_id={"qset": to}
        )

    def query_all():
        at = qbuf.at[pl.ds(0, questions - mine)]
        return pltpu.make_async_remote_copy(at, at, qs, qr, device_id={"qset": above})

    passages = table.shape[1]

    def find(q, n):
        def look(p, found):
            at0, at1, count = found
            hit = table[g, p] == q
            at0 = jnp.where(hit & (count == 0), p, at0)
            at1 = jnp.where(hit & (count == 1), p, at1)
            return at0, at1, count + hit.astype(jnp.int32)

        zero = jnp.int32(0)
        at0, at1, count = lax.fori_loop(0, passages, look, (zero, zero, zero))
        first[q], second[q], hits[q] = at0, at1, count
        return n

    lane = lax.broadcasted_iota(jnp.int32, (1, LANES), 1)
    low = lane < HD

    def key_values(slots):
        together = jnp.concatenate([part(*s)[...] for s in slots], axis=0)
        result = jnp.dot(together, wkv[...], preferred_element_type=F32).astype(BF16)
        for i, (slot, chunk) in enumerate(slots):
            at = pl.ds(pl.multiple_of(chunk * piece, piece), piece)
            kv[slot, at, :] = result[i * piece : (i + 1) * piece]

    def attend(slot):
        asked = qbuf[table[g, slot]]
        ats = [slice(j * LANES, (j + 1) * LANES) for j in range(cols // LANES)]
        scores = []
        for at in ats:
            pair = asked[:, at]
            none = jnp.zeros_like(pair)
            stacked = jnp.concatenate([jnp.where(low, pair, none), jnp.where(low, none, pair)], axis=0)
            scores.append(
                lax.dot_general(
                    stacked, kv[slot, :, at], (((1,), (1,)), ((), ())), preferred_element_type=F32
                )
            )
        tops = [jnp.max(one, axis=-1, keepdims=True) for one in scores]
        weights = [jnp.exp(one - top) for one, top in zip(scores, tops)]
        products = [
            jnp.dot(
                one.astype(BF16),
                kv[slot, :, cols + j * LANES : cols + (j + 1) * LANES],
                preferred_element_type=F32,
            )
            for j, one in enumerate(weights)
        ]
        sums = [jnp.sum(one, axis=-1, keepdims=True) for one in weights]
        for at, top, summed, product in zip(ats, tops, sums, products):
            num[slot, :, at] = jnp.where(low, product[:tokens], product[tokens:])
            peak[slot, :, at] = jnp.where(low, top[:tokens], top[tokens:])
            total[slot, :, at] = jnp.where(low, summed[:tokens], summed[tokens:])

    wkv_load.wait()
    block = 64

    def unzip(i, n):
        at = pl.ds(pl.multiple_of(i * block, block), block)
        wkv[at, :cols] = wkv_in[at, 0, :]
        wkv[at, cols:] = wkv_in[at, 1, :]
        return n

    lax.fori_loop(0, width // block, unzip, 0)

    def whole_values(slot):
        result = jnp.dot(rows[slot], wkv[...], preferred_element_type=F32)
        kv[slot] = result.astype(BF16)

    def partner_part(m):
        die_copy(rows.at[partner, pl.ds(0, 2 * piece)], 1 + m).wait_recv()
        key_values([from_left(m, other), from_right(m, other)])

    def die_right(m):
        die_copy(part(*from_left(m, c)), 1 + m).start()

    def die_left(m):
        die_copy(part(*from_right(m, c)), 1 + m).start()

    hold = 2
    catch = messages - 4
    partner_at = min(LAG, catch)

    def part_done(m):
        return m + LAG if m + LAG < catch else max(catch, m + 1)

    def step(m, n):
        @pl.when(m > catch)
        def _():
            partner_part(m - 1)

        right_copy(m, 1).wait_recv()

        @pl.when(m + CHUNKS < messages)
        def _():
            right_copy(m + CHUNKS, 0).start()

        @pl.when((1 - c) * messages + m > hold)
        def _():
            die_right(m)

        left_copy(m, 1).wait_recv()

        @pl.when(m + CHUNKS < messages)
        def _():
            left_copy(m + CHUNKS, 0).start()

        @pl.when((1 - c) * messages + m > hold)
        def _():
            die_left(m)

        @pl.when(m == 0)
        def _():
            whole_values(me)

        key_values([from_left(m, c), from_right(m, c)])

        @pl.when(m == 1)
        def _():
            own_queries()
            if_below(lambda: pl.semaphore_wait(rising, 1))

            @pl.when(g > 0)
            def _():
                if_above(
                    lambda: pl.semaphore_signal(rising, inc=1, device_id={"qset": above})
                )

        @pl.when(m == hold)
        def _():
            @pl.when(c == 1)
            def _():
                die_own(partner).wait_recv()
                die_own(me).start()

                def late(k, t):
                    die_right(k)
                    die_left(k)
                    return t

                lax.fori_loop(0, hold + 1, late, 0)

            if_above(lambda: pl.semaphore_wait(falling, 1))
            if_below(lambda: pl.semaphore_signal(falling, inc=1, device_id={"qset": below}))
            lax.fori_loop(1, groups, lambda i, k: (query_copy(i).start(), k)[1], 0)

        @pl.when(m == hold + 1)
        def _():
            table_load.wait()
            lax.fori_loop(0, questions, find, 0)

        @pl.when(m == partner_at)
        def _():
            @pl.when(c == 0)
            def _():
                die_own(partner).wait_recv()

            whole_values(partner)

        if catch > LAG:

            @pl.when(m >= LAG)
            def _():
                @pl.when(m < catch)
                def _():
                    partner_part(m - LAG)

        @pl.when(m == catch)
        def _():
            lax.fori_loop(
                max(0, catch - LAG), catch, lambda k, t: (partner_part(k), t)[1], 0
            )

        @pl.when(m == messages // 2)
        def _():
            query_all().wait_recv()
            lax.fori_loop(0, CORES, lambda i, k: (attend(seq_at(x, i)), k)[1], 0)

        for far in range(1, chips // 2):

            @pl.when(m == max(part_done(far * CHUNKS - 1), messages // 2 + far))
            def _():
                def both(i, k):
                    attend(seq_at(x - far, i))
                    attend(seq_at(x + far, i))
                    return k

                lax.fori_loop(0, CORES, both, 0)

        return n

    lax.fori_loop(0, messages, step, 0)
    attend(seq_at(x + chips // 2, c))
    partner_part(messages - 1)
    attend(seq_at(x + chips // 2, other))

    pairs = cols // LANES

    def alternate(k, n):
        reach = lax.div(k + 1, 2)
        return n // 2 - reach + 2 * reach * lax.rem(k, 2)

    short = tokens // PARTS

    def out_copy(own, cut, i):
        to = lax.rem(g + i, groups)
        here = pl.ds(cut * short, short)
        return pltpu.make_async_remote_copy(
            osend.at[own, to, here],
            orecv.at[own, g, here],
            os_, or_.at[own * PARTS + cut], device_id={"qset": to},
        )

    def out_all(own, cut):
        at = orecv.at[own, pl.ds(0, groups - 1), pl.ds(cut * short, short)]
        return pltpu.make_async_remote_copy(
            at, at, os_, or_.at[own * PARTS + cut], device_id={"qset": above}
        )

    def lse_copy(own, i):
        to = lax.rem(g + i, groups)
        return pltpu.make_async_remote_copy(
            lsend.at[own, to],
            lrecv.at[own, g],
            ss, sr.at[own], device_id={"qset": to},
        )

    def lse_all(own):
        at = lrecv.at[own, pl.ds(0, groups - 1)]
        return pltpu.make_async_remote_copy(at, at, ss, sr.at[own], device_id={"qset": above})

    def merge(own, to, mix_at, lse_at):
        q = to * mine + own
        at0, at1, count = first[q], second[q], hits[q]
        lses = []
        for j in range(pairs):
            at = slice(j * LANES, (j + 1) * LANES)
            top0 = jnp.where(count >= 1, peak[at0, :, at], DEAD)
            top1 = jnp.where(count >= 2, peak[at1, :, at], DEAD)
            top = jnp.maximum(top0, top1)
            scale0 = jnp.where(count >= 1, jnp.exp(top0 - top), 0.0)
            scale1 = jnp.where(count >= 2, jnp.exp(top1 - top), 0.0)
            mass = scale0 * total[at0, :, at] + scale1 * total[at1, :, at]
            mass = jnp.where(count >= 1, mass, 1.0)
            mix = (scale0 * num[at0, :, at] + scale1 * num[at1, :, at]) / mass
            mix_at[:, at] = mix.astype(BF16)
            lse = jnp.where(count >= 1, top + jnp.log(mass), DEAD)
            turned = jnp.transpose(lse)
            lses += [turned[:1], turned[HD : HD + 1]]
        lse_at[...] = jnp.concatenate(lses, axis=1)

    def merge_and_send(own):
        def one(k, n):
            i = alternate(k, groups)
            to = lax.rem(g + i, groups)
            merge(own, to, osend.at[own, to], lsend.at[own, to])
            lse_copy(own, i).start()
            out_copy(own, 0, i).start()
            return n

        lax.fori_loop(0, groups - 1, one, 0)
        for cut in range(1, PARTS):

            def rest(k, n):
                out_copy(own, cut, alternate(k, groups)).start()
                return n

            lax.fori_loop(0, groups - 1, rest, 0)

    for own in range(mine):
        merge_and_send(own)
    for own in range(mine):
        merge(own, g, orecv.at[own, g], lrecv.at[own, g])
    pltpu.make_async_copy(wo, wo, load_sem.at[CHUNKS + 6]).wait()

    def pair_copy(piece):
        return pltpu.make_async_remote_copy(
            psend.at[piece], precv.at[piece], ps, pr.at[piece],
            device_id={"seq": partner},
        )

    def chip_part(chip):
        return pl.ds(pl.multiple_of(chip * cols, cols), cols)

    def sum_copy(piece, i):
        to = lax.rem(x + i, chips)
        return pltpu.make_async_remote_copy(
            xsend.at[piece, :, chip_part(to)], xrecv.at[piece, i],
            xs, xr.at[piece], device_id={"seq": seq_at(to, c)},
        )

    def sum_all(piece):
        at = xrecv.at[piece, pl.ds(1, chips - 1)]
        return pltpu.make_async_remote_copy(at, at, xs, xr.at[piece], device_id={"seq": right})

    def share_of(own):
        lse_all(own).wait_recv()
        every = jnp.concatenate([lrecv[own, k] for k in range(groups)], axis=0)
        top = jnp.max(every, axis=0, keepdims=True)
        share = jnp.exp(every - top)
        share = share / jnp.sum(share, axis=0, keepdims=True)
        for j in range(pairs):
            shares[j] = jnp.transpose(share[:, j * LANES : (j + 1) * LANES])

    def project(own, cut):
        piece = own * PARTS + cut
        here = slice(cut * short, (cut + 1) * short)
        odd_here = slice(HD + cut * short, HD + (cut + 1) * short)
        out_all(own, cut).wait_recv()
        for j in range(pairs):
            at = slice(j * LANES, (j + 1) * LANES)
            mixed = jnp.zeros((short, LANES), F32)
            for source in range(groups):
                at_source = slice(source, source + 1)
                scale = jnp.where(
                    low, shares[j, here, at_source], shares[j, odd_here, at_source]
                )
                mixed = mixed + scale * orecv[own, source, here, at].astype(F32)
            att[:, at] = mixed.astype(BF16)

        psend[piece] = jnp.dot(att[...], wo[other], preferred_element_type=F32).astype(BF16)
        pair_copy(piece).start()
        half[...] = jnp.dot(att[...], wo[c], preferred_element_type=F32)
        pair_copy(piece).wait_recv()

        def add(i):
            at = chip_part(lax.rem(x + i, chips))
            xsend[piece, :, at] = (half[:, at] + precv[piece, :, at].astype(F32)).astype(BF16)

        def to_chip(k, n):
            i = alternate(k, chips)
            add(i)
            sum_copy(piece, i).start()
            return n

        lax.fori_loop(0, chips - 1, to_chip, 0)
        add(0)

    for own in range(mine):
        share_of(own)
        for cut in range(PARTS):
            project(own, cut)

    def sent(all_of, sem):
        pltpu.make_async_remote_copy(
            all_of, all_of, sem, qr, device_id={"seq": right}
        ).wait_send()

    sent(rows.at[pl.ds(0, chips - 1)], rs)
    sent(rows.at[pl.ds(0, chips)], ds)
    sent(qbuf.at[pl.ds(0, questions - mine)], qs)
    sent(osend.at[:, pl.ds(0, groups - 1)], os_)
    sent(lsend.at[:, pl.ds(0, groups - 1)], ss)
    feature = pl.ds(pl.multiple_of(me * cols, cols), cols)
    for piece in range(mine * PARTS):
        here = slice(piece * short, (piece + 1) * short)
        result = dec_raw[here, feature].astype(F32) + xsend[piece, :, chip_part(x)].astype(F32)
        sum_all(piece).wait_recv()
        for i in range(1, chips):
            result = result + xrecv[piece, i].astype(F32)
        own, cut = divmod(piece, PARTS)
        out_ref[own, cut * short : (cut + 1) * short, :] = result.astype(BF16)
    sent(psend, ps)
    sent(xrecv.at[:, pl.ds(0, chips - 1)], xs)


def body(
    states, enc_gain, dec_states, dec_gain, query_weight, key_value_weight, out_weight, question_of
):
    shards, groups = lax.axis_size("seq"), lax.axis_size("qset")
    chips = shards // CORES
    plen, width = states.shape[2:]
    mine, tokens = dec_states.shape[:2]
    cols = query_weight.shape[1]
    questions = mine * groups
    messages = (chips - 1) * CHUNKS // 2
    pieces, short = mine * PARTS, tokens // PARTS
    hbm = pl.BlockSpec(memory_space=pl.ANY)
    vmem = pl.BlockSpec(memory_space=pltpu.VMEM)
    dma = lambda n: pltpu.SemaphoreType.DMA((n,))
    one = pltpu.SemaphoreType.DMA
    return pl.pallas_call(
        kernel,
        out_shape=pltpu.VMEM((mine, tokens, cols), BF16),
        in_specs=[hbm] * 8,
        out_specs=vmem,
        scratch_shapes=[
            pltpu.VMEM((plen, width), BF16),
            pltpu.VMEM((mine * tokens, width), BF16),
            pltpu.VMEM((mine * tokens, width), BF16),
            pltpu.VMEM((shards, plen, width), BF16),
            pltpu.VMEM((width, cols), BF16),
            pltpu.VMEM((width, 2, cols), BF16),
            pltpu.VMEM((width, 2 * cols), BF16),
            pltpu.VMEM((CORES, cols, chips * cols), BF16),
            pltpu.VMEM((shards, plen, 2 * cols), BF16),
            pltpu.VMEM((questions, tokens, cols), BF16),
            pltpu.VMEM((shards, tokens, cols), F32),
            pltpu.VMEM((shards, tokens, cols), F32),
            pltpu.VMEM((shards, tokens, cols), F32),
            pltpu.VMEM((mine, groups, tokens, cols), BF16),
            pltpu.VMEM((mine, groups, tokens, cols), BF16),
            pltpu.VMEM((mine, groups, 1, tokens * cols // HD), F32),
            pltpu.VMEM((mine, groups, 1, tokens * cols // HD), F32),
            pltpu.VMEM((cols // LANES, LANES, groups), F32),
            pltpu.VMEM((short, cols), BF16),
            pltpu.VMEM((short, chips * cols), F32),
            pltpu.VMEM((pieces, short, chips * cols), BF16),
            pltpu.VMEM((pieces, short, chips * cols), BF16),
            pltpu.VMEM((pieces, short, chips * cols), BF16),
            pltpu.VMEM((pieces, chips, short, cols), BF16),
            pltpu.VMEM((16, width), F32),
            pltpu.VMEM((width,), BF16),
            pltpu.VMEM((width,), BF16),
            pltpu.SMEM(question_of.shape[:2], jnp.int32),
            pltpu.SMEM((questions,), jnp.int32),
            pltpu.SMEM((questions,), jnp.int32),
            pltpu.SMEM((questions,), jnp.int32),
            dma(CHUNKS + 7),
            one, dma(messages), dma(messages),
            one, dma(1 + messages),
            one, one, one, dma(pieces), one, dma(mine),
            one, dma(pieces), one, dma(pieces),
            pltpu.SemaphoreType.REGULAR, pltpu.SemaphoreType.REGULAR,
        ],
        compiler_params=pltpu.CompilerParams(
            collective_id=0, has_side_effects=True, vmem_limit_bytes=60 * 1024 * 1024
        ),
        name="reader_step",
    )(
        question_of[:, :, 0],
        states.reshape(plen, width),
        enc_gain,
        dec_states.reshape(mine * tokens, width),
        dec_gain,
        query_weight,
        key_value_weight,
        out_weight,
    )


def solution(mesh):
    return jax.shard_map(
        body,
        mesh=mesh,
        in_specs=(
            P(("groups", "qset"), "seq", None, None),
            P(),
            P(("groups", "qset"), None, None),
            P(),
            P(None, "seq"),
            P(None, None, "seq"),
            P("seq", None),
            P("groups", None, None),
        ),
        out_specs=P(("groups", "qset"), None, "seq"),
        check_vma=False,
    )
```
